32 devices in a mesh: dp: 32 (over z, y, x, core).
Axes of the slice: x: 2, y: 2, z: 4, core: 2. Of those that a mesh axis runs over, the one named last changes fastest.
Arguments:
- tokens: bfloat16 [32768, 1024], P('dp'), may hold values from -6 to 6
- segment_ids: int32 [64, 512], P('dp'), may hold values from 0 to 15, never falling along the last dimension, each value on 1 to 256 neighbouring positions
- out_grad: bfloat16 [32768, 1024], P('dp'), may hold values from -6 to 6
- qkv_master: float32 [3145728], P('dp'), may hold values from -0.1875 to 0.1875
- qkv_first: float32 [3145728], P('dp'), may hold values from -320 to 320
- qkv_second: float32 [3145728], P('dp'), may hold values from 327.68 to 32768
- proj_master: float32 [1048576], P('dp'), may hold values from -1 to 1
- proj_first: float32 [1048576], P('dp'), may hold values from -320 to 320
- proj_second: float32 [1048576], P('dp'), may hold values from 327.68 to 32768
- up_master: float32 [4194304], P('dp'), may hold values from -0.1875 to 0.1875
- up_first: float32 [4194304], P('dp'), may hold values from -320 to 320
- up_second: float32 [4194304], P('dp'), may hold values from 327.68 to 32768
- down_master: float32 [4194304], P('dp'), may hold values from -0.09375 to 0.09375
- down_first: float32 [4194304], P('dp'), may hold values from -320 to 320
- down_second: float32 [4194304], P('dp'), may hold values from 327.68 to 32768
- vector_master: float32 [12288], P('dp'), may hold values from -1.5 to 1.5, as said below
- vector_first: float32 [12288], P('dp'), may hold values from -320 to 320
- vector_second: float32 [12288], P('dp'), may hold values from 327.68 to 32768
Outputs:
- layer_out: bfloat16 [32768, 1024], P('dp')
- input_grad: bfloat16 [32768, 1024], P('dp')
- qkv_grad: float32 [3145728], P('dp')
- qkv_first_new: float32 [3145728], P('dp')
- qkv_second_new: float32 [3145728], P('dp')
- qkv_master_new: float32 [3145728], P('dp')
- qkv_copy: bfloat16 [3145728], P('dp')
- proj_grad: float32 [1048576], P('dp')
- proj_first_new: float32 [1048576], P('dp')
- proj_second_new: float32 [1048576], P('dp')
- proj_master_new: float32 [1048576], P('dp')
- proj_copy: bfloat16 [1048576], P('dp')
- up_grad: float32 [4194304], P('dp')
- up_first_new: float32 [4194304], P('dp')
- up_second_new: float32 [4194304], P('dp')
- up_master_new: float32 [4194304], P('dp')
- up_copy: bfloat16 [4194304], P('dp')
- down_grad: float32 [4194304], P('dp')
- down_first_new: float32 [4194304], P('dp')
- down_second_new: float32 [4194304], P('dp')
- down_master_new: float32 [4194304], P('dp')
- down_copy: bfloat16 [4194304], P('dp')
- vector_grad: float32 [12288], P('dp')
- vector_first_new: float32 [12288], P('dp')
- vector_second_new: float32 [12288], P('dp')
- vector_master_new: float32 [12288], P('dp')
- vector_copy: bfloat16 [12288], P('dp')
The draws below stay inside these ranges and needn't reach their ends.
Inputs may be any that keep to these rules, and one draw needn't show every extreme that they name: `segment_ids`: ids never fall along a sequence; tokens attend only to tokens of the same id. `vector_master`: the two norm gains lie in 0.5 to 1.5.
All inputs are finite; a program needn't handle non-finite values.
Results may differ from the reference program's by a relative error of at most 0.012.
The reference program's roundings to bfloat16 on the way count: a program that leaves them out, or rounds other values in their place, can miss the bound.
Values may be sent and summed in bfloat16 or wider, within the bound.
A program may use at most 256 MiB of HBM per device.

```python
import math
import jax
import jax.numpy as jnp
import numpy as np
from jax import lax

D = 1024
HEADS = 16
HEAD_DIM = 64
FF = 4096
LEN = 512
DOCS = 16
STEP = 3
SEQS = 64
TOKENS = 32768
VEC = 12288


def draw_vector_master(key, part):
    position = jnp.arange(VEC)
    in_gain = (position >= 3 * D) & (position < 4 * D) | (position >= 6 * D + FF) & (position < 7 * D + FF)
    gain_draw = jax.random.uniform(jax.random.fold_in(key, 1), (VEC,), jnp.float32, 0.5, 1.5)
    others = jnp.clip(0.5 * jax.random.normal(jax.random.fold_in(key, 2), (VEC,), jnp.float32), -1.5, 1.5)
    return jnp.where(in_gain, gain_draw, others)


def with_spikes(entries, own_key, source, target, shards_of, factor):
    def block_of(dim):
        return (jnp.arange(entries.shape[dim]) // (entries.shape[dim] // shards_of)).reshape((-1,) + (1,) * (entries.ndim - 1 - dim))

    near = jax.random.permutation(own_key, shards_of)[block_of(target)]
    second = (block_of(target) + shards_of // 2) % shards_of
    return jnp.where((block_of(source) == near) | (block_of(source) == second), factor * entries, entries)


def block_levels(own_key, shape, split, least, largest):
    def one(dim, shards_of):
        draws = jax.random.uniform(jax.random.fold_in(jax.random.fold_in(own_key, 6), dim), (shards_of,), jnp.float32, least / len(split), largest / len(split))
        return jnp.repeat(jnp.exp(draws), shape[dim] // shards_of).reshape((-1,) + (1,) * (len(shape) - dim - 1))

    loudness = one(*split[0])
    for cut in split[1:]:
        loudness = loudness * one(*cut)
    return loudness


def length_profile(amount, total, most, skew):
    loads = [(1 << 20) // math.isqrt(rank ** skew) + 1 for rank in range(2, amount + 1)]
    spare, holding = total - most - (amount - 1), [1] * (amount - 1)
    while spare > 0:
        candidates = [i for i in range(amount - 1) if holding[i] < most]
        mass, remaining = sum([loads[i] for i in candidates]), spare
        for i in candidates:
            more = min(most - holding[i], max(1, remaining * loads[i] // mass), spare)
            holding[i] = holding[i] + more
            spare = spare - more
    return np.array([most] + holding)


def uneven_parts(stream_key, count, total, bound, lean):
    if count == 2:
        one = jax.random.randint(stream_key, (), max(1, total - bound), min(bound, total - 1) + 1)
        return jnp.stack([one, total - one])
    lengths = jnp.asarray(length_profile(count, total, bound, lean), jnp.int32)
    twos = (count - 1) // 2
    giver, taker = lengths[1:1 + 2 * twos:2], lengths[2:2 + 2 * twos:2]
    margin = jnp.minimum(giver - 1, bound - taker)
    passed = jax.random.randint(jax.random.fold_in(stream_key, 1), (twos,), 0, 1 << 20) % (margin + 1)
    lengths = lengths.at[1:1 + 2 * twos:2].set(giver - passed).at[2:2 + 2 * twos:2].set(taker + passed)
    return lengths[jax.random.permutation(jax.random.fold_in(stream_key, 2), count)]


def noise(key, shape, deviation, limit, shards=(), dtype=jnp.bfloat16):
    level = block_levels(key, shape, shards, -0.22, 0.18) if shards else 1.0
    values = jax.random.normal(key, shape, jnp.float32) * deviation * level
    return jnp.minimum(jnp.maximum(values, -limit), limit).astype(dtype)


def noise_with(rng, dims, scale, limit, shards, heavy, dtype=jnp.bfloat16):
    values = scale * jax.random.normal(rng, dims, jnp.float32)
    if shards:
        values = values * block_levels(rng, dims, shards, -0.22, 0.18)
    return jnp.clip(with_spikes(values, jax.random.fold_in(rng, 3), *heavy), -limit, limit).astype(dtype)


def setup_inputs(seed: int = 0) -> dict:
    seeds = jax.random.split(jax.random.key(seed), 19)
    tokens = noise(seeds[0], (TOKENS, D), 1.0, 6.0, ((0, 32),))
    segment_ids = jax.vmap(lambda own: jnp.searchsorted(jnp.cumsum(uneven_parts(own, DOCS, LEN, LEN // 2, 2)), jnp.arange(LEN), side="right"))(jax.random.split(seeds[1], SEQS)).reshape((SEQS, LEN)).astype(jnp.int32)
    out_grad = noise_with(seeds[2], (TOKENS, D), 1.0, 6.0, ((0, 32),), (0, 1, 32, 2.75))
    qkv_master = noise(seeds[3], (3 * D * D,), D ** -0.5, 0.1875, ((0, 32),), jnp.float32)
    qkv_first = noise(seeds[4], (3 * D * D,), (0.3 * TOKENS ** 0.5), 320.0, ((0, 32),), jnp.float32)
    qkv_second = jnp.clip(jnp.exp(math.log(32768.0) - 4.6051702 * jax.random.uniform(seeds[5], (3 * D * D,), jnp.float32) ** block_levels(seeds[5], (3 * D * D,), ((0, 32),), -0.2, 0.2)), 327.68, 32768.0)
    proj_master = noise(seeds[6], (D * D,), (D // 32) ** -0.5, 1.0, ((0, 32),), jnp.float32)
    proj_first = noise(seeds[7], (D * D,), (0.3 * TOKENS ** 0.5), 320.0, ((0, 32),), jnp.float32)
    proj_second = jnp.clip(jnp.exp(math.log(32768.0) - 4.6051702 * jax.random.uniform(seeds[8], (D * D,), jnp.float32) ** block_levels(seeds[8], (D * D,), ((0, 32),), -0.2, 0.2)), 327.68, 32768.0)
    up_master = noise(seeds[9], (D * FF,), D ** -0.5, 0.1875, ((0, 32),), jnp.float32)
    up_first = noise(seeds[10], (D * FF,), (0.3 * TOKENS ** 0.5), 320.0, ((0, 32),), jnp.float32)
    up_second = jnp.clip(jnp.exp(math.log(32768.0) - 4.6051702 * jax.random.uniform(seeds[11], (D * FF,), jnp.float32) ** block_levels(seeds[11], (D * FF,), ((0, 32),), -0.2, 0.2)), 327.68, 32768.0)
    down_master = noise(seeds[12], (FF * D,), FF ** -0.5, 0.09375, ((0, 32),), jnp.float32)
    down_first = noise(seeds[13], (FF * D,), (0.3 * TOKENS ** 0.5), 320.0, ((0, 32),), jnp.float32)
    down_second = jnp.clip(jnp.exp(math.log(32768.0) - 4.6051702 * jax.random.uniform(seeds[14], (FF * D,), jnp.float32) ** block_levels(seeds[14], (FF * D,), ((0, 32),), -0.2, 0.2)), 327.68, 32768.0)
    vector_master = draw_vector_master(jax.random.fold_in(seeds[18], 71), 0)
    vector_first = noise(seeds[16], (VEC,), (0.3 * TOKENS ** 0.5), 320.0, ((0, 32),), jnp.float32)
    vector_second = jnp.clip(jnp.exp(math.log(32768.0) - 4.6051702 * jax.random.uniform(seeds[17], (VEC,), jnp.float32) ** block_levels(seeds[17], (VEC,), ((0, 32),), -0.2, 0.2)), 327.68, 32768.0)
    return {"tokens": tokens, "segment_ids": segment_ids, "out_grad": out_grad, "qkv_master": qkv_master, "qkv_first": qkv_first, "qkv_second": qkv_second, "proj_master": proj_master, "proj_first": proj_first, "proj_second": proj_second, "up_master": up_master, "up_first": up_first, "up_second": up_second, "down_master": down_master, "down_first": down_first, "down_second": down_second, "vector_master": vector_master, "vector_first": vector_first, "vector_second": vector_second}


@jax.custom_vjp
def low(v):
    return lax.optimization_barrier(v.astype(jnp.bfloat16)).astype(jnp.float32)

@jax.custom_vjp
def low_back(v):
    return v

def low_keep(v):
    return (low(v), None)

def low_pass(kept, grad):
    return (grad,)

def back_keep(v):
    return (v, None)

def back_low(kept, grad):
    return (low(grad),)
low.defvjp(low_keep, low_pass)
low_back.defvjp(back_keep, back_low)
NORM_EPS = 1e-05
BETA_FIRST = 0.5
BETA_SECOND = 0.5
ADAM_EPS = 1e-08
WEIGHT_DECAY = 0.01
MASK_FILL = -1000000000.0
RATES = (0.01, 0.03, 0.01, 0.005, 0.05)

def layer_norm(hidden, gain, shift):
    center = hidden - lax.optimization_barrier(jnp.mean(hidden, axis=-1, keepdims=True))
    spread = lax.optimization_barrier(jnp.mean(center * center, axis=-1, keepdims=True))
    return center * lax.rsqrt(spread + NORM_EPS) * gain + shift

def split_vector(vector):
    return (vector[0:D], vector[D:2 * D], vector[2 * D:3 * D], vector[3 * D:4 * D], vector[4 * D:5 * D], vector[5 * D:5 * D + FF], vector[5 * D + FF:6 * D + FF], vector[6 * D + FF:7 * D + FF], vector[7 * D + FF:8 * D + FF])

def forward(inputs, segments, weights):
    highest = lax.Precision.HIGHEST
    qkv_weight, proj_weight, up_weight, down_weight, vector = weights
    bias_query, bias_value, bias_proj, gain_first, shift_first, bias_up, bias_down, gain_second, shift_second = split_vector(vector)
    groups, length = segments.shape
    bias_all = jnp.concatenate([bias_query, jnp.zeros_like(bias_query), bias_value])
    packed = jnp.einsum('gtd,de->gte', inputs, qkv_weight, precision=highest) + bias_all
    packed = low(low_back(packed)).reshape(groups, length, 3, HEADS, HEAD_DIM)
    queries = packed[:, :, 0]
    key_rows = packed[:, :, 1]
    values = packed[:, :, 2]
    scores = jnp.einsum('gqhd,gkhd->ghqk', queries, key_rows, precision=highest) * HEAD_DIM ** (-0.5)
    scores = low_back(scores)
    same_doc = segments[:, None, :, None] == segments[:, None, None, :]
    scores = jnp.where(same_doc, scores, MASK_FILL)
    probs = low(jax.nn.softmax(scores, axis=-1))
    attended = jnp.einsum('ghqk,gkhd->gqhd', probs, values, precision=highest).reshape(groups, length, D)
    attended = low(low_back(attended))
    branch = jnp.einsum('gtd,de->gte', attended, proj_weight, precision=highest) + bias_proj
    normed = layer_norm(inputs + low_back(branch), gain_first, shift_first)
    upward = jnp.einsum('gtd,de->gte', low(normed), up_weight, precision=highest) + bias_up
    activated = low(jax.nn.gelu(low_back(upward), approximate=False))
    downward = jnp.einsum('gtd,de->gte', activated, down_weight, precision=highest) + bias_down
    return layer_norm(normed + low_back(downward), gain_second, shift_second)

def unround(master):
    return lax.optimization_barrier(master.astype(jnp.bfloat16)).astype(jnp.float32)

def adam_update(master, moment_one, moment_two, grad, rate):
    one_new = BETA_FIRST * moment_one + (1.0 - BETA_FIRST) * grad
    two_new = BETA_SECOND * moment_two + (1.0 - BETA_SECOND) * grad * grad
    one_hat = one_new / (1.0 - BETA_FIRST ** STEP)
    two_hat = two_new / (1.0 - BETA_SECOND ** STEP)
    master_new = master - rate * (one_hat / (jnp.sqrt(two_hat) + ADAM_EPS) + WEIGHT_DECAY * master)
    return (grad, one_new, two_new, master_new, master_new.astype(jnp.bfloat16))

def reference(tokens, segment_ids, out_grad, qkv_master, qkv_first, qkv_second, proj_master, proj_first, proj_second, up_master, up_first, up_second, down_master, down_first, down_second, vector_master, vector_first, vector_second):
    masters = (qkv_master, proj_master, up_master, down_master, vector_master)
    matrix_shapes = ((D, 3 * D), (D, D), (D, FF), (FF, D), (VEC,))
    weights = tuple((unround(master).reshape(matrix_shape) for master, matrix_shape in zip(masters, matrix_shapes)))
    per_scan = 4
    blocks = SEQS // per_scan
    inputs = tokens.astype(jnp.float32).reshape(blocks, per_scan, LEN, D)
    segments = segment_ids.reshape(blocks, per_scan, LEN)
    cotangent = out_grad.astype(jnp.float32).reshape(blocks, per_scan, LEN, D)

    def advance(totals, block_data):
        block_in, block_seg, block_cot = block_data
        result, pullback = jax.vjp(lambda given_in, params: forward(given_in, block_seg, params), block_in, weights)
        input_part, weight_part = pullback(block_cot)
        totals = jax.tree.map(lambda earlier, latest: earlier + latest, totals, weight_part)
        return (totals, (result.astype(jnp.bfloat16), input_part.astype(jnp.bfloat16)))
    initial = jax.tree.map(jnp.zeros_like, weights)
    summed, (outputs, input_parts) = lax.scan(advance, initial, (inputs, segments, cotangent))
    layer_out = outputs.reshape(TOKENS, D)
    input_grad = input_parts.reshape(TOKENS, D)
    qkv_out = adam_update(qkv_master, qkv_first, qkv_second, summed[0].reshape(-1), RATES[0])
    proj_out = adam_update(proj_master, proj_first, proj_second, summed[1].reshape(-1), RATES[1])
    up_out = adam_update(up_master, up_first, up_second, summed[2].reshape(-1), RATES[2])
    down_out = adam_update(down_master, down_first, down_second, summed[3].reshape(-1), RATES[3])
    vector_out = adam_update(vector_master, vector_first, vector_second, summed[4].reshape(-1), RATES[4])
    return (layer_out, input_grad, qkv_out[0], qkv_out[1], qkv_out[2], qkv_out[3], qkv_out[4], proj_out[0], proj_out[1], proj_out[2], proj_out[3], proj_out[4], up_out[0], up_out[1], up_out[2], up_out[3], up_out[4], down_out[0], down_out[1], down_out[2], down_out[3], down_out[4], vector_out[0], vector_out[1], vector_out[2], vector_out[3], vector_out[4])
```

```python
import functools

import jax
import jax.numpy as jnp
from jax import lax
from jax.experimental import pallas as pl
from jax.experimental.pallas import tpu as pltpu
from jax.sharding import PartitionSpec as P

D = 1024
HEADS = 16
HEAD_DIM = 64
FF = 4096
STEP = 3
LANES = 128
PAIRS = HEADS * HEAD_DIM // LANES

NORM_EPS = 1e-05
BETA_FIRST = 0.5
BETA_SECOND = 0.5
ADAM_EPS = 1e-08
WEIGHT_DECAY = 0.01
MASK_FILL = -1000000000.0
RATES = (0.01, 0.03, 0.01, 0.005, 0.05)
SCALE = HEAD_DIM ** (-0.5)
HALF_ROOT = 0.7071067811865476
PDF_TOP = 0.3989422804014327

F32 = jnp.float32
BF16 = jnp.bfloat16
MESH = pl.DeviceIdType.MESH


def dot_over(left, right, left_dim, right_dim):
    return lax.dot_general(
        left, right, (((left_dim,), (right_dim,)), ((), ())), preferred_element_type=F32
    )


def depth_of(mesh):
    devices = list(mesh.devices.flat)
    if len(devices) % 8:
        return 0
    try:
        spots = [(*d.coords, d.core_on_chip) for d in devices]
    except AttributeError:
        return 0
    low = [min(s[i] for s in spots) for i in range(4)]
    depth = len(devices) // 8
    for index, (x, y, z, core) in enumerate(spots):
        spot = (((z - low[2]) * 2 + y - low[1]) * 2 + x - low[0]) * 2 + core - low[3]
        if spot != index:
            return 0
    return depth


class Place:
    def __init__(self, depth):
        me = lax.axis_index("dp")
        self.depth = depth
        self.core = me % 2
        self.x = (me // 2) % 2
        self.y = (me // 4) % 2
        self.z = me // 8

    def index(self, z, y, x, core):
        return ((z * 2 + y) * 2 + x) * 2 + core

    def ahead(self, k):
        return (self.z + k) % self.depth

    def back(self, k):
        return (self.z + self.depth - k) % self.depth

    def twin(self):
        return self.index(self.z, self.y, self.x, 1 - self.core)

    def x_mate(self):
        return self.index(self.z, self.y, 1 - self.x, self.core)

    def y_mate(self):
        return self.index(self.z, 1 - self.y, self.x, self.core)

    def z_mate(self, k):
        return self.index(self.ahead(k), self.y, self.x, self.core)

    def greet(self):
        barrier = pltpu.get_barrier_semaphore()
        mates = [self.twin(), self.x_mate(), self.y_mate()]
        mates += [self.z_mate(k) for k in range(1, self.depth)]
        for mate in mates:
            pl.semaphore_signal(barrier, inc=1, device_id=(mate,), device_id_type=MESH)
        pl.semaphore_wait(barrier, len(mates))


def send(source, target, send_sem, recv_sem, device):
    return pltpu.make_async_remote_copy(
        src_ref=source,
        dst_ref=target,
        send_sem=send_sem,
        recv_sem=recv_sem,
        device_id=(device,),
        device_id_type=MESH,
    )


class Gather:
    BY_Z, BY_X, BY_Y, UPPER, LOWER, OWN, FROM_X, FROM_Y, CROSS = range(9)

    def __init__(self, place, blocks, full, send_sems, recv_sems, local_sems):
        self.place = place
        self.blocks = blocks
        self.full = full
        self.sems = (send_sems, recv_sems)
        self.local_sems = local_sems
        self.depth = place.depth

    def home(self, w):
        p = self.place
        return self.full[w].at[p.z, p.y, p.x, p.core]

    def copy(self, w, k, kind):
        p, full = self.place, self.full[w]
        half = self.blocks[w].shape[0] // 2
        sems = [sem.at[w, k, kind] for sem in self.sems]
        zz = p.back(k)
        if kind == self.BY_Z:
            return send(self.blocks[w], self.home(w), *sems, p.z_mate(k))
        if kind in (self.BY_X, self.BY_Y, self.OWN):
            block = full.at[zz, p.y, p.x, p.core]
            source = self.blocks[w] if k == 0 else block
            mate = {self.BY_X: p.x_mate, self.BY_Y: p.y_mate, self.OWN: p.twin}[kind]()
            return send(source, block, *sems, mate)
        if kind == self.UPPER:
            block = full.at[zz, p.y, 1 - p.x, p.core, pl.ds(0, half)]
            return send(block, block, *sems, p.y_mate())
        if kind == self.LOWER:
            block = full.at[zz, 1 - p.y, p.x, p.core, pl.ds(half, half)]
            return send(block, block, *sems, p.x_mate())
        if kind == self.FROM_X:
            block = full.at[zz, p.y, 1 - p.x, p.core]
        elif kind == self.FROM_Y:
            block = full.at[zz, 1 - p.y, p.x, p.core]
        else:
            block = full.at[zz, 1 - p.y, 1 - p.x, p.core]
        return send(block, block, *sems, p.twin())

    def local(self, w):
        return pltpu.make_async_copy(self.blocks[w], self.home(w), self.local_sems.at[w])

    def start(self, w):
        for k in range(1, self.depth):
            self.copy(w, k, self.BY_Z).start()
        self.local(w).start()

    def spread(self, w, k):
        if k:
            self.copy(w, k, self.BY_Z).wait_recv()
        for kind in (self.BY_X, self.BY_Y, self.OWN):
            self.copy(w, k, kind).start()

    def relay(self, w, k):
        self.copy(w, k, self.BY_X).wait_recv()
        self.copy(w, k, self.UPPER).start()
        self.copy(w, k, self.FROM_X).start()
        self.copy(w, k, self.BY_Y).wait_recv()
        self.copy(w, k, self.LOWER).start()
        self.copy(w, k, self.FROM_Y).start()

    def hand_over(self, w, k):
        self.copy(w, k, self.UPPER).wait_recv()
        self.copy(w, k, self.LOWER).wait_recv()
        self.copy(w, k, self.CROSS).start()

    def finish(self, w):
        self.local(w).wait()
        for k in range(self.depth):
            for kind in (self.OWN, self.FROM_X, self.FROM_Y, self.CROSS):
                self.copy(w, k, kind).wait_recv()
            for kind in range(9):
                if kind != self.BY_Z or k:
                    self.copy(w, k, kind).wait_send()

    def step(self, units, t):
        lag = self.depth
        if t < len(units):
            self.spread(*units[t])
        if 0 <= t - lag < len(units):
            self.relay(*units[t - lag])
        if 0 <= t - 2 * lag < len(units):
            self.hand_over(*units[t - 2 * lag])

    def run(self):
        count = len(self.blocks)
        for w in range(count):
            self.start(w)
        units = [(w, k) for w in range(count) for k in range(self.depth)]
        for t in range(len(units) + 2 * self.depth):
            self.step(units, t)
        for w in range(count):
            self.finish(w)


def gather_kernel(depth, count, *refs):
    blocks, full, sems = refs[:count], refs[count : 2 * count], refs[2 * count :]
    place = Place(depth)
    place.greet()
    Gather(place, blocks, full, *sems).run()


def gather_sems(count, depth):
    return [
        pltpu.SemaphoreType.DMA((count, depth, 9)),
        pltpu.SemaphoreType.DMA((count, depth, 9)),
        pltpu.SemaphoreType.DMA((count,)),
    ]


def gather(blocks, depth, collective_id):
    count = len(blocks)
    return pl.pallas_call(
        functools.partial(gather_kernel, depth, count),
        in_specs=[pl.BlockSpec(memory_space=pltpu.VMEM)] * count,
        out_specs=[pl.BlockSpec(memory_space=pl.ANY)] * count,
        out_shape=[jax.ShapeDtypeStruct((depth, 2, 2, 2) + b.shape, b.dtype) for b in blocks],
        scratch_shapes=gather_sems(count, depth),
        compiler_params=pltpu.CompilerParams(
            collective_id=collective_id, has_side_effects=True
        ),
        name="gather",
    )(*blocks)


class Scatter:
    TWIN, UPPER_Y, LOWER_X, UPPER_X, LOWER_Y, BY_Z = range(6)

    def __init__(self, place, grads, out, bufs, send_sems, recv_sems, local_sems):
        self.place = place
        self.grads = grads
        self.out = out
        self.bufs = bufs
        self.sems = (send_sems, recv_sems)
        self.local_sems = local_sems
        self.depth = place.depth
        self.order = list(range(1, self.depth)) + [0]

    def load(self, w, k):
        p = self.place
        return pltpu.make_async_copy(
            self.grads[w].at[p.ahead(k), :, :, p.core],
            self.bufs[w][0].at[k],
            self.local_sems.at[w, k],
        )

    def copy(self, w, k, kind):
        p = self.place
        sums, twin, upper_y, lower_x, upper_x, lower_y, by_z = self.bufs[w]
        half = sums.shape[3] // 2
        sems = [sem.at[w, k, kind] for sem in self.sems]
        top, bottom = pl.ds(0, half), pl.ds(half, half)
        if kind == self.TWIN:
            source = self.grads[w].at[p.ahead(k), :, :, 1 - p.core]
            return send(source, twin.at[k], *sems, p.twin())
        if kind == self.UPPER_Y:
            return send(sums.at[k, 1 - p.y, :, top], upper_y.at[k], *sems, p.y_mate())
        if kind == self.LOWER_X:
            return send(sums.at[k, :, 1 - p.x, bottom], lower_x.at[k], *sems, p.x_mate())
        if kind == self.UPPER_X:
            return send(sums.at[k, p.y, 1 - p.x, top], upper_x.at[k], *sems, p.x_mate())
        if kind == self.LOWER_Y:
            return send(sums.at[k, 1 - p.y, p.x, bottom], lower_y.at[k], *sems, p.y_mate())
        return send(sums.at[k, p.y, p.x], by_z.at[k], *sems, p.z_mate(k))

    @staticmethod
    def add(target, extra):
        total = target[...].astype(F32) + extra[...].astype(F32)
        target[...] = total.astype(target.dtype)

    def start(self, w):
        for k in self.order:
            self.copy(w, k, self.TWIN).start()
            self.load(w, k).start()

    def first(self, w, k):
        sums, twin = self.bufs[w][:2]
        self.load(w, k).wait()
        self.copy(w, k, self.TWIN).wait_recv()

        def body(i, carry):
            self.add(sums.at[k, i // 2, i % 2], twin.at[k, i // 2, i % 2])
            return carry

        lax.fori_loop(0, 4, body, 0)
        self.copy(w, k, self.UPPER_Y).start()
        self.copy(w, k, self.LOWER_X).start()

    def second(self, w, k):
        p = self.place
        sums, _, upper_y, lower_x = self.bufs[w][:4]
        half = sums.shape[3] // 2
        self.copy(w, k, self.UPPER_Y).wait_recv()
        self.copy(w, k, self.LOWER_X).wait_recv()

        def body(i, carry):
            self.add(sums.at[k, p.y, i, pl.ds(0, half)], upper_y.at[k, i])
            self.add(sums.at[k, i, p.x, pl.ds(half, half)], lower_x.at[k, i])
            return carry

        lax.fori_loop(0, 2, body, 0)
        self.copy(w, k, self.UPPER_X).start()
        self.copy(w, k, self.LOWER_Y).start()

    def third(self, w, k):
        p = self.place
        sums, _, _, _, upper_x, lower_y, _ = self.bufs[w]
        half = sums.shape[3] // 2
        self.copy(w, k, self.UPPER_X).wait_recv()
        self.copy(w, k, self.LOWER_Y).wait_recv()
        self.add(sums.at[k, p.y, p.x, pl.ds(0, half)], upper_x.at[k])
        self.add(sums.at[k, p.y, p.x, pl.ds(half, half)], lower_y.at[k])
        if k:
            self.copy(w, k, self.BY_Z).start()

    def finish(self, w):
        p = self.place
        sums, by_z = self.bufs[w][0], self.bufs[w][6]
        for k in range(1, self.depth):
            self.copy(w, k, self.BY_Z).wait_recv()
        total = sums[0, p.y, p.x].astype(F32)
        for k in range(1, self.depth):
            total = total + by_z[k].astype(F32)
        self.out[w][...] = total
        for k in range(self.depth):
            for kind in range(6):
                if kind != self.BY_Z or k:
                    self.copy(w, k, kind).wait_send()

    def step(self, units, t):
        lag = self.depth
        if t < len(units):
            self.first(*units[t])
        if 0 <= t - lag < len(units):
            self.second(*units[t - lag])
        if 0 <= t - 2 * lag < len(units):
            self.third(*units[t - 2 * lag])

    def run(self):
        count = len(self.grads)
        for w in range(count):
            self.start(w)
        units = [(w, k) for w in range(count) for k in self.order]
        for t in range(len(units) + 2 * self.depth):
            self.step(units, t)
        for w in range(count):
            self.finish(w)


def scatter_scratch(grads, depth):
    scratch = []
    for grad in grads:
        rows, columns = grad.shape[-2:]
        half = rows // 2
        shapes = [(depth, 2, 2, rows, columns)] * 2
        shapes += [(depth, 2, half, columns)] * 2 + [(depth, half, columns)] * 2
        shapes += [(depth, rows, columns)]
        scratch += [pltpu.VMEM(shape, grad.dtype) for shape in shapes]
    count = len(grads)
    scratch += [pltpu.SemaphoreType.DMA((count, depth, 6))] * 2
    return scratch + [pltpu.SemaphoreType.DMA((count, depth))]


def scatter_kernel(depth, count, *refs):
    grads, out, rest = refs[:count], refs[count : 2 * count], refs[2 * count :]
    bufs = [rest[7 * w : 7 * w + 7] for w in range(count)]
    place = Place(depth)
    place.greet()
    Scatter(place, grads, out, bufs, *rest[7 * count :]).run()


def scatter(grads, depth, collective_id):
    count = len(grads)
    return pl.pallas_call(
        functools.partial(scatter_kernel, depth, count),
        in_specs=[pl.BlockSpec(memory_space=pl.ANY)] * count,
        out_specs=[pl.BlockSpec(memory_space=pltpu.VMEM)] * count,
        out_shape=[jax.ShapeDtypeStruct(g.shape[-2:], F32) for g in grads],
        scratch_shapes=scatter_scratch(grads, depth),
        compiler_params=pltpu.CompilerParams(
            collective_id=collective_id, has_side_effects=True, vmem_limit_bytes=60 << 20
        ),
        name="scatter",
    )(*grads)


def own_lanes(head):
    lane = lax.broadcasted_iota(jnp.int32, (1, LANES), 1)
    return (lane < HEAD_DIM) == (head == 0)


def mask_once(ids_row, ids_column, mask):
    @pl.when(pl.program_id(1) == 0)
    def _():
        mask[...] = jnp.where(ids_column[0] == ids_row[0], 0.0, MASK_FILL).astype(F32)


def attend_kernel(ids_row, ids_column, qkv, attended, log_total, mask):
    mask_once(ids_row, ids_column, mask)
    query = qkv[:, 0:LANES] * BF16(SCALE)
    key = qkv[:, LANES : 2 * LANES]
    value = qkv[:, 2 * LANES : 3 * LANES]
    length = query.shape[0]
    chunk = length // 2
    outs = []
    for head in range(2):
        own_key = jnp.where(own_lanes(head), key, BF16(0))
        parts = []
        for at in range(0, length, chunk):
            scores = dot_over(own_key, query[at : at + chunk], 1, 1) + mask[:, at : at + chunk]
            top = jnp.max(scores, axis=0, keepdims=True)
            weights = jnp.exp(scores - top)
            total = jnp.sum(weights, axis=0, keepdims=True)
            log_total[0, 0, head : head + 1, at : at + chunk] = top + jnp.log(total)
            probs = (weights * (1.0 / total)).astype(BF16)
            parts.append(dot_over(probs, value, 0, 0))
        outs.append(jnp.concatenate(parts, axis=0))
    attended[...] = jnp.where(own_lanes(0), outs[0], outs[1]).astype(BF16)


def attend_back_kernel(ids_row, ids_column, qkv, attended_grad, log_total, qkv_grad, mask):
    mask_once(ids_row, ids_column, mask)
    query = qkv[:, 0:LANES]
    key = qkv[:, LANES : 2 * LANES]
    value = qkv[:, 2 * LANES : 3 * LANES]
    grad = attended_grad[...]
    scaled = query * BF16(SCALE)
    length = query.shape[0]
    chunk = length // 2
    query_grads, key_grads, value_grads = [], [], []
    for head in range(2):
        own_key = jnp.where(own_lanes(head), key, BF16(0))
        own_value = jnp.where(own_lanes(head), value, BF16(0))
        key_grad = value_grad = None
        parts = []
        for at in range(0, length, chunk):
            piece = slice(at, at + chunk)
            scores = dot_over(own_key, scaled[piece], 1, 1) + mask[:, piece]
            probs = jnp.exp(scores - log_total[0, 0, head : head + 1, piece])
            prob_grad = dot_over(own_value, grad[piece], 1, 1)
            row_dot = jnp.sum(probs * prob_grad, axis=0, keepdims=True)
            score_grad = (probs * (prob_grad - row_dot)).astype(BF16)
            value_part = dot_over(probs.astype(BF16), grad[piece], 1, 0)
            key_part = dot_over(score_grad, query[piece], 1, 0)
            value_grad = value_part if value_grad is None else value_grad + value_part
            key_grad = key_part if key_grad is None else key_grad + key_part
            parts.append(dot_over(score_grad, key, 0, 0))
        query_grads.append(jnp.concatenate(parts, axis=0))
        key_grads.append(key_grad)
        value_grads.append(value_grad)
    first = own_lanes(0)
    qkv_grad[:, 0:LANES] = (jnp.where(first, *query_grads) * SCALE).astype(BF16)
    qkv_grad[:, LANES : 2 * LANES] = (jnp.where(first, *key_grads) * SCALE).astype(BF16)
    qkv_grad[:, 2 * LANES : 3 * LANES] = jnp.where(first, *value_grads).astype(BF16)


def attention_specs(length):
    ids_row = pl.BlockSpec((1, 1, length), lambda b, h: (b, 0, 0))
    ids_column = pl.BlockSpec((1, length, 1), lambda b, h: (b, 0, 0))
    qkv = pl.BlockSpec((length, 3 * LANES), lambda b, h: (b, h))
    one = pl.BlockSpec((length, LANES), lambda b, h: (b, h))
    log_total = pl.BlockSpec((1, 1, 2, length), lambda b, h: (b, h, 0, 0))
    return ids_row, ids_column, qkv, one, log_total


def attend(qkv, doc_ids):
    count, length = doc_ids.shape
    ids_row, ids_column, wide, one, log_total = attention_specs(length)
    return pl.pallas_call(
        attend_kernel,
        grid=(count, PAIRS),
        in_specs=[ids_row, ids_column, wide],
        out_specs=[one, log_total],
        out_shape=[
            jax.ShapeDtypeStruct((count * length, D), BF16),
            jax.ShapeDtypeStruct((count, PAIRS, 2, length), F32),
        ],
        scratch_shapes=[pltpu.VMEM((length, length), F32)],
        name="attend",
    )(doc_ids.reshape(count, 1, length), doc_ids.reshape(count, length, 1), qkv)


def attend_back(qkv, doc_ids, attended_grad, totals):
    count, length = doc_ids.shape
    ids_row, ids_column, wide, one, log_total = attention_specs(length)
    return pl.pallas_call(
        attend_back_kernel,
        grid=(count, PAIRS),
        in_specs=[ids_row, ids_column, wide, one, log_total],
        out_specs=wide,
        out_shape=jax.ShapeDtypeStruct((count * length, 3 * D), BF16),
        scratch_shapes=[pltpu.VMEM((length, length), F32)],
        name="attend_back",
    )(
        doc_ids.reshape(count, 1, length),
        doc_ids.reshape(count, length, 1),
        qkv,
        attended_grad,
        totals,
    )


def split_vector(vector):
    sizes = (D, D, D, D, D, FF, D, D, D)
    parts, at = [], 0
    for size in sizes:
        parts.append(vector[at : at + size])
        at += size
    return parts


def by_pair(columns):
    rows = columns.shape[0]
    return columns.reshape(rows, 3, PAIRS, LANES).swapaxes(1, 2).reshape(rows, 3 * D)


def by_kind(columns):
    rows = columns.shape[0]
    return columns.reshape(rows, PAIRS, 3, LANES).swapaxes(1, 2).reshape(rows, 3 * D)


def normalized(hidden):
    center = hidden - jnp.mean(hidden, axis=-1, keepdims=True)
    root = lax.rsqrt(jnp.mean(center * center, axis=-1, keepdims=True) + NORM_EPS)
    return center * root, root


def norm_back(grad, normed, root, gain):
    scaled = grad * gain
    mean = jnp.mean(scaled, axis=-1, keepdims=True)
    along = jnp.mean(scaled * normed, axis=-1, keepdims=True)
    return root * (scaled - mean - normed * along)


def column_sums(rows):
    return jnp.sum(rows.astype(F32), axis=0)


def times(rows, matrix):
    return jnp.dot(rows, matrix, preferred_element_type=F32)


def weight_grad(left_rows, right_rows, dtype):
    return dot_over(left_rows, right_rows, 0, 0).astype(dtype)


def back_product(grad_rows, matrix):
    return dot_over(grad_rows, matrix, 1, 1)


def layer_step(tokens, doc_ids, cotangent, weights, grad_type):
    qkv_weight, proj_weight, up_weight, down_weight, vector = weights
    (
        bias_query,
        bias_value,
        bias_proj,
        gain_first,
        shift_first,
        bias_up,
        bias_down,
        gain_second,
        shift_second,
    ) = split_vector(vector.astype(F32))
    bias_all = jnp.concatenate([bias_query, jnp.zeros_like(bias_query), bias_value])
    bias_all = by_pair(bias_all[None])[0]
    qkv = (times(tokens, qkv_weight) + bias_all).astype(BF16)
    attended, totals = attend(qkv, doc_ids)
    hidden = tokens.astype(F32) + times(attended, proj_weight) + bias_proj
    normed, root = normalized(hidden)
    branch = normed * gain_first + shift_first
    branch_low = branch.astype(BF16)
    upward = times(branch_low, up_weight) + bias_up
    cdf = 0.5 * (1.0 + lax.erf(upward * HALF_ROOT))
    activated = (upward * cdf).astype(BF16)
    slope = cdf + upward * (PDF_TOP * jnp.exp(-0.5 * upward * upward))
    second_in = branch + times(activated, down_weight) + bias_down
    second_normed, second_root = normalized(second_in)
    output = (second_normed * gain_second + shift_second).astype(BF16)

    cotangent = cotangent.astype(F32)
    gain_second_grad = column_sums(cotangent * second_normed)
    shift_second_grad = column_sums(cotangent)
    second_grad = norm_back(cotangent, second_normed, second_root, gain_second)
    down_rows = second_grad.astype(BF16)
    down_grad = weight_grad(activated, down_rows, grad_type)
    up_rows = (back_product(down_rows, down_weight) * slope).astype(BF16)
    up_grad = weight_grad(branch_low, up_rows, grad_type)
    branch_grad = back_product(up_rows, up_weight) + second_grad
    gain_first_grad = column_sums(branch_grad * normed)
    shift_first_grad = column_sums(branch_grad)
    hidden_grad = norm_back(branch_grad, normed, root, gain_first)
    proj_rows = hidden_grad.astype(BF16)
    proj_grad = weight_grad(attended, proj_rows, grad_type)
    attended_grad = back_product(proj_rows, proj_weight).astype(BF16)
    qkv_rows = attend_back(qkv, doc_ids, attended_grad, totals)
    qkv_grad = weight_grad(tokens, qkv_rows, grad_type)
    qkv_sums = by_kind(column_sums(qkv_rows)[None])[0]
    input_grad = (back_product(qkv_rows, qkv_weight) + hidden_grad).astype(BF16)
    vector_grad = jnp.concatenate(
        [
            qkv_sums[0:D],
            qkv_sums[2 * D : 3 * D],
            column_sums(proj_rows),
            gain_first_grad,
            shift_first_grad,
            column_sums(up_rows),
            column_sums(down_rows),
            gain_second_grad,
            shift_second_grad,
        ]
    )
    return output, input_grad, (qkv_grad, proj_grad, up_grad, down_grad, vector_grad)


def adam_update(master, moment_one, moment_two, grad, rate):
    one_new = BETA_FIRST * moment_one + (1.0 - BETA_FIRST) * grad
    two_new = BETA_SECOND * moment_two + (1.0 - BETA_SECOND) * grad * grad
    one_hat = one_new / (1.0 - BETA_FIRST**STEP)
    two_hat = two_new / (1.0 - BETA_SECOND**STEP)
    master_new = master - rate * (one_hat / (jnp.sqrt(two_hat) + ADAM_EPS) + WEIGHT_DECAY * master)
    return (grad, one_new, two_new, master_new, master_new.astype(BF16))


WIDTHS = (3 * D, D, FF, D)


def gather_weights(masters, devices, depth):
    lowered = [master.astype(BF16) for master in masters]
    blocks = [low.reshape(-1, width) for low, width in zip(lowered, WIDTHS)]
    blocks[0] = by_pair(blocks[0])
    if not depth:
        flat = [lax.all_gather(block, "dp", axis=0, tiled=True) for block in blocks]
        return (*flat, lax.all_gather(lowered[4], "dp", axis=0, tiled=True))
    rows = lowered[4].shape[0] // LANES
    vector = jnp.pad(lowered[4].reshape(rows, LANES), ((0, 32 - rows), (0, 0)))
    full = gather([vector, *blocks], depth, 1)
    matrices = [whole.reshape(-1, width) for whole, width in zip(full[1:], WIDTHS)]
    return (*matrices, full[0].reshape(devices, 32, LANES)[:, :rows].reshape(-1))


def scatter_grads(grads, devices, depth):
    if not depth:
        owned = [
            lax.psum_scatter(
                grad.reshape(devices, -1, grad.shape[-1]), "dp", scatter_dimension=0, tiled=True
            )[0]
            for grad in (*grads[:4], grads[4][None].reshape(-1, 1))
        ]
    else:
        rows = grads[4].shape[0] // devices // LANES
        vector = jnp.pad(grads[4].reshape(devices, rows, LANES), ((0, 0), (0, 16 - rows), (0, 0)))
        shape = (depth, 2, 2, 2)
        blocks = [grad.reshape(*shape, -1, grad.shape[-1]) for grad in grads[:4]]
        owned = scatter([*reversed(blocks), vector.reshape(*shape, 16, LANES)], depth, 2)
        owned = [*reversed(owned[:4]), owned[4][:rows]]
    owned[0] = by_kind(owned[0])
    return [own.reshape(-1) for own in owned]


def body(depth, tokens, segment_ids, out_grad, *states):
    devices = lax.axis_size("dp")
    masters = states[0::3]
    weights = gather_weights(masters, devices, depth)
    grad_type = BF16 if depth else F32
    output, input_grad, grads = layer_step(tokens, segment_ids, out_grad, weights, grad_type)
    owned = scatter_grads(grads, devices, depth)
    outs = [output, input_grad]
    for i in range(5):
        outs += adam_update(*states[3 * i : 3 * i + 3], owned[i], RATES[i])
    return tuple(outs)


def solution(mesh):
    rows = P("dp", None)
    flat = P("dp")
    return jax.shard_map(
        functools.partial(body, depth_of(mesh)),
        mesh=mesh,
        in_specs=(rows,) * 3 + (flat,) * 15,
        out_specs=(rows,) * 2 + (flat,) * 25,
        check_vma=False,
    )
```

```python
import functools

import jax
import jax.numpy as jnp
from jax import lax
from jax.experimental import pallas as pl
from jax.experimental.pallas import tpu as pltpu
from jax.sharding import PartitionSpec as P

D = 1024
HEADS = 16
HEAD_DIM = 64
FF = 4096
STEP = 3
LANES = 128
PAIRS = HEADS * HEAD_DIM // LANES

NORM_EPS = 1e-05
BETA_FIRST = 0.5
BETA_SECOND = 0.5
ADAM_EPS = 1e-08
WEIGHT_DECAY = 0.01
MASK_FILL = -1000000000.0
RATES = (0.01, 0.03, 0.01, 0.005, 0.05)
SCALE = HEAD_DIM ** (-0.5)
HALF_ROOT = 0.7071067811865476
PDF_TOP = 0.3989422804014327

F32 = jnp.float32
BF16 = jnp.bfloat16
MESH = pl.DeviceIdType.MESH


def dot_over(left, right, left_dim, right_dim):
    return lax.dot_general(
        left, right, (((left_dim,), (right_dim,)), ((), ())), preferred_element_type=F32
    )


def depth_of(mesh):
    devices = list(mesh.devices.flat)
    if len(devices) % 8:
        return 0
    try:
        spots = [(*d.coords, d.core_on_chip) for d in devices]
    except AttributeError:
        return 0
    low = [min(s[i] for s in spots) for i in range(4)]
    depth = len(devices) // 8
    for index, (x, y, z, core) in enumerate(spots):
        spot = (((z - low[2]) * 2 + y - low[1]) * 2 + x - low[0]) * 2 + core - low[3]
        if spot != index:
            return 0
    return depth


class Place:
    def __init__(self, depth):
        me = lax.axis_index("dp")
        self.depth = depth
        self.core = me % 2
        self.x = (me // 2) % 2
        self.y = (me // 4) % 2
        self.z = me // 8

    def index(self, z, y, x, core):
        return ((z * 2 + y) * 2 + x) * 2 + core

    def ahead(self, k):
        return (self.z + k) % self.depth

    def back(self, k):
        return (self.z + self.depth - k) % self.depth

    def twin(self):
        return self.index(self.z, self.y, self.x, 1 - self.core)

    def x_mate(self):
        return self.index(self.z, self.y, 1 - self.x, self.core)

    def y_mate(self):
        return self.index(self.z, 1 - self.y, self.x, self.core)

    def z_mate(self, k):
        return self.index(self.ahead(k), self.y, self.x, self.core)

    def greet(self):
        barrier = pltpu.get_barrier_semaphore()
        mates = [self.twin(), self.x_mate(), self.y_mate()]
        mates += [self.z_mate(k) for k in range(1, self.depth)]
        for mate in mates:
            pl.semaphore_signal(barrier, inc=1, device_id=(mate,), device_id_type=MESH)
        pl.semaphore_wait(barrier, len(mates))


def send(source, target, send_sem, recv_sem, device):
    return pltpu.make_async_remote_copy(
        src_ref=source,
        dst_ref=target,
        send_sem=send_sem,
        recv_sem=recv_sem,
        device_id=(device,),
        device_id_type=MESH,
    )


class Gather:
    BY_Z, BY_X, BY_Y, UPPER, LOWER, OWN, FROM_X, FROM_Y, CROSS = range(9)

    def __init__(self, place, blocks, full, send_sems, recv_sems, local_sems):
        self.place = place
        self.blocks = blocks
        self.full = full
        self.sems = (send_sems, recv_sems)
        self.local_sems = local_sems
        self.depth = place.depth

    def home(self, w):
        p = self.place
        return self.full[w].at[p.z, p.y, p.x, p.core]

    def copy(self, w, k, kind):
        p, full = self.place, self.full[w]
        half = self.blocks[w].shape[0] // 2
        sems = [sem.at[w, k, kind] for sem in self.sems]
        zz = p.back(k)
        if kind == self.BY_Z:
            return send(self.blocks[w], self.home(w), *sems, p.z_mate(k))
        if kind in (self.BY_X, self.BY_Y, self.OWN):
            block = full.at[zz, p.y, p.x, p.core]
            source = self.blocks[w] if k == 0 else block
            mate = {self.BY_X: p.x_mate, self.BY_Y: p.y_mate, self.OWN: p.twin}[kind]()
            return send(source, block, *sems, mate)
        if kind == self.UPPER:
            block = full.at[zz, p.y, 1 - p.x, p.core, pl.ds(0, half)]
            return send(block, block, *sems, p.y_mate())
        if kind == self.LOWER:
            block = full.at[zz, 1 - p.y, p.x, p.core, pl.ds(half, half)]
            return send(block, block, *sems, p.x_mate())
        if kind == self.FROM_X:
            block = full.at[zz, p.y, 1 - p.x, p.core]
        elif kind == self.FROM_Y:
            block = full.at[zz, 1 - p.y, p.x, p.core]
        else:
            block = full.at[zz, 1 - p.y, 1 - p.x, p.core]
        return send(block, block, *sems, p.twin())

    def local(self, w):
        return pltpu.make_async_copy(self.blocks[w], self.home(w), self.local_sems.at[w])

    def start(self, w):
        for k in range(1, self.depth):
            self.copy(w, k, self.BY_Z).start()
        self.local(w).start()

    def spread(self, w, k):
        if k:
            self.copy(w, k, self.BY_Z).wait_recv()
        for kind in (self.BY_X, self.BY_Y, self.OWN):
            self.copy(w, k, kind).start()

    def relay(self, w, k):
        self.copy(w, k, self.BY_X).wait_recv()
        self.copy(w, k, self.UPPER).start()
        self.copy(w, k, self.FROM_X).start()
        self.copy(w, k, self.BY_Y).wait_recv()
        self.copy(w, k, self.LOWER).start()
        self.copy(w, k, self.FROM_Y).start()

    def hand_over(self, w, k):
        self.copy(w, k, self.UPPER).wait_recv()
        self.copy(w, k, self.LOWER).wait_recv()
        self.copy(w, k, self.CROSS).start()

    def finish(self, w):
        self.local(w).wait()
        for k in range(self.depth):
            for kind in (self.OWN, self.FROM_X, self.FROM_Y, self.CROSS):
                self.copy(w, k, kind).wait_recv()
            for kind in range(9):
                if kind != self.BY_Z or k:
                    self.copy(w, k, kind).wait_send()

    def step(self, units, t):
        lag = self.depth
        if t < len(units):
            self.spread(*units[t])
        if 0 <= t - lag < len(units):
            self.relay(*units[t - lag])
        if 0 <= t - 2 * lag < len(units):
            self.hand_over(*units[t - 2 * lag])

    def units(self):
        return [(w, k) for w in range(len(self.blocks)) for k in range(self.depth)]

    def start_all(self):
        for w in range(len(self.blocks)):
            self.start(w)

    def finish_all(self):
        for w in range(len(self.blocks)):
            self.finish(w)

    def run(self):
        self.start_all()
        units = self.units()
        for t in range(len(units) + 2 * self.depth):
            self.step(units, t)
        self.finish_all()


def gather_kernel(depth, count, *refs):
    blocks, full, sems = refs[:count], refs[count : 2 * count], refs[2 * count :]
    place = Place(depth)
    place.greet()
    Gather(place, blocks, full, *sems).run()


def gather_sems(count, depth):
    return [
        pltpu.SemaphoreType.DMA((count, depth, 9)),
        pltpu.SemaphoreType.DMA((count, depth, 9)),
        pltpu.SemaphoreType.DMA((count,)),
    ]


def gather(blocks, depth, collective_id):
    count = len(blocks)
    return pl.pallas_call(
        functools.partial(gather_kernel, depth, count),
        in_specs=[pl.BlockSpec(memory_space=pltpu.VMEM)] * count,
        out_specs=[pl.BlockSpec(memory_space=pl.ANY)] * count,
        out_shape=[jax.ShapeDtypeStruct((depth, 2, 2, 2) + b.shape, b.dtype) for b in blocks],
        scratch_shapes=gather_sems(count, depth),
        compiler_params=pltpu.CompilerParams(
            collective_id=collective_id, has_side_effects=True
        ),
        name="gather",
    )(*blocks)


class Scatter:
    TWIN, UPPER_Y, LOWER_X, UPPER_X, LOWER_Y, BY_Z = range(6)

    def __init__(self, place, grads, out, bufs, send_sems, recv_sems, local_sems):
        self.place = place
        self.grads = grads
        self.out = out
        self.bufs = bufs
        self.sems = (send_sems, recv_sems)
        self.local_sems = local_sems
        self.depth = place.depth
        self.order = list(range(1, self.depth)) + [0]

    def load(self, w, k):
        p = self.place
        return pltpu.make_async_copy(
            self.grads[w].at[p.ahead(k), :, :, p.core],
            self.bufs[w][0].at[k],
            self.local_sems.at[w, k],
        )

    def copy(self, w, k, kind):
        p = self.place
        sums, twin, upper_y, lower_x, upper_x, lower_y, by_z = self.bufs[w]
        half = sums.shape[3] // 2
        sems = [sem.at[w, k, kind] for sem in self.sems]
        top, bottom = pl.ds(0, half), pl.ds(half, half)
        if kind == self.TWIN:
            source = self.grads[w].at[p.ahead(k), :, :, 1 - p.core]
            return send(source, twin.at[k], *sems, p.twin())
        if kind == self.UPPER_Y:
            return send(sums.at[k, 1 - p.y, :, top], upper_y.at[k], *sems, p.y_mate())
        if kind == self.LOWER_X:
            return send(sums.at[k, :, 1 - p.x, bottom], lower_x.at[k], *sems, p.x_mate())
        if kind == self.UPPER_X:
            return send(sums.at[k, p.y, 1 - p.x, top], upper_x.at[k], *sems, p.x_mate())
        if kind == self.LOWER_Y:
            return send(sums.at[k, 1 - p.y, p.x, bottom], lower_y.at[k], *sems, p.y_mate())
        return send(sums.at[k, p.y, p.x], by_z.at[k], *sems, p.z_mate(k))

    @staticmethod
    def add(target, extra):
        total = target[...].astype(F32) + extra[...].astype(F32)
        target[...] = total.astype(target.dtype)

    def start(self, w):
        for k in self.order:
            self.copy(w, k, self.TWIN).start()
            self.load(w, k).start()

    def first(self, w, k):
        sums, twin = self.bufs[w][:2]
        self.load(w, k).wait()
        self.copy(w, k, self.TWIN).wait_recv()

        def body(i, carry):
            self.add(sums.at[k, i // 2, i % 2], twin.at[k, i // 2, i % 2])
            return carry

        lax.fori_loop(0, 4, body, 0)
        self.copy(w, k, self.UPPER_Y).start()
        self.copy(w, k, self.LOWER_X).start()

    def second(self, w, k):
        p = self.place
        sums, _, upper_y, lower_x = self.bufs[w][:4]
        half = sums.shape[3] // 2
        self.copy(w, k, self.UPPER_Y).wait_recv()
        self.copy(w, k, self.LOWER_X).wait_recv()

        def body(i, carry):
            self.add(sums.at[k, p.y, i, pl.ds(0, half)], upper_y.at[k, i])
            self.add(sums.at[k, i, p.x, pl.ds(half, half)], lower_x.at[k, i])
            return carry

        lax.fori_loop(0, 2, body, 0)
        self.copy(w, k, self.UPPER_X).start()
        self.copy(w, k, self.LOWER_Y).start()

    def third(self, w, k):
        p = self.place
        sums, _, _, _, upper_x, lower_y, _ = self.bufs[w]
        half = sums.shape[3] // 2
        self.copy(w, k, self.UPPER_X).wait_recv()
        self.copy(w, k, self.LOWER_Y).wait_recv()
        self.add(sums.at[k, p.y, p.x, pl.ds(0, half)], upper_x.at[k])
        self.add(sums.at[k, p.y, p.x, pl.ds(half, half)], lower_y.at[k])
        if k:
            self.copy(w, k, self.BY_Z).start()

    def finish(self, w):
        p = self.place
        sums, by_z = self.bufs[w][0], self.bufs[w][6]
        for k in range(1, self.depth):
            self.copy(w, k, self.BY_Z).wait_recv()
        total = sums[0, p.y, p.x].astype(F32)
        for k in range(1, self.depth):
            total = total + by_z[k].astype(F32)
        self.out[w][...] = total
        for k in range(self.depth):
            for kind in range(6):
                if kind != self.BY_Z or k:
                    self.copy(w, k, kind).wait_send()

    def step(self, units, t):
        lag = self.depth
        if t < len(units):
            self.first(*units[t])
        if 0 <= t - lag < len(units):
            self.second(*units[t - lag])
        if 0 <= t - 2 * lag < len(units):
            self.third(*units[t - 2 * lag])

    def units(self):
        return [(w, k) for w in range(len(self.grads)) for k in self.order]

    def start_all(self):
        for w in range(len(self.grads)):
            self.start(w)

    def finish_all(self):
        for w in range(len(self.grads)):
            self.finish(w)

    def run(self):
        self.start_all()
        units = self.units()
        for t in range(len(units) + 2 * self.depth):
            self.step(units, t)
        self.finish_all()


def scatter_scratch(grads, depth):
    scratch = []
    for grad in grads:
        rows, columns = grad.shape[-2:]
        half = rows // 2
        shapes = [(depth, 2, 2, rows, columns)] * 2
        shapes += [(depth, 2, half, columns)] * 2 + [(depth, half, columns)] * 2
        shapes += [(depth, rows, columns)]
        scratch += [pltpu.VMEM(shape, grad.dtype) for shape in shapes]
    count = len(grads)
    scratch += [pltpu.SemaphoreType.DMA((count, depth, 6))] * 2
    return scratch + [pltpu.SemaphoreType.DMA((count, depth))]


def scatter_kernel(depth, count, *refs):
    grads, out, rest = refs[:count], refs[count : 2 * count], refs[2 * count :]
    bufs = [rest[7 * w : 7 * w + 7] for w in range(count)]
    place = Place(depth)
    place.greet()
    Scatter(place, grads, out, bufs, *rest[7 * count :]).run()


def scatter(grads, depth, collective_id):
    count = len(grads)
    return pl.pallas_call(
        functools.partial(scatter_kernel, depth, count),
        in_specs=[pl.BlockSpec(memory_space=pl.ANY)] * count,
        out_specs=[pl.BlockSpec(memory_space=pltpu.VMEM)] * count,
        out_shape=[jax.ShapeDtypeStruct(g.shape[-2:], F32) for g in grads],
        scratch_shapes=scatter_scratch(grads, depth),
        compiler_params=pltpu.CompilerParams(
            collective_id=collective_id, has_side_effects=True, vmem_limit_bytes=60 << 20
        ),
        name="scatter",
    )(*grads)


def own_lanes(head):
    lane = lax.broadcasted_iota(jnp.int32, (1, LANES), 1)
    return (lane < HEAD_DIM) == (head == 0)


def fill_masks(ids_row, ids_column, masks):
    for b in range(masks.shape[0]):
        masks[b] = jnp.where(ids_column[b] == ids_row[b], 0.0, MASK_FILL).astype(F32)


def at_step(t, work):
    pl.when(pl.program_id(0) * pl.num_programs(1) + pl.program_id(1) == t)(work)


def host(side, steps):
    units = side.units()
    count = len(units) + 2 * side.depth

    def open_up():
        side.place.greet()
        side.start_all()

    at_step(0, open_up)
    for t in range(min(count, steps - 1)):
        at_step(t, functools.partial(side.step, units, t))

    def rest():
        for t in range(steps - 1, count):
            side.step(units, t)
        side.finish_all()

    return lambda: at_step(steps - 1, rest)


def attend_kernel(depth, count, steps, *refs):
    ids_row, ids_column, tokens, weight, bias = refs[:5]
    blocks, refs = refs[5 : 5 + count], refs[5 + count :]
    qkv, attended, log_total = refs[:3]
    full, refs = refs[3 : 3 + count], refs[3 + count :]
    masks, sems = refs[0], refs[1:]
    finish = None
    if count:
        finish = host(Gather(Place(depth), blocks, full, *sems), steps)
    at_step(0, lambda: fill_masks(ids_row, ids_column, masks))
    b = pl.program_id(1)
    length = masks.shape[1]
    rows = tokens[pl.ds(pl.multiple_of(b * length, length), length), :]
    qkv[...] = (dot_over(rows, weight[...], 1, 0) + bias[0]).astype(BF16)
    query = qkv[:, 0:LANES] * BF16(SCALE)
    key = qkv[:, LANES : 2 * LANES]
    value = qkv[:, 2 * LANES : 3 * LANES]
    chunk = length // 2
    outs = []
    for head in range(2):
        own_key = jnp.where(own_lanes(head), key, BF16(0))
        parts = []
        for at in range(0, length, chunk):
            scores = dot_over(own_key, query[at : at + chunk], 1, 1)
            scores = scores + masks[b, :, at : at + chunk]
            top = jnp.max(scores, axis=0, keepdims=True)
            weights = jnp.exp(scores - top)
            total = jnp.sum(weights, axis=0, keepdims=True)
            log_total[0, 0, head : head + 1, at : at + chunk] = top + jnp.log(total)
            probs = (weights * (1.0 / total)).astype(BF16)
            parts.append(dot_over(probs, value, 0, 0))
        outs.append(jnp.concatenate(parts, axis=0))
    attended[...] = jnp.where(own_lanes(0), outs[0], outs[1]).astype(BF16)
    if finish:
        finish()


def attend_back_kernel(depth, count, steps, *refs):
    ids_row, ids_column, tokens, qkv, attended_grad, log_total = refs[:6]
    grads, refs = refs[6 : 6 + count], refs[6 + count :]
    qkv_grad, weight_grads, sums = refs[:3]
    out, refs = refs[3 : 3 + count], refs[3 + count :]
    masks, refs = refs[0], refs[1:]
    finish = None
    if count:
        bufs = [refs[7 * w : 7 * w + 7] for w in range(count)]
        finish = host(Scatter(Place(depth), grads, out, bufs, *refs[7 * count : -1]), steps)
    at_step(0, lambda: fill_masks(ids_row, ids_column, masks))
    b = pl.program_id(1)
    query = qkv[:, 0:LANES]
    key = qkv[:, LANES : 2 * LANES]
    value = qkv[:, 2 * LANES : 3 * LANES]
    grad = attended_grad[...]
    scaled = query * BF16(SCALE)
    length = query.shape[0]
    chunk = length // 2
    query_grads, key_grads, value_grads = [], [], []
    for head in range(2):
        own_key = jnp.where(own_lanes(head), key, BF16(0))
        own_value = jnp.where(own_lanes(head), value, BF16(0))
        key_grad = value_grad = None
        parts = []
        for at in range(0, length, chunk):
            piece = slice(at, at + chunk)
            scores = dot_over(own_key, scaled[piece], 1, 1) + masks[b, :, piece]
            probs = jnp.exp(scores - log_total[0, 0, head : head + 1, piece])
            prob_grad = dot_over(own_value, grad[piece], 1, 1)
            row_dot = jnp.sum(probs * prob_grad, axis=0, keepdims=True)
            score_grad = (probs * (prob_grad - row_dot)).astype(BF16)
            value_part = dot_over(probs.astype(BF16), grad[piece], 1, 0)
            key_part = dot_over(score_grad, query[piece], 1, 0)
            value_grad = value_part if value_grad is None else value_grad + value_part
            key_grad = key_part if key_grad is None else key_grad + key_part
            parts.append(dot_over(score_grad, key, 0, 0))
        query_grads.append(jnp.concatenate(parts, axis=0))
        key_grads.append(key_grad)
        value_grads.append(value_grad)
    first = own_lanes(0)
    qkv_grad[:, 0:LANES] = (jnp.where(first, *query_grads) * SCALE).astype(BF16)
    qkv_grad[:, LANES : 2 * LANES] = (jnp.where(first, *key_grads) * SCALE).astype(BF16)
    qkv_grad[:, 2 * LANES : 3 * LANES] = jnp.where(first, *value_grads).astype(BF16)
    rows = tokens[pl.ds(pl.multiple_of(b * length, length), length), :]
    rows_grad = qkv_grad[...]
    part = dot_over(rows, rows_grad, 0, 0)
    part_sums = jnp.sum(rows_grad.astype(F32), axis=0, keepdims=True)
    total = refs[-1]

    @pl.when(b == 0)
    def _():
        total[...] = part
        sums[0] = part_sums

    @pl.when(b > 0)
    def _():
        total[...] += part
        sums[0] += part_sums

    @pl.when(b == pl.num_programs(1) - 1)
    def _():
        weight_grads[...] = total[...].astype(weight_grads.dtype)

    if finish:
        finish()


def whole(shape):
    return pl.BlockSpec(shape, lambda h, b: (0,) * len(shape))


def attention_specs(count, length):
    rows = whole((count, 1, length))
    columns = whole((count, length, 1))
    tokens = whole((count * length, D))
    wide = pl.BlockSpec((length, 3 * LANES), lambda h, b: (b, h))
    one = pl.BlockSpec((length, LANES), lambda h, b: (b, h))
    log_total = pl.BlockSpec((1, 1, 2, length), lambda h, b: (b, h, 0, 0))
    weight = pl.BlockSpec((D, 3 * LANES), lambda h, b: (0, h))
    vector = pl.BlockSpec((1, 1, 3 * LANES), lambda h, b: (h, 0, 0))
    return rows, columns, tokens, wide, one, log_total, weight, vector


def kernel_params(collective_id, count):
    if not count:
        return pltpu.CompilerParams(vmem_limit_bytes=60 << 20)
    return pltpu.CompilerParams(
        collective_id=collective_id, has_side_effects=True, vmem_limit_bytes=60 << 20
    )


def attend(tokens, doc_ids, weight, bias, blocks, depth, collective_id):
    count, length = doc_ids.shape
    rows, columns, all_tokens, wide, one, log_total, part, vector = attention_specs(count, length)
    in_place = pl.BlockSpec(memory_space=pl.ANY)
    return pl.pallas_call(
        functools.partial(attend_kernel, depth, len(blocks), PAIRS * count),
        grid=(PAIRS, count),
        in_specs=[rows, columns, all_tokens, part, vector] + [whole(b.shape) for b in blocks],
        out_specs=[wide, one, log_total] + [in_place] * len(blocks),
        out_shape=[
            jax.ShapeDtypeStruct((count * length, 3 * D), BF16),
            jax.ShapeDtypeStruct((count * length, D), BF16),
            jax.ShapeDtypeStruct((count, PAIRS, 2, length), F32),
        ]
        + [jax.ShapeDtypeStruct((depth, 2, 2, 2) + b.shape, b.dtype) for b in blocks],
        scratch_shapes=[pltpu.VMEM((count, length, length), F32)]
        + (gather_sems(len(blocks), depth) if blocks else []),
        compiler_params=kernel_params(collective_id, len(blocks)),
        name="attend",
    )(
        doc_ids.reshape(count, 1, length),
        doc_ids.reshape(count, length, 1),
        tokens,
        weight,
        bias.reshape(PAIRS, 1, 3 * LANES),
        *blocks,
    )


def attend_back(tokens, qkv, doc_ids, attended_grad, totals, dtype, grads, depth, collective_id):
    count, length = doc_ids.shape
    rows, columns, all_tokens, wide, one, log_total, part, vector = attention_specs(count, length)
    in_place = pl.BlockSpec(memory_space=pl.ANY)
    blocks = [g.shape[-2:] for g in grads]
    return pl.pallas_call(
        functools.partial(attend_back_kernel, depth, len(grads), PAIRS * count),
        grid=(PAIRS, count),
        in_specs=[rows, columns, all_tokens, wide, one, log_total] + [in_place] * len(grads),
        out_specs=[wide, part, vector] + [whole(shape) for shape in blocks],
        out_shape=[
            jax.ShapeDtypeStruct((count * length, 3 * D), BF16),
            jax.ShapeDtypeStruct((D, 3 * D), dtype),
            jax.ShapeDtypeStruct((PAIRS, 1, 3 * LANES), F32),
        ]
        + [jax.ShapeDtypeStruct(shape, F32) for shape in blocks],
        scratch_shapes=[pltpu.VMEM((count, length, length), F32)]
        + (scatter_scratch(grads, depth) if grads else [])
        + [pltpu.VMEM((D, 3 * LANES), F32)],
        compiler_params=kernel_params(collective_id, len(grads)),
        name="attend_back",
    )(
        doc_ids.reshape(count, 1, length),
        doc_ids.reshape(count, length, 1),
        tokens,
        qkv,
        attended_grad,
        totals,
        *grads,
    )


def split_vector(vector):
    sizes = (D, D, D, D, D, FF, D, D, D)
    parts, at = [], 0
    for size in sizes:
        parts.append(vector[at : at + size])
        at += size
    return parts


def by_pair(columns):
    rows = columns.shape[0]
    return columns.reshape(rows, 3, PAIRS, LANES).swapaxes(1, 2).reshape(rows, 3 * D)


def by_kind(columns):
    rows = columns.shape[0]
    return columns.reshape(rows, PAIRS, 3, LANES).swapaxes(1, 2).reshape(rows, 3 * D)


def normalized(hidden):
    center = hidden - jnp.mean(hidden, axis=-1, keepdims=True)
    root = lax.rsqrt(jnp.mean(center * center, axis=-1, keepdims=True) + NORM_EPS)
    return center * root, root


def norm_back(grad, normed, root, gain):
    scaled = grad * gain
    mean = jnp.mean(scaled, axis=-1, keepdims=True)
    along = jnp.mean(scaled * normed, axis=-1, keepdims=True)
    return root * (scaled - mean - normed * along)


def column_sums(rows):
    return jnp.sum(rows.astype(F32), axis=0)


def times(rows, matrix):
    return jnp.dot(rows, matrix, preferred_element_type=F32)


def weight_grad(left_rows, right_rows, dtype):
    return dot_over(left_rows, right_rows, 0, 0).astype(dtype)


def back_product(grad_rows, matrix):
    return dot_over(grad_rows, matrix, 1, 1)


def layer_step(tokens, doc_ids, cotangent, masters, devices, depth):
    grad_type = BF16 if depth else F32
    shape = (depth, 2, 2, 2)
    blocks, low_vector = lowered_blocks(masters)
    if depth:
        rows = low_vector.shape[0] // LANES
        padded = jnp.pad(low_vector.reshape(rows, LANES), ((0, 32 - rows), (0, 0)))
        vectors, qkv_weight = gather([padded, blocks[0]], depth, 1)
        vector = vectors.reshape(devices, 32, LANES)[:, :rows].reshape(-1)
        qkv_weight = qkv_weight.reshape(D, 3 * D)
    else:
        weights = [lax.all_gather(b, "dp", axis=0, tiled=True) for b in blocks]
        qkv_weight, proj_weight, up_weight, down_weight = weights
        vector = lax.all_gather(low_vector, "dp", axis=0, tiled=True)
    (
        bias_query,
        bias_value,
        bias_proj,
        gain_first,
        shift_first,
        bias_up,
        bias_down,
        gain_second,
        shift_second,
    ) = split_vector(vector.astype(F32))
    bias_all = jnp.concatenate([bias_query, jnp.zeros_like(bias_query), bias_value])
    bias_all = by_pair(bias_all[None])[0]
    riders = blocks[1:] if depth else []
    qkv, attended, totals, *carried = attend(
        tokens, doc_ids, qkv_weight, bias_all, riders, depth, 2
    )
    if depth:
        proj_weight, up_weight, down_weight = [
            c.reshape(-1, width) for c, width in zip(carried, WIDTHS[1:])
        ]
    hidden = tokens.astype(F32) + times(attended, proj_weight) + bias_proj
    normed, root = normalized(hidden)
    branch = normed * gain_first + shift_first
    branch_low = branch.astype(BF16)
    upward = times(branch_low, up_weight) + bias_up
    cdf = 0.5 * (1.0 + lax.erf(upward * HALF_ROOT))
    activated = (upward * cdf).astype(BF16)
    slope = cdf + upward * (PDF_TOP * jnp.exp(-0.5 * upward * upward))
    second_in = branch + times(activated, down_weight) + bias_down
    second_normed, second_root = normalized(second_in)
    output = (second_normed * gain_second + shift_second).astype(BF16)

    cotangent = cotangent.astype(F32)
    gain_second_grad = column_sums(cotangent * second_normed)
    shift_second_grad = column_sums(cotangent)
    second_grad = norm_back(cotangent, second_normed, second_root, gain_second)
    down_rows = second_grad.astype(BF16)
    down_grad = weight_grad(activated, down_rows, grad_type)
    up_rows = (back_product(down_rows, down_weight) * slope).astype(BF16)
    up_grad = weight_grad(branch_low, up_rows, grad_type)
    branch_grad = back_product(up_rows, up_weight) + second_grad
    gain_first_grad = column_sums(branch_grad * normed)
    shift_first_grad = column_sums(branch_grad)
    hidden_grad = norm_back(branch_grad, normed, root, gain_first)
    proj_rows = hidden_grad.astype(BF16)
    proj_grad = weight_grad(attended, proj_rows, grad_type)
    attended_grad = back_product(proj_rows, proj_weight).astype(BF16)
    riders = [g.reshape(*shape, -1, g.shape[1]) for g in (down_grad, up_grad)] if depth else []
    qkv_rows, qkv_grad, qkv_sums, *summed = attend_back(
        tokens, qkv, doc_ids, attended_grad, totals, grad_type, riders, depth, 3
    )
    input_grad = (back_product(qkv_rows, qkv_weight) + hidden_grad).astype(BF16)
    qkv_sums = by_kind(qkv_sums.reshape(1, -1))[0]
    vector_grad = jnp.concatenate(
        [
            qkv_sums[0:D],
            qkv_sums[2 * D : 3 * D],
            column_sums(proj_rows),
            gain_first_grad,
            shift_first_grad,
            column_sums(up_rows),
            column_sums(down_rows),
            gain_second_grad,
            shift_second_grad,
        ]
    )
    if depth:
        padded = jnp.pad(vector_grad.reshape(devices, rows, LANES), ((0, 0), (0, 16 - rows), (0, 0)))
        last = [g.reshape(*shape, -1, g.shape[1]) for g in (qkv_grad, proj_grad)]
        owned = scatter([*last, padded.reshape(*shape, 16, LANES)], depth, 4)
        owned = [owned[0], owned[1], summed[1], summed[0], owned[2][:rows]]
    else:
        grads = (qkv_grad, proj_grad, up_grad, down_grad, vector_grad[:, None])
        owned = [
            lax.psum_scatter(
                grad.reshape(devices, -1, grad.shape[-1]), "dp", scatter_dimension=0, tiled=True
            )[0]
            for grad in grads
        ]
    owned[0] = by_kind(owned[0])
    return output, input_grad, [own.reshape(-1) for own in owned]


def adam_update(master, moment_one, moment_two, grad, rate):
    one_new = BETA_FIRST * moment_one + (1.0 - BETA_FIRST) * grad
    two_new = BETA_SECOND * moment_two + (1.0 - BETA_SECOND) * grad * grad
    one_hat = one_new / (1.0 - BETA_FIRST**STEP)
    two_hat = two_new / (1.0 - BETA_SECOND**STEP)
    master_new = master - rate * (one_hat / (jnp.sqrt(two_hat) + ADAM_EPS) + WEIGHT_DECAY * master)
    return (grad, one_new, two_new, master_new, master_new.astype(BF16))


WIDTHS = (3 * D, D, FF, D)


def lowered_blocks(masters):
    lowered = [master.astype(BF16) for master in masters]
    blocks = [low.reshape(-1, width) for low, width in zip(lowered, WIDTHS)]
    blocks[0] = by_pair(blocks[0])
    return blocks, lowered[4]


def body(depth, tokens, segment_ids, out_grad, *states):
    devices = lax.axis_size("dp")
    masters = states[0::3]
    output, input_grad, owned = layer_step(
        tokens, segment_ids, out_grad, masters, devices, depth
    )
    outs = [output, input_grad]
    for i in range(5):
        outs += adam_update(*states[3 * i : 3 * i + 3], owned[i], RATES[i])
    return tuple(outs)


def solution(mesh):
    rows = P("dp", None)
    flat = P("dp")
    return jax.shard_map(
        functools.partial(body, depth_of(mesh)),
        mesh=mesh,
        in_specs=(rows,) * 3 + (flat,) * 15,
        out_specs=(rows,) * 2 + (flat,) * 25,
        check_vma=False,
    )
```

```python
import functools

import jax
import jax.numpy as jnp
from jax import lax
from jax.experimental import pallas as pl
from jax.experimental.pallas import tpu as pltpu
from jax.sharding import PartitionSpec as P

D = 1024
HEADS = 16
HEAD_DIM = 64
FF = 4096
STEP = 3
LANES = 128
PAIRS = HEADS * HEAD_DIM // LANES

NORM_EPS = 1e-05
BETA_FIRST = 0.5
BETA_SECOND = 0.5
ADAM_EPS = 1e-08
WEIGHT_DECAY = 0.01
MASK_FILL = -1000000000.0
RATES = (0.01, 0.03, 0.01, 0.005, 0.05)
SCALE = HEAD_DIM ** (-0.5)
HALF_ROOT = 0.7071067811865476
PDF_TOP = 0.3989422804014327

F32 = jnp.float32
BF16 = jnp.bfloat16
MESH = pl.DeviceIdType.MESH


def dot_over(left, right, left_dim, right_dim):
    return lax.dot_general(
        left, right, (((left_dim,), (right_dim,)), ((), ())), preferred_element_type=F32
    )


def depth_of(mesh):
    devices = list(mesh.devices.flat)
    if len(devices) % 8:
        return 0
    try:
        spots = [(*d.coords, d.core_on_chip) for d in devices]
    except AttributeError:
        return 0
    low = [min(s[i] for s in spots) for i in range(4)]
    depth = len(devices) // 8
    for index, (x, y, z, core) in enumerate(spots):
        spot = (((z - low[2]) * 2 + y - low[1]) * 2 + x - low[0]) * 2 + core - low[3]
        if spot != index:
            return 0
    return depth


class Place:
    def __init__(self, depth):
        me = lax.axis_index("dp")
        self.depth = depth
        self.core = me % 2
        self.x = (me // 2) % 2
        self.y = (me // 4) % 2
        self.z = me // 8

    def index(self, z, y, x, core):
        return ((z * 2 + y) * 2 + x) * 2 + core

    def ahead(self, k):
        return (self.z + k) % self.depth

    def back(self, k):
        return (self.z + self.depth - k) % self.depth

    def twin(self):
        return self.index(self.z, self.y, self.x, 1 - self.core)

    def x_mate(self):
        return self.index(self.z, self.y, 1 - self.x, self.core)

    def y_mate(self):
        return self.index(self.z, 1 - self.y, self.x, self.core)

    def z_mate(self, k):
        return self.index(self.ahead(k), self.y, self.x, self.core)

    def greet(self):
        barrier = pltpu.get_barrier_semaphore()
        mates = [self.twin(), self.x_mate(), self.y_mate()]
        mates += [self.z_mate(k) for k in range(1, self.depth)]
        for mate in mates:
            pl.semaphore_signal(barrier, inc=1, device_id=(mate,), device_id_type=MESH)
        pl.semaphore_wait(barrier, len(mates))


def send(source, target, send_sem, recv_sem, device):
    return pltpu.make_async_remote_copy(
        src_ref=source,
        dst_ref=target,
        send_sem=send_sem,
        recv_sem=recv_sem,
        device_id=(device,),
        device_id_type=MESH,
    )


class Gather:
    BY_Z, BY_X, BY_Y, UPPER, LOWER, OWN, FROM_X, FROM_Y, CROSS = range(9)

    def __init__(self, place, blocks, full, send_sems, recv_sems, local_sems):
        self.place = place
        self.blocks = blocks
        self.full = full
        self.sems = (send_sems, recv_sems)
        self.local_sems = local_sems
        self.depth = place.depth

    def home(self, w):
        p = self.place
        return self.full[w].at[p.z, p.y, p.x, p.core]

    def copy(self, w, k, kind):
        p, full = self.place, self.full[w]
        half = self.blocks[w].shape[0] // 2
        sems = [sem.at[w, k, kind] for sem in self.sems]
        zz = p.back(k)
        if kind == self.BY_Z:
            return send(self.blocks[w], self.home(w), *sems, p.z_mate(k))
        if kind in (self.BY_X, self.BY_Y, self.OWN):
            block = full.at[zz, p.y, p.x, p.core]
            source = self.blocks[w] if k == 0 else block
            mate = {self.BY_X: p.x_mate, self.BY_Y: p.y_mate, self.OWN: p.twin}[kind]()
            return send(source, block, *sems, mate)
        if kind == self.UPPER:
            block = full.at[zz, p.y, 1 - p.x, p.core, pl.ds(0, half)]
            return send(block, block, *sems, p.y_mate())
        if kind == self.LOWER:
            block = full.at[zz, 1 - p.y, p.x, p.core, pl.ds(half, half)]
            return send(block, block, *sems, p.x_mate())
        if kind == self.FROM_X:
            block = full.at[zz, p.y, 1 - p.x, p.core]
        elif kind == self.FROM_Y:
            block = full.at[zz, 1 - p.y, p.x, p.core]
        else:
            block = full.at[zz, 1 - p.y, 1 - p.x, p.core]
        return send(block, block, *sems, p.twin())

    def local(self, w):
        return pltpu.make_async_copy(self.blocks[w], self.home(w), self.local_sems.at[w])

    def start(self, w):
        for k in range(1, self.depth):
            self.copy(w, k, self.BY_Z).start()
        self.local(w).start()

    def spread(self, w, k):
        if k:
            self.copy(w, k, self.BY_Z).wait_recv()
        for kind in (self.BY_X, self.BY_Y, self.OWN):
            self.copy(w, k, kind).start()

    def relay(self, w, k):
        self.copy(w, k, self.BY_X).wait_recv()
        self.copy(w, k, self.UPPER).start()
        self.copy(w, k, self.FROM_X).start()
        self.copy(w, k, self.BY_Y).wait_recv()
        self.copy(w, k, self.LOWER).start()
        self.copy(w, k, self.FROM_Y).start()

    def hand_over(self, w, k):
        self.copy(w, k, self.UPPER).wait_recv()
        self.copy(w, k, self.LOWER).wait_recv()
        self.copy(w, k, self.CROSS).start()

    def receive(self, w, k):
        if k == 0:
            self.local(w).wait()
        for kind in (self.OWN, self.FROM_X, self.FROM_Y, self.CROSS):
            self.copy(w, k, kind).wait_recv()

    def receive_all(self, w):
        for k in range(self.depth):
            self.receive(w, k)

    def sent(self, w):
        for k in range(self.depth):
            for kind in range(9):
                if kind != self.BY_Z or k:
                    self.copy(w, k, kind).wait_send()

    def sent_all(self):
        for w in range(len(self.blocks)):
            self.sent(w)

    def step(self, units, t):
        lag = self.depth
        if t < len(units):
            self.spread(*units[t])
        if 0 <= t - lag < len(units):
            self.relay(*units[t - lag])
        if 0 <= t - 2 * lag < len(units):
            self.hand_over(*units[t - 2 * lag])

    def units(self):
        return [(w, k) for w in range(len(self.blocks)) for k in range(self.depth)]

    def start_all(self):
        for w in range(len(self.blocks)):
            self.start(w)

def gather_sems(count, depth):
    return [
        pltpu.SemaphoreType.DMA((count, depth, 9)),
        pltpu.SemaphoreType.DMA((count, depth, 9)),
        pltpu.SemaphoreType.DMA((count,)),
    ]


class Scatter:
    TWIN, UPPER_Y, LOWER_X, UPPER_X, LOWER_Y, BY_Z = range(6)

    def __init__(self, place, grads, out, bufs, send_sems, recv_sems, local_sems, resident=()):
        self.place = place
        self.resident = resident
        self.grads = grads
        self.out = out
        self.bufs = bufs
        self.sems = (send_sems, recv_sems)
        self.local_sems = local_sems
        self.depth = place.depth
        self.order = list(range(1, self.depth)) + [0]

    def load(self, w, k):
        p = self.place
        return pltpu.make_async_copy(
            self.grads[w].at[p.ahead(k), :, :, p.core],
            self.bufs[w][6].at[k],
            self.local_sems.at[w, k],
        )

    def sums(self, w, k):
        if w in self.resident:
            return self.grads[w].at[self.place.ahead(k), :, :, self.place.core]
        return self.bufs[w][6].at[k]

    def half(self, w):
        return self.grads[w].shape[-2] // 2

    def copy(self, w, k, kind):
        p = self.place
        twin, upper_y, lower_x, upper_x, lower_y, by_z = self.bufs[w][:6]
        sums, half = self.sums(w, k), self.half(w)
        sems = [sem.at[w, k, kind] for sem in self.sems]
        top, bottom = pl.ds(0, half), pl.ds(half, half)
        if kind == self.TWIN:
            source = self.grads[w].at[p.ahead(k), :, :, 1 - p.core]
            return send(source, twin.at[k], *sems, p.twin())
        if kind == self.UPPER_Y:
            return send(sums.at[1 - p.y, :, top], upper_y.at[k], *sems, p.y_mate())
        if kind == self.LOWER_X:
            return send(sums.at[:, 1 - p.x, bottom], lower_x.at[k], *sems, p.x_mate())
        if kind == self.UPPER_X:
            return send(sums.at[p.y, 1 - p.x, top], upper_x.at[k], *sems, p.x_mate())
        if kind == self.LOWER_Y:
            return send(sums.at[1 - p.y, p.x, bottom], lower_y.at[k], *sems, p.y_mate())
        return send(sums.at[p.y, p.x], by_z.at[k], *sems, p.z_mate(k))

    @staticmethod
    def add(target, extra):
        total = target[...].astype(F32) + extra[...].astype(F32)
        target[...] = total.astype(target.dtype)

    def start(self, w):
        for k in self.order:
            self.begin(w, k)

    def begin(self, w, k):
        self.copy(w, k, self.TWIN).start()
        if w not in self.resident:
            self.load(w, k).start()

    def first(self, w, k):
        sums, twin = self.sums(w, k), self.bufs[w][0]
        if w not in self.resident:
            self.load(w, k).wait()
        self.copy(w, k, self.TWIN).wait_recv()

        def body(i, carry):
            self.add(sums.at[i // 2, i % 2], twin.at[k, i // 2, i % 2])
            return carry

        lax.fori_loop(0, 4, body, 0)
        self.copy(w, k, self.UPPER_Y).start()
        self.copy(w, k, self.LOWER_X).start()

    def second(self, w, k):
        p = self.place
        sums, half = self.sums(w, k), self.half(w)
        upper_y, lower_x = self.bufs[w][1:3]
        self.copy(w, k, self.UPPER_Y).wait_recv()
        self.copy(w, k, self.LOWER_X).wait_recv()

        def body(i, carry):
            self.add(sums.at[p.y, i, pl.ds(0, half)], upper_y.at[k, i])
            self.add(sums.at[i, p.x, pl.ds(half, half)], lower_x.at[k, i])
            return carry

        lax.fori_loop(0, 2, body, 0)
        self.copy(w, k, self.UPPER_X).start()
        self.copy(w, k, self.LOWER_Y).start()

    def third(self, w, k):
        p = self.place
        sums, half = self.sums(w, k), self.half(w)
        upper_x, lower_y = self.bufs[w][3:5]
        self.copy(w, k, self.UPPER_X).wait_recv()
        self.copy(w, k, self.LOWER_Y).wait_recv()
        self.add(sums.at[p.y, p.x, pl.ds(0, half)], upper_x.at[k])
        self.add(sums.at[p.y, p.x, pl.ds(half, half)], lower_y.at[k])
        if isinstance(k, int):
            if k:
                self.copy(w, k, self.BY_Z).start()
        else:
            pl.when(k != 0)(lambda: self.copy(w, k, self.BY_Z).start())

    def finish(self, w):
        p = self.place
        by_z = self.bufs[w][5]
        for k in range(1, self.depth):
            self.copy(w, k, self.BY_Z).wait_recv()
        total = self.sums(w, 0)[p.y, p.x].astype(F32)
        for k in range(1, self.depth):
            total = total + by_z[k].astype(F32)
        self.out[w][...] = total
        for k in range(self.depth):
            for kind in range(6):
                if kind != self.BY_Z or k:
                    self.copy(w, k, kind).wait_send()


BUFS = 7


def scatter_scratch(grads, depth, resident=()):
    scratch = []
    for w, grad in enumerate(grads):
        rows, columns = grad.shape[-2:]
        half = rows // 2
        shapes = [(depth, 2, 2, rows, columns)]
        shapes += [(depth, 2, half, columns)] * 2 + [(depth, half, columns)] * 2
        shapes += [(depth, rows, columns)]
        shapes += [(8, LANES) if w in resident else (depth, 2, 2, rows, columns)]
        scratch += [pltpu.VMEM(shape, grad.dtype) for shape in shapes]
    count = len(grads)
    scratch += [pltpu.SemaphoreType.DMA((count, depth, 6))] * 2
    return scratch + [pltpu.SemaphoreType.DMA((count, depth))]


def own_lanes(head):
    lane = lax.broadcasted_iota(jnp.int32, (1, LANES), 1)
    return (lane < HEAD_DIM) == (head == 0)


def fill_masks(ids_row, ids_column, masks):
    for b in range(masks.shape[0]):
        masks[b] = jnp.where(ids_column[b] == ids_row[b], 0.0, MASK_FILL).astype(F32)


def at_step(t, work):
    pl.when(pl.program_id(0) * pl.num_programs(1) + pl.program_id(1) == t)(work)


GROUPS = 4
GROUP_PAIRS = PAIRS // GROUPS
GROUP_WIDTH = 3 * LANES * GROUP_PAIRS


def rows_of(block):
    return block.reshape(-1, block.shape[-1])


def qkv_rows_of(rows, weight, h):
    columns = pl.ds(pl.multiple_of((h % GROUP_PAIRS) * 3 * LANES, 3 * LANES), 3 * LANES)
    if len(weight.shape) == 2:
        return dot_over(rows, weight[:, columns], 1, 0)
    return dot_over(rows, rows_of(weight[:, :, :, :, :, columns]), 1, 0)


def attend_kernel(depth, count, seqs, per, *refs):
    ids_row, ids_column, tokens = refs[:3]
    if depth:
        blocks, refs = refs[3 : 3 + count], refs[3 + count :]
        qkv, attended, log_total, whole_qkv, whole_vector = refs[:5]
        riders, refs = refs[5 : 5 + count - GROUPS], refs[5 + count - GROUPS :]
        masks, bias, groups, refs = refs[0], refs[1], refs[2 : 2 + GROUPS], refs[2 + GROUPS :]
        place = Place(depth)
        side = Gather(place, blocks, [*groups, *riders], *refs[:3])
        out_sems = refs[3]
        units = side.units()

        def out_copy(g):
            columns = pl.ds(0, GROUP_WIDTH)
            target = pl.ds(g * GROUP_WIDTH, GROUP_WIDTH)
            return pltpu.make_async_copy(
                groups[g].at[:, :, :, :, :, columns],
                whole_qkv.at[:, :, :, :, :, target],
                out_sems.at[g],
            )

        vector_copy = pltpu.make_async_copy(
            groups[0].at[:, :, :, :, :, pl.ds(GROUP_WIDTH, LANES)], whole_vector, out_sems.at[GROUPS]
        )

        def open_up():
            place.greet()
            side.start_all()
            for t in range(3 * depth):
                side.step(units, t)
            side.receive_all(0)
            out_copy(0).start()
            vector_copy.start()
            for r in range(2 * PAIRS):
                d, j = r // per, r % per
                spot = (d // 8, d // 4 % 2, d // 2 % 2, d % 2)
                row = groups[0][(*spot, slice(j, j + 1), slice(GROUP_WIDTH, GROUP_WIDTH + LANES))]
                bias[r] = row.astype(F32)

        at_step(0, open_up)
        steps = seqs * GROUP_PAIRS

        def each(work, w):
            for k in range(depth):
                work(w, k)

        def ready(g):
            side.receive_all(g)
            out_copy(g).start()

        steps = seqs * PAIRS
        plan = [[] for _ in range(steps)]

        def put(i, work, *what):
            plan[min(i, steps - 1)].append(functools.partial(work, *what))

        proj, up = GROUPS, GROUPS + 1
        put(1, each, side.spread, 3)
        put(2, each, side.hand_over, 1)
        put(2, each, side.relay, 2)
        put(3, each, side.spread, proj)
        put(steps // GROUPS, ready, 1)
        for k in range(depth):
            put(4 + k, side.spread, up, k)
        put(5, each, side.relay, 3)
        put(6, each, side.hand_over, 2)
        put(7, each, side.relay, proj)
        put(2 * steps // GROUPS, ready, 2)
        put(8, each, side.hand_over, 3)
        put(10, each, side.hand_over, proj)
        put(3 * steps // GROUPS, ready, 3)
        for k in range(depth):
            put(9 + 2 * k, side.relay, up, k)
        put(13, side.hand_over, up, 0)
        for i in range(1, steps):

            def more(i=i):
                for work in plan[i]:
                    work()

            if plan[i]:
                at_step(i, more)
    else:
        weight, bias, qkv, attended, log_total, masks = refs[3:]
    at_step(0, lambda: fill_masks(ids_row, ids_column, masks))
    h, b = pl.program_id(0), pl.program_id(1)
    length = masks.shape[1]
    rows = tokens[pl.ds(pl.multiple_of(b * length, length), length), :]
    if depth:
        shifts = [bias[h], jnp.zeros((1, LANES), F32), bias[PAIRS + h]]
        shift = jnp.concatenate(shifts, axis=1)
        for g in range(GROUPS):

            @pl.when(h // GROUP_PAIRS == g)
            def _():
                qkv[...] = (qkv_rows_of(rows, groups[g], h) + shift).astype(BF16)
    else:
        qkv[...] = (dot_over(rows, weight[...], 1, 0) + bias[0]).astype(BF16)
    query = qkv[:, 0:LANES] * BF16(SCALE)
    key = qkv[:, LANES : 2 * LANES]
    value = qkv[:, 2 * LANES : 3 * LANES]
    chunk = length // 2
    outs = []
    for head in range(2):
        own_key = jnp.where(own_lanes(head), key, BF16(0))
        parts = []
        for at in range(0, length, chunk):
            scores = dot_over(own_key, query[at : at + chunk], 1, 1)
            scores = scores + masks[b, :, at : at + chunk]
            top = jnp.max(scores, axis=0, keepdims=True)
            weights = jnp.exp(scores - top)
            total = jnp.sum(weights, axis=0, keepdims=True)
            log_total[0, 0, head : head + 1, at : at + chunk] = top + jnp.log(total)
            probs = (weights * (1.0 / total)).astype(BF16)
            parts.append(dot_over(probs, value, 0, 0))
        outs.append(jnp.concatenate(parts, axis=0))
    attended[...] = jnp.where(own_lanes(0), outs[0], outs[1]).astype(BF16)
    if depth:

        def close():
            for k in range(1, depth):
                side.hand_over(up, k)
            for w in range(GROUPS, count):
                side.receive_all(w)
            side.sent_all()
            vector_copy.wait()
            for g in range(GROUPS):
                out_copy(g).wait()

        at_step(seqs * PAIRS - 1, close)


def attend_back_kernel(depth, seqs, per_device, *refs):
    ids_row, ids_column, tokens, qkv, attended_grad, log_total, weight, hidden_grad = refs[:8]
    steps = seqs * PAIRS
    i = pl.program_id(0)
    last = pl.num_programs(0) - 1
    spot = jnp.minimum(i, steps - 1)
    h, b = spot // seqs, spot % seqs
    if depth:
        up_grad, proj_grad, vector_part, input_grad = refs[8:12]
        out, refs = refs[12 : 15 + GROUPS], refs[15 + GROUPS :]
        masks, kept, total, sums, vector, *refs = refs
        groups, refs = refs[:GROUPS], refs[GROUPS:]
        grads = [up_grad, proj_grad, *groups, vector]
        count = len(grads)
        bufs = [refs[BUFS * w : BUFS * w + BUFS] for w in range(count)]
        place = Place(depth)
        side = Scatter(place, grads, out, bufs, *refs[BUFS * count :], resident=range(2, count))
        plan = [[] for _ in range(steps + tokens.shape[0] // ROW_BLOCK)]

        def put(at, work, *what):
            plan[min(at, len(plan) - 1)].append(functools.partial(work, *what))

        def each(work, w):
            def body(k, carry):
                work(w, k)
                return carry

            lax.fori_loop(0, depth, body, 0)

        up, proj, vec = 0, 1, count - 1
        put(0, place.greet)
        put(0, side.start, up)
        put(0, side.start, proj)
        for n, k in enumerate(side.order):
            put(1 + 2 * n, side.first, up, k)
            put(4 + 2 * n + n // 2, side.second, up, k)
            put(7 + 2 * n + n // 2, side.third, up, k)
        put(2, each, side.first, proj)
        put(5, each, side.second, proj)
        put(8, each, side.third, proj)
        per = steps // GROUPS
        for g in range(GROUPS):
            at = per * (g + 1)
            put(at, each, side.begin, 2 + g)
            put(at + 1, each, side.first, 2 + g)
            put(at + min(4, GROUPS + 1 - g), each, side.second, 2 + g)
            put(at + min(7, GROUPS + 2 - g), each, side.third, 2 + g)
        rows_each = per_device

        def make_vector():
            vector[...] = vector_part[...]
            for r in range(2 * PAIRS):
                d, j = r // rows_each, r % rows_each
                source = 0 if r < PAIRS else 2 * LANES
                row = sums[r % PAIRS, :, source : source + LANES]
                vector[d // 8, d // 4 % 2, d // 2 % 2, d % 2, j : j + 1, :] = row

        put(steps, make_vector)
        put(steps + 1, each, side.begin, vec)
        put(steps + 2, each, side.first, vec)
        put(steps + 3, each, side.second, vec)
        for at, works in enumerate(plan):

            def run(works=works):
                for work in works:
                    work()

            if works:
                pl.when(i == at)(run)
    else:
        input_grad, weight_grads, sums, masks, kept, total = refs[8:]
    pl.when(i == 0)(lambda: fill_masks(ids_row, ids_column, masks))
    length = qkv.shape[0]
    chunk = length // 2
    wide = pl.ds(pl.multiple_of(h * 3 * LANES, 3 * LANES), 3 * LANES)
    tall = pl.ds(pl.multiple_of(b * length, length), length)

    @pl.when(i < steps)
    def _():
        query = qkv[:, 0:LANES]
        key = qkv[:, LANES : 2 * LANES]
        value = qkv[:, 2 * LANES : 3 * LANES]
        grad = attended_grad[...]
        scaled = query * BF16(SCALE)
        query_grads, key_grads, value_grads = [], [], []
        for head in range(2):
            own_key = jnp.where(own_lanes(head), key, BF16(0))
            own_value = jnp.where(own_lanes(head), value, BF16(0))
            key_grad = value_grad = None
            parts = []
            for at in range(0, length, chunk):
                piece = slice(at, at + chunk)
                scores = dot_over(own_key, scaled[piece], 1, 1) + masks[b, :, piece]
                probs = jnp.exp(scores - log_total[0, 0, head : head + 1, piece])
                prob_grad = dot_over(own_value, grad[piece], 1, 1)
                row_dot = jnp.sum(probs * prob_grad, axis=0, keepdims=True)
                score_grad = (probs * (prob_grad - row_dot)).astype(BF16)
                value_part = dot_over(probs.astype(BF16), grad[piece], 1, 0)
                key_part = dot_over(score_grad, query[piece], 1, 0)
                value_grad = value_part if value_grad is None else value_grad + value_part
                key_grad = key_part if key_grad is None else key_grad + key_part
                parts.append(dot_over(score_grad, key, 0, 0))
            query_grads.append(jnp.concatenate(parts, axis=0))
            key_grads.append(key_grad)
            value_grads.append(value_grad)
        first = own_lanes(0)
        own = [
            (jnp.where(first, *query_grads) * SCALE).astype(BF16),
            (jnp.where(first, *key_grads) * SCALE).astype(BF16),
            jnp.where(first, *value_grads).astype(BF16),
        ]
        rows_grad = jnp.concatenate(own, axis=1)
        kept[tall, wide] = rows_grad
        part = dot_over(tokens[tall, :], rows_grad, 0, 0)
        part_sums = jnp.sum(rows_grad.astype(F32), axis=0, keepdims=True)

        @pl.when(b == 0)
        def _():
            total[...] = part
            sums[h] = part_sums

        @pl.when(b > 0)
        def _():
            total[...] += part
            sums[h] += part_sums

        @pl.when(b == seqs - 1)
        def _():
            if depth:
                where = (h % GROUP_PAIRS) * 3 * LANES
                columns = pl.ds(pl.multiple_of(where, 3 * LANES), 3 * LANES)
                for g in range(GROUPS):

                    @pl.when(h // GROUP_PAIRS == g)
                    def _():
                        shape = groups[g].shape[:5] + (3 * LANES,)
                        groups[g][:, :, :, :, :, columns] = total[...].astype(BF16).reshape(shape)
            else:
                weight_grads[...] = total[...]

    @pl.when(i >= steps)
    def _():
        at = pl.multiple_of((i - steps) * ROW_BLOCK, ROW_BLOCK)
        back = dot_over(kept[pl.ds(at, ROW_BLOCK), :], weight[...], 1, 1)
        input_grad[...] = (back + hidden_grad[...]).astype(BF16)

    if depth:

        @pl.when(i == last)
        def _():
            each(side.third, vec)
            for w in range(count):
                side.finish(w)


def whole(shape):
    return pl.BlockSpec(shape, lambda h, b: (0,) * len(shape))


def attention_specs(count, length):
    rows = whole((count, 1, length))
    columns = whole((count, length, 1))
    tokens = whole((count * length, D))
    wide = pl.BlockSpec((length, 3 * LANES), lambda h, b: (b, h))
    one = pl.BlockSpec((length, LANES), lambda h, b: (b, h))
    log_total = pl.BlockSpec((1, 1, 2, length), lambda h, b: (b, h, 0, 0))
    weight = pl.BlockSpec((D, 3 * LANES), lambda h, b: (0, h))
    vector = pl.BlockSpec((1, 1, 3 * LANES), lambda h, b: (h, 0, 0))
    return rows, columns, tokens, wide, one, log_total, weight, vector


def kernel_params(collective_id, remote, limit=60 << 20):
    if not remote:
        return pltpu.CompilerParams(vmem_limit_bytes=limit)
    return pltpu.CompilerParams(
        collective_id=collective_id, has_side_effects=True, vmem_limit_bytes=limit
    )


def attend(tokens, doc_ids, weight, bias, blocks, per, depth, collective_id):
    count, length = doc_ids.shape
    rows, columns, all_tokens, wide, one, log_total, part, vector = attention_specs(count, length)
    in_place = pl.BlockSpec(memory_space=pl.ANY)
    out_shape = [
        jax.ShapeDtypeStruct((count * length, 3 * D), BF16),
        jax.ShapeDtypeStruct((count * length, D), BF16),
        jax.ShapeDtypeStruct((count, PAIRS, 2, length), F32),
    ]
    out_specs = [wide, one, log_total]
    in_specs = [rows, columns, all_tokens]
    scratch = [pltpu.VMEM((count, length, length), F32)]
    grid3 = (depth, 2, 2, 2)
    if depth:
        in_specs += [whole(b.shape) for b in blocks]
        tall = blocks[0].shape[0]
        shapes = [(*grid3, tall, 3 * D), (*grid3, tall, LANES)]
        shapes += [grid3 + b.shape for b in blocks[GROUPS:]]
        out_shape += [jax.ShapeDtypeStruct(shape, BF16) for shape in shapes]
        out_specs += [in_place] * len(shapes)
        scratch += [pltpu.VMEM((2 * PAIRS, 1, LANES), F32)]
        scratch += [pltpu.VMEM(grid3 + b.shape, BF16) for b in blocks[:GROUPS]]
        scratch += gather_sems(len(blocks), depth) + [pltpu.SemaphoreType.DMA((GROUPS + 1,))]
        operands = blocks
    else:
        in_specs += [part, vector]
        operands = [weight, bias.reshape(PAIRS, 1, 3 * LANES)]
    return pl.pallas_call(
        functools.partial(attend_kernel, depth, len(blocks), count, per),
        grid=(PAIRS, count),
        in_specs=in_specs,
        out_specs=out_specs,
        out_shape=out_shape,
        scratch_shapes=scratch,
        compiler_params=kernel_params(collective_id, len(blocks)),
        name="attend",
    )(
        doc_ids.reshape(count, 1, length),
        doc_ids.reshape(count, length, 1),
        tokens,
        *operands,
    )


def attend_back(
    tokens, qkv, doc_ids, attended_grad, totals, weight, hidden_grad, grads, per_device, depth, collective_id
):
    seqs, length = doc_ids.shape
    steps = seqs * PAIRS
    blocks = seqs * length // ROW_BLOCK

    def h(i):
        return jnp.minimum(i, steps - 1) // seqs

    def b(i):
        return jnp.minimum(i, steps - 1) % seqs

    def late(i):
        return jnp.maximum(i - steps, 0)

    def once(shape):
        return pl.BlockSpec(shape, lambda i: (0,) * len(shape), pipeline_mode=pl.Buffered(1))

    in_place = pl.BlockSpec(memory_space=pl.ANY)
    in_specs = [
        once((seqs, 1, length)),
        once((seqs, length, 1)),
        once((seqs * length, D)),
        pl.BlockSpec((length, 3 * LANES), lambda i: (b(i), h(i))),
        pl.BlockSpec((length, LANES), lambda i: (b(i), h(i))),
        pl.BlockSpec((1, 1, 2, length), lambda i: (b(i), h(i), 0, 0)),
        once((D, 3 * D)),
        pl.BlockSpec((ROW_BLOCK, D), lambda i: (late(i), 0)),
    ]
    out_specs = [pl.BlockSpec((ROW_BLOCK, D), lambda i: (late(i), 0))]
    out_shape = [jax.ShapeDtypeStruct((seqs * length, D), BF16)]
    scratch = [
        pltpu.VMEM((seqs, length, length), F32),
        pltpu.VMEM((seqs * length, 3 * D), BF16),
        pltpu.VMEM((D, 3 * LANES), F32),
    ]
    if depth:
        up_grad, proj_grad, vector = grads
        tall = up_grad.shape[-2]
        group = jax.ShapeDtypeStruct((depth, 2, 2, 2, tall, GROUP_WIDTH), BF16)
        moved = [up_grad, proj_grad, *([group] * GROUPS), vector]
        in_specs += [in_place, in_place, flat(vector.shape)]
        out_specs += [flat(m.shape[-2:]) for m in moved]
        out_shape += [jax.ShapeDtypeStruct(m.shape[-2:], F32) for m in moved]
        scratch += [pltpu.VMEM((PAIRS, 1, 3 * LANES), F32), pltpu.VMEM(vector.shape, F32)]
        scratch += [pltpu.VMEM(group.shape, BF16)] * GROUPS
        scratch += scatter_scratch(moved, depth, resident=range(2, len(moved)))
    else:
        out_specs += [
            pl.BlockSpec((D, 3 * LANES), lambda i: (0, h(i))),
            flat((PAIRS, 1, 3 * LANES)),
        ]
        out_shape += [
            jax.ShapeDtypeStruct((D, 3 * D), F32),
            jax.ShapeDtypeStruct((PAIRS, 1, 3 * LANES), F32),
        ]
    return pl.pallas_call(
        functools.partial(attend_back_kernel, depth, seqs, per_device),
        grid=(steps + blocks,),
        in_specs=in_specs,
        out_specs=out_specs,
        out_shape=out_shape,
        scratch_shapes=scratch,
        compiler_params=kernel_params(collective_id, depth, 63 << 20),
        name="attend_back",
    )(
        doc_ids.reshape(seqs, 1, length),
        doc_ids.reshape(seqs, length, 1),
        tokens,
        qkv,
        attended_grad,
        totals,
        weight,
        hidden_grad,
        *grads,
    )


TILE = 512
ROW_CHUNK = 256


def widen_kernel(depth, tiles, *refs):
    low, up_weight, up_bias, normed, scales, block = refs[:6]
    activated, slope, second_in, whole_down = refs[6:10]
    kept, down, out_sems, *sems = refs[10:]
    place = Place(depth)
    side = Gather(place, [block], [down], *sems)
    units = side.units()
    i = pl.program_id(0)
    per = tiles // depth

    def out_copy(k):
        zz = place.back(k)
        return pltpu.make_async_copy(down.at[zz], whole_down.at[zz], out_sems.at[k])

    def step_of(t, work):
        pl.when(i == t)(work)

    def open_up():
        place.greet()
        side.start_all()

    step_of(0, open_up)
    for t in range(tiles):
        step_of(t, functools.partial(side.step, units, t))

    @pl.when(i < tiles)
    def _():
        for at in range(0, low.shape[0], ROW_CHUNK):
            rows = slice(at, at + ROW_CHUNK)
            upward = dot_over(low[rows, :], up_weight[...], 1, 0) + up_bias[...]
            cdf = 0.5 * (1.0 + lax.erf(upward * HALF_ROOT))
            value = (upward * cdf).astype(BF16)
            activated[rows, :] = value
            kept[i, rows, :] = value
            slope[rows, :] = cdf + upward * (PDF_TOP * jnp.exp(-0.5 * upward * upward))

    for k in range(depth):

        def layer(k=k):
            if tiles + k < len(units) + 2 * depth:
                side.step(units, tiles + k)
            side.receive(0, k)
            out_copy(k).start()
            zz = place.back(k)
            for at in range(0, low.shape[0], ROW_CHUNK):
                rows = slice(at, at + ROW_CHUNK)
                if k == 0:
                    total = normed[rows, :] * scales[0:1, :] + scales[1:2, :] + scales[2:3, :]
                else:
                    total = second_in[rows, :]
                for n in range(per):
                    tile = kept[zz * per + n, rows, :]
                    weight = rows_of(down[zz, n * 2 // per : (n + 1) * 2 // per])
                    total = total + dot_over(tile, weight, 1, 0)
                second_in[rows, :] = total

        step_of(tiles + k, layer)

    def close():
        for t in range(tiles + depth, len(units) + 2 * depth):
            side.step(units, t)
        side.sent_all()
        for k in range(depth):
            out_copy(k).wait()

    step_of(tiles + depth - 1, close)


def flat(shape):
    return pl.BlockSpec(shape, lambda i: (0,) * len(shape))


def widen(low, up_weight, up_bias, normed, scales, block, depth, collective_id):
    count = low.shape[0]
    tiles = FF // TILE
    last = tiles - 1
    tile = pl.BlockSpec((count, TILE), lambda i: (0, jnp.minimum(i, last)))
    spread = (depth, 2, 2, 2) + block.shape
    return pl.pallas_call(
        functools.partial(widen_kernel, depth, tiles),
        grid=(tiles + depth,),
        in_specs=[
            flat(low.shape),
            pl.BlockSpec((D, TILE), lambda i: (0, jnp.minimum(i, last))),
            pl.BlockSpec((1, TILE), lambda i: (0, jnp.minimum(i, last))),
            flat(normed.shape),
            flat(scales.shape),
            flat(block.shape),
        ],
        out_specs=[tile, tile, flat((count, D)), pl.BlockSpec(memory_space=pl.ANY)],
        out_shape=[
            jax.ShapeDtypeStruct((count, FF), BF16),
            jax.ShapeDtypeStruct((count, FF), F32),
            jax.ShapeDtypeStruct((count, D), F32),
            jax.ShapeDtypeStruct(spread, BF16),
        ],
        scratch_shapes=[
            pltpu.VMEM((tiles, count, TILE), BF16),
            pltpu.VMEM(spread, BF16),
            pltpu.SemaphoreType.DMA((depth,)),
            *gather_sems(1, depth),
        ],
        compiler_params=kernel_params(collective_id, 1),
        name="widen",
    )(low, up_weight, up_bias[None], normed, scales, block)


def widen_back_kernel(depth, tiles, *refs):
    rows_grad, activated, slope, down_weight, low_turned, up_weight = refs[:6]
    up_grad, branch_grad, sums, down_out = refs[6:10]
    kept, down_grad, total, *rest = refs[10:]
    place = Place(depth)
    side = Scatter(place, [down_grad], [down_out], [rest[:BUFS]], *rest[BUFS:], resident=(0,))
    i = pl.program_id(0)
    per = tiles // depth

    def step_of(t, work):
        pl.when(i == t)(work)

    step_of(0, place.greet)
    for zz in range(depth):
        k = (zz + depth - place.z) % depth
        ready = (zz + 1) * per
        step_of(ready, functools.partial(side.begin, 0, k))
        step_of(ready + 1, functools.partial(side.first, 0, k))
        step_of(ready + 3, functools.partial(side.second, 0, k))
        step_of(ready + 5, functools.partial(side.third, 0, k))

    @pl.when(i < tiles)
    def _():
        for at in range(0, rows_grad.shape[0], ROW_CHUNK):
            rows = slice(at, at + ROW_CHUNK)
            back = dot_over(rows_grad[rows, :], down_weight[...], 1, 1)
            kept[i, rows, :] = (back * slope[rows, :]).astype(BF16)
        sums[0] = jnp.sum(kept[i].astype(F32), axis=0, keepdims=True)
        grad = dot_over(activated[...], rows_grad[...], 0, 0).astype(BF16)
        blocks = TILE // down_grad.shape[4]
        grad = grad.reshape(1, blocks // 4, 2, 2, down_grad.shape[4], D)[0]
        part = pl.ds((i % per) * (blocks // 4), blocks // 4)
        down_grad[i // per, part] = grad

    @pl.when(i >= tiles)
    def _():
        tile = kept[i - tiles]
        up_grad[...] = dot_over(low_turned[...], tile, 1, 0).astype(BF16)
        for at in range(0, rows_grad.shape[0], ROW_CHUNK):
            rows = slice(at, at + ROW_CHUNK)
            part = dot_over(tile[rows, :], up_weight[...], 1, 1)

            @pl.when(i == tiles)
            def _():
                total[rows, :] = part

            @pl.when(i > tiles)
            def _():
                total[rows, :] += part

    @pl.when(i == 2 * tiles - 1)
    def _():
        branch_grad[...] = total[...]
        side.finish(0)


def widen_back(rows_grad, activated, slope, down_weight, low_turned, up_weight, depth, collective_id):
    count = rows_grad.shape[0]
    tiles = FF // TILE
    last = tiles - 1

    def early(i):
        return jnp.minimum(i, last)

    def late(i):
        return jnp.maximum(i - tiles, 0)

    shares = 8 * depth
    spread = jax.ShapeDtypeStruct((depth, 2, 2, 2, FF // shares, D), BF16)
    return pl.pallas_call(
        functools.partial(widen_back_kernel, depth, tiles),
        grid=(2 * tiles,),
        in_specs=[
            flat(rows_grad.shape),
            pl.BlockSpec((count, TILE), lambda i: (0, early(i))),
            pl.BlockSpec((count, TILE), lambda i: (0, early(i))),
            pl.BlockSpec((TILE, D), lambda i: (early(i), 0)),
            flat(low_turned.shape),
            pl.BlockSpec((D, TILE), lambda i: (0, late(i))),
        ],
        out_specs=[
            pl.BlockSpec((D, TILE), lambda i: (0, late(i))),
            flat((count, D)),
            pl.BlockSpec((1, 1, TILE), lambda i: (early(i), 0, 0)),
            flat(spread.shape[-2:]),
        ],
        out_shape=[
            jax.ShapeDtypeStruct((D, FF), BF16),
            jax.ShapeDtypeStruct((count, D), F32),
            jax.ShapeDtypeStruct((tiles, 1, TILE), F32),
            jax.ShapeDtypeStruct(spread.shape[-2:], F32),
        ],
        scratch_shapes=[
            pltpu.VMEM((tiles, count, TILE), BF16),
            pltpu.VMEM(spread.shape, BF16),
            pltpu.VMEM((count, D), F32),
            *scatter_scratch([spread], depth, resident=(0,)),
        ],
        compiler_params=kernel_params(collective_id, 1),
        name="widen_back",
    )(rows_grad, activated, slope, down_weight, low_turned, up_weight)


ROW_BLOCK = 256


def mean_of(rows):
    return jnp.sum(rows, axis=-1, keepdims=True) * (1.0 / D)


def normalized(hidden):
    center = hidden - mean_of(hidden)
    root = lax.rsqrt(mean_of(center * center) + NORM_EPS)
    return center * root, root


def norm_back(grad, normed, root, gain):
    scaled = grad * gain
    return root * (scaled - mean_of(scaled) - normed * mean_of(scaled * normed))


def add_sums(sums, *rows):
    new = [jnp.sum(r.astype(F32), axis=0, keepdims=True) for r in rows]

    @pl.when(pl.program_id(0) == 0)
    def _():
        sums[...] = jnp.zeros_like(sums)

    for j, n in enumerate(new):
        sums[j : j + 1, :] += n


def project_kernel(attended, tokens, weight, scales, normed, root, low, turned):
    hidden = dot_over(attended[...], weight[...], 1, 0)
    hidden = tokens[...].astype(F32) + hidden + scales[0:1, :]
    normed[...], root[...] = normalized(hidden)
    branch = normed[...] * scales[1:2, :] + scales[2:3, :]
    low[...] = branch.astype(BF16)
    turned[...] = branch.T.astype(BF16)


def output_kernel(second_in, cotangent, scales, output, rows, grad, sums):
    normed, root = normalized(second_in[...])
    output[...] = (normed * scales[0:1, :] + scales[1:2, :]).astype(BF16)
    upstream = cotangent[...].astype(F32)
    grad[...] = norm_back(upstream, normed, root, scales[0:1, :])
    rows[...] = grad[...].astype(BF16)
    add_sums(sums, upstream * normed, upstream, rows[...])


def project_back_kernel(
    branch_grad, second_grad, normed, root, attended, weight, scales, grad, back, weight_grads, sums, total
):
    upstream = branch_grad[...] + second_grad[...]
    grad[...] = norm_back(upstream, normed[...], root[...], scales[0:1, :])
    rows = grad[...].astype(BF16)
    back[...] = dot_over(rows, weight[...], 1, 1).astype(BF16)
    add_sums(sums, upstream * normed[...], upstream, rows)
    part = dot_over(attended[...], rows, 0, 0)

    @pl.when(pl.program_id(0) == 0)
    def _():
        total[...] = part

    @pl.when(pl.program_id(0) > 0)
    def _():
        total[...] += part

    @pl.when(pl.program_id(0) == pl.num_programs(0) - 1)
    def _():
        weight_grads[...] = total[...].astype(weight_grads.dtype)


def row_block(width=D):
    return pl.BlockSpec((ROW_BLOCK, width), lambda i: (i, 0))


def row_call(kernel, count, in_specs, out_specs, outs, scratch=()):
    return pl.pallas_call(
        kernel,
        grid=(count // ROW_BLOCK,),
        in_specs=in_specs,
        out_specs=out_specs,
        out_shape=[jax.ShapeDtypeStruct(shape, dtype) for shape, dtype in outs],
        scratch_shapes=list(scratch),
        compiler_params=pltpu.CompilerParams(vmem_limit_bytes=60 << 20),
        name=kernel.__name__,
    )


SUMS = (8, D)


def project(attended, tokens, weight, scales):
    count = tokens.shape[0]
    block, matrix = row_block(), flat((D, D))
    turned = pl.BlockSpec((D, ROW_BLOCK), lambda i: (0, i))
    outs = [((count, D), F32), ((count, 1), F32), ((count, D), BF16), ((D, count), BF16)]
    return row_call(
        project_kernel,
        count,
        [block, block, matrix, flat(scales.shape)],
        [block, row_block(1), block, turned],
        outs,
    )(attended, tokens, weight, scales)


def output_and_grad(second_in, cotangent, scales):
    count = second_in.shape[0]
    block = row_block()
    shape = (count, D)
    return row_call(
        output_kernel,
        count,
        [block, block, flat(scales.shape)],
        [block, block, block, flat(SUMS)],
        [(shape, BF16), (shape, BF16), (shape, F32), (SUMS, F32)],
    )(second_in, cotangent, scales)


def project_back(branch_grad, second_grad, normed, root, attended, weight, scales, dtype):
    count = attended.shape[0]
    block, matrix = row_block(), flat((D, D))
    shape = (count, D)
    return row_call(
        project_back_kernel,
        count,
        [block, block, block, row_block(1), block, matrix, flat(scales.shape)],
        [block, block, matrix, flat(SUMS)],
        [(shape, F32), (shape, BF16), ((D, D), dtype), (SUMS, F32)],
        [pltpu.VMEM((D, D), F32)],
    )(branch_grad, second_grad, normed, root, attended, weight, scales)


def split_vector(vector):
    sizes = (D, D, D, D, D, FF, D, D, D)
    parts, at = [], 0
    for size in sizes:
        parts.append(vector[at : at + size])
        at += size
    return parts


def by_pair(columns):
    rows = columns.shape[0]
    return columns.reshape(rows, 3, PAIRS, LANES).swapaxes(1, 2).reshape(rows, 3 * D)


def by_kind(columns):
    rows = columns.shape[0]
    return columns.reshape(rows, PAIRS, 3, LANES).swapaxes(1, 2).reshape(rows, 3 * D)


def stacked(*vectors):
    return jnp.pad(jnp.stack(vectors), ((0, 8 - len(vectors)), (0, 0)))


def column_sums(rows):
    return jnp.sum(rows.astype(F32), axis=0)


def times(rows, matrix):
    return jnp.dot(rows, matrix, preferred_element_type=F32)


def weight_grad(left_rows, right_rows, dtype):
    return dot_over(left_rows, right_rows, 0, 0).astype(dtype)


def back_product(grad_rows, matrix):
    return dot_over(grad_rows, matrix, 1, 1)


def layer_step(tokens, doc_ids, cotangent, masters, devices, depth):
    grad_type = BF16 if depth else F32
    shape = (depth, 2, 2, 2)
    blocks, low_vector = lowered_blocks(masters)
    rows = low_vector.shape[0] // LANES
    if depth:
        tall = blocks[0].shape[0]
        padded = jnp.pad(low_vector.reshape(rows, LANES), ((0, tall - rows), (0, 0)))
        first = [blocks[0][:, g * GROUP_WIDTH : (g + 1) * GROUP_WIDTH] for g in range(GROUPS)]
        first[0] = jnp.concatenate([first[0], padded], axis=1)
        qkv, attended, totals, qkv_weight, vectors, proj_weight, up_weight = attend(
            tokens, doc_ids, None, None, first + blocks[1:3], rows, depth, 1
        )
        vector = vectors.reshape(devices, tall, LANES)[:, :rows].reshape(-1)
        qkv_weight, proj_weight, up_weight = map(rows_of, (qkv_weight, proj_weight, up_weight))
    else:
        weights = [lax.all_gather(b, "dp", axis=0, tiled=True) for b in blocks]
        qkv_weight, proj_weight, up_weight, down_weight = weights
        vector = lax.all_gather(low_vector, "dp", axis=0, tiled=True)
    (
        bias_query,
        bias_value,
        bias_proj,
        gain_first,
        shift_first,
        bias_up,
        bias_down,
        gain_second,
        shift_second,
    ) = split_vector(vector.astype(F32))
    if not depth:
        bias_all = jnp.concatenate([bias_query, jnp.zeros_like(bias_query), bias_value])
        bias_all = by_pair(bias_all[None])[0]
        qkv, attended, totals = attend(tokens, doc_ids, qkv_weight, bias_all, [], 0, 0, 0)
    normed, root, branch_low, low_turned = project(
        attended, tokens, proj_weight, stacked(bias_proj, gain_first, shift_first)
    )
    if depth:
        activated, slope, second_in, down_weight = widen(
            branch_low,
            up_weight,
            bias_up,
            normed,
            stacked(gain_first, shift_first, bias_down),
            blocks[3],
            depth,
            2,
        )
        down_weight = rows_of(down_weight)
    else:
        upward = times(branch_low, up_weight) + bias_up
        cdf = 0.5 * (1.0 + lax.erf(upward * HALF_ROOT))
        activated = (upward * cdf).astype(BF16)
        slope = cdf + upward * (PDF_TOP * jnp.exp(-0.5 * upward * upward))
        branch = normed * gain_first + shift_first
        second_in = branch + times(activated, down_weight) + bias_down
    output, down_rows, second_grad, second_sums = output_and_grad(
        second_in, cotangent, stacked(gain_second, shift_second)
    )
    if depth:
        up_grad, branch_grad, bias_up_grad, down_owned = widen_back(
            down_rows, activated, slope, down_weight, low_turned, up_weight, depth, 3
        )
        bias_up_grad = bias_up_grad.reshape(-1)
    else:
        down_grad = weight_grad(activated, down_rows, F32)
        up_rows = (back_product(down_rows, down_weight) * slope).astype(BF16)
        bias_up_grad = column_sums(up_rows)
        up_grad = weight_grad(branch_low, up_rows, F32)
        branch_grad = back_product(up_rows, up_weight)
    hidden_grad, attended_grad, proj_grad, first_sums = project_back(
        branch_grad,
        second_grad,
        normed,
        root,
        attended,
        proj_weight,
        stacked(gain_first),
        grad_type,
    )
    known = [
        first_sums[2],
        first_sums[0],
        first_sums[1],
        bias_up_grad,
        second_sums[2],
        second_sums[0],
        second_sums[1],
    ]
    riders = []
    if depth:
        vector_part = jnp.concatenate([jnp.zeros((2 * D,), F32), *known])
        vector_part = vector_part.reshape(devices, rows, LANES)
        vector_part = jnp.pad(vector_part, ((0, 0), (0, 16 - rows), (0, 0)))
        riders = [g.reshape(*shape, -1, g.shape[1]) for g in (up_grad, proj_grad)]
        riders += [vector_part.reshape(*shape, 16, LANES)]
    input_grad, *summed = attend_back(
        tokens,
        qkv,
        doc_ids,
        attended_grad,
        totals,
        qkv_weight,
        hidden_grad,
        riders,
        rows,
        depth,
        4,
    )
    if depth:
        up_owned, proj_owned, *qkv_owned, vector_owned = summed
        owned = [jnp.concatenate(qkv_owned, axis=1), proj_owned, up_owned, down_owned]
        owned += [vector_owned[:rows]]
    else:
        qkv_grad, qkv_sums = summed
        qkv_sums = by_kind(qkv_sums.reshape(1, -1))[0]
        vector_grad = jnp.concatenate([qkv_sums[0:D], qkv_sums[2 * D : 3 * D], *known])
        grads = (qkv_grad, proj_grad, up_grad, down_grad, vector_grad[:, None])
        owned = [
            lax.psum_scatter(
                grad.reshape(devices, -1, grad.shape[-1]), "dp", scatter_dimension=0, tiled=True
            )[0]
            for grad in grads
        ]
    owned[0] = by_kind(owned[0])
    return output, input_grad, [own.reshape(-1) for own in owned]


def adam_update(master, moment_one, moment_two, grad, rate):
    one_new = BETA_FIRST * moment_one + (1.0 - BETA_FIRST) * grad
    two_new = BETA_SECOND * moment_two + (1.0 - BETA_SECOND) * grad * grad
    one_hat = one_new / (1.0 - BETA_FIRST**STEP)
    two_hat = two_new / (1.0 - BETA_SECOND**STEP)
    master_new = master - rate * (one_hat / (jnp.sqrt(two_hat) + ADAM_EPS) + WEIGHT_DECAY * master)
    return (grad, one_new, two_new, master_new, master_new.astype(BF16))


WIDTHS = (3 * D, D, FF, D)


def lowered_blocks(masters):
    lowered = [master.astype(BF16) for master in masters]
    blocks = [low.reshape(-1, width) for low, width in zip(lowered, WIDTHS)]
    blocks[0] = by_pair(blocks[0])
    return blocks, lowered[4]


def body(depth, tokens, segment_ids, out_grad, *states):
    devices = lax.axis_size("dp")
    masters = states[0::3]
    output, input_grad, owned = layer_step(
        tokens, segment_ids, out_grad, masters, devices, depth
    )
    outs = [output, input_grad]
    for i in range(5):
        outs += adam_update(*states[3 * i : 3 * i + 3], owned[i], RATES[i])
    return tuple(outs)


def solution(mesh):
    rows = P("dp", None)
    flat = P("dp")
    return jax.shard_map(
        functools.partial(body, depth_of(mesh)),
        mesh=mesh,
        in_specs=(rows,) * 3 + (flat,) * 15,
        out_specs=(rows,) * 2 + (flat,) * 25,
        check_vma=False,
    )
```

```python
import functools

import jax
import jax.numpy as jnp
from jax import lax
from jax.experimental import pallas as pl
from jax.experimental.pallas import tpu as pltpu
from jax.sharding import PartitionSpec as P

D = 1024
HEADS = 16
HEAD_DIM = 64
FF = 4096
STEP = 3
LANES = 128
PAIRS = HEADS * HEAD_DIM // LANES

NORM_EPS = 1e-05
BETA_FIRST = 0.5
BETA_SECOND = 0.5
ADAM_EPS = 1e-08
WEIGHT_DECAY = 0.01
MASK_FILL = -1000000000.0
RATES = (0.01, 0.03, 0.01, 0.005, 0.05)
SCALE = HEAD_DIM ** (-0.5)
HALF_ROOT = 0.7071067811865476
PDF_TOP = 0.3989422804014327

F32 = jnp.float32
BF16 = jnp.bfloat16
MESH = pl.DeviceIdType.MESH


def dot_over(left, right, left_dim, right_dim):
    return lax.dot_general(
        left, right, (((left_dim,), (right_dim,)), ((), ())), preferred_element_type=F32
    )


PLANNED_DEPTH = 4


def depth_of(mesh):
    devices = list(mesh.devices.flat)
    if len(devices) % 8:
        return 0
    try:
        spots = [(*d.coords, d.core_on_chip) for d in devices]
    except AttributeError:
        return 0
    low = [min(s[i] for s in spots) for i in range(4)]
    depth = len(devices) // 8
    if depth != PLANNED_DEPTH:
        return 0
    for index, (x, y, z, core) in enumerate(spots):
        spot = (((z - low[2]) * 2 + y - low[1]) * 2 + x - low[0]) * 2 + core - low[3]
        if spot != index:
            return 0
    return depth


class Place:
    def __init__(self, depth):
        me = lax.axis_index("dp")
        self.depth = depth
        self.core = me % 2
        self.x = (me // 2) % 2
        self.y = (me // 4) % 2
        self.z = me // 8

    def index(self, z, y, x, core):
        return ((z * 2 + y) * 2 + x) * 2 + core

    def ahead(self, k):
        return (self.z + k) % self.depth

    def back(self, k):
        return (self.z + self.depth - k) % self.depth

    def twin(self):
        return self.index(self.z, self.y, self.x, 1 - self.core)

    def x_mate(self):
        return self.index(self.z, self.y, 1 - self.x, self.core)

    def y_mate(self):
        return self.index(self.z, 1 - self.y, self.x, self.core)

    def z_mate(self, k):
        return self.index(self.ahead(k), self.y, self.x, self.core)

    def greet(self):
        barrier = pltpu.get_barrier_semaphore()
        mates = [self.twin(), self.x_mate(), self.y_mate()]
        mates += [self.z_mate(k) for k in range(1, self.depth)]
        for mate in mates:
            pl.semaphore_signal(barrier, inc=1, device_id=(mate,), device_id_type=MESH)
        pl.semaphore_wait(barrier, len(mates))


def send(source, target, send_sem, recv_sem, device):
    return pltpu.make_async_remote_copy(
        src_ref=source,
        dst_ref=target,
        send_sem=send_sem,
        recv_sem=recv_sem,
        device_id=(device,),
        device_id_type=MESH,
    )


class Gather:
    BY_Z, BY_X, BY_Y, UPPER, LOWER, OWN, FROM_X, FROM_Y, CROSS = range(9)

    def __init__(self, place, blocks, full, send_sems, recv_sems, local_sems):
        self.place = place
        self.blocks = blocks
        self.full = full
        self.sems = (send_sems, recv_sems)
        self.local_sems = local_sems
        self.depth = place.depth

    def home(self, w):
        p = self.place
        return self.full[w].at[p.z, p.y, p.x, p.core]

    def copy(self, w, k, kind):
        p, full = self.place, self.full[w]
        half = self.blocks[w].shape[0] // 2
        sems = [sem.at[w, k, kind] for sem in self.sems]
        zz = p.back(k)
        if kind == self.BY_Z:
            return send(self.blocks[w], self.home(w), *sems, p.z_mate(k))
        if kind in (self.BY_X, self.BY_Y, self.OWN):
            block = full.at[zz, p.y, p.x, p.core]
            source = self.blocks[w] if k == 0 else block
            mate = {self.BY_X: p.x_mate, self.BY_Y: p.y_mate, self.OWN: p.twin}[kind]()
            return send(source, block, *sems, mate)
        if kind == self.UPPER:
            block = full.at[zz, p.y, 1 - p.x, p.core, pl.ds(0, half)]
            return send(block, block, *sems, p.y_mate())
        if kind == self.LOWER:
            block = full.at[zz, 1 - p.y, p.x, p.core, pl.ds(half, half)]
            return send(block, block, *sems, p.x_mate())
        if kind == self.FROM_X:
            block = full.at[zz, p.y, 1 - p.x, p.core]
        elif kind == self.FROM_Y:
            block = full.at[zz, 1 - p.y, p.x, p.core]
        else:
            block = full.at[zz, 1 - p.y, 1 - p.x, p.core]
        return send(block, block, *sems, p.twin())

    def local(self, w):
        return pltpu.make_async_copy(self.blocks[w], self.home(w), self.local_sems.at[w])

    def start(self, w):
        for k in range(1, self.depth):
            self.copy(w, k, self.BY_Z).start()
        self.local(w).start()

    def spread(self, w, k):
        if k:
            self.copy(w, k, self.BY_Z).wait_recv()
        for kind in (self.BY_X, self.BY_Y, self.OWN):
            self.copy(w, k, kind).start()

    def relay(self, w, k):
        self.copy(w, k, self.BY_X).wait_recv()
        self.copy(w, k, self.UPPER).start()
        self.copy(w, k, self.FROM_X).start()
        self.copy(w, k, self.BY_Y).wait_recv()
        self.copy(w, k, self.LOWER).start()
        self.copy(w, k, self.FROM_Y).start()

    def hand_over(self, w, k):
        self.copy(w, k, self.UPPER).wait_recv()
        self.copy(w, k, self.LOWER).wait_recv()
        self.copy(w, k, self.CROSS).start()

    def receive(self, w, k):
        if k == 0:
            self.local(w).wait()
        for kind in (self.OWN, self.FROM_X, self.FROM_Y, self.CROSS):
            self.copy(w, k, kind).wait_recv()

    def receive_all(self, w):
        for k in range(self.depth):
            self.receive(w, k)

    def sent(self, w):
        for k in range(self.depth):
            for kind in range(9):
                if kind != self.BY_Z or k:
                    self.copy(w, k, kind).wait_send()

    def sent_all(self):
        for w in range(len(self.blocks)):
            self.sent(w)

    def step(self, units, t):
        lag = self.depth
        if t < len(units):
            self.spread(*units[t])
        if 0 <= t - lag < len(units):
            self.relay(*units[t - lag])
        if 0 <= t - 2 * lag < len(units):
            self.hand_over(*units[t - 2 * lag])

    def units(self):
        return [(w, k) for w in range(len(self.blocks)) for k in range(self.depth)]

    def start_all(self):
        for w in range(len(self.blocks)):
            self.start(w)

def gather_sems(count, depth):
    return [
        pltpu.SemaphoreType.DMA((count, depth, 9)),
        pltpu.SemaphoreType.DMA((count, depth, 9)),
        pltpu.SemaphoreType.DMA((count,)),
    ]


class Scatter:
    TWIN, UPPER_Y, LOWER_X, UPPER_X, LOWER_Y, BY_Z = range(6)

    def __init__(self, place, grads, out, bufs, send_sems, recv_sems, local_sems, resident=()):
        self.place = place
        self.resident = resident
        self.grads = grads
        self.out = out
        self.bufs = bufs
        self.sems = (send_sems, recv_sems)
        self.local_sems = local_sems
        self.depth = place.depth
        self.order = list(range(1, self.depth)) + [0]

    def load(self, w, k):
        p = self.place
        return pltpu.make_async_copy(
            self.grads[w].at[p.ahead(k), :, :, p.core],
            self.bufs[w][6].at[k],
            self.local_sems.at[w, k],
        )

    def sums(self, w, k):
        if w in self.resident:
            return self.grads[w].at[self.place.ahead(k), :, :, self.place.core]
        return self.bufs[w][6].at[k]

    def half(self, w):
        return self.grads[w].shape[-2] // 2

    def copy(self, w, k, kind):
        p = self.place
        twin, upper_y, lower_x, upper_x, lower_y, by_z = self.bufs[w][:6]
        sums, half = self.sums(w, k), self.half(w)
        sems = [sem.at[w, k, kind] for sem in self.sems]
        top, bottom = pl.ds(0, half), pl.ds(half, half)
        if kind == self.TWIN:
            source = self.grads[w].at[p.ahead(k), :, :, 1 - p.core]
            return send(source, twin.at[k], *sems, p.twin())
        if kind == self.UPPER_Y:
            return send(sums.at[1 - p.y, :, top], upper_y.at[k], *sems, p.y_mate())
        if kind == self.LOWER_X:
            return send(sums.at[:, 1 - p.x, bottom], lower_x.at[k], *sems, p.x_mate())
        if kind == self.UPPER_X:
            return send(sums.at[p.y, 1 - p.x, top], upper_x.at[k], *sems, p.x_mate())
        if kind == self.LOWER_Y:
            return send(sums.at[1 - p.y, p.x, bottom], lower_y.at[k], *sems, p.y_mate())
        return send(sums.at[p.y, p.x], by_z.at[k], *sems, p.z_mate(k))

    @staticmethod
    def add(target, extra):
        total = target[...].astype(F32) + extra[...].astype(F32)
        target[...] = total.astype(target.dtype)

    def start(self, w):
        for k in self.order:
            self.begin(w, k)

    def begin(self, w, k):
        self.copy(w, k, self.TWIN).start()
        if w not in self.resident:
            self.load(w, k).start()

    def first(self, w, k):
        sums, twin = self.sums(w, k), self.bufs[w][0]
        if w not in self.resident:
            self.load(w, k).wait()
        self.copy(w, k, self.TWIN).wait_recv()

        def body(i, carry):
            self.add(sums.at[i // 2, i % 2], twin.at[k, i // 2, i % 2])
            return carry

        lax.fori_loop(0, 4, body, 0)
        self.copy(w, k, self.UPPER_Y).start()
        self.copy(w, k, self.LOWER_X).start()

    def second(self, w, k):
        p = self.place
        sums, half = self.sums(w, k), self.half(w)
        upper_y, lower_x = self.bufs[w][1:3]
        self.copy(w, k, self.UPPER_Y).wait_recv()
        self.copy(w, k, self.LOWER_X).wait_recv()

        def body(i, carry):
            self.add(sums.at[p.y, i, pl.ds(0, half)], upper_y.at[k, i])
            self.add(sums.at[i, p.x, pl.ds(half, half)], lower_x.at[k, i])
            return carry

        lax.fori_loop(0, 2, body, 0)
        self.copy(w, k, self.UPPER_X).start()
        self.copy(w, k, self.LOWER_Y).start()

    def third(self, w, k):
        p = self.place
        sums, half = self.sums(w, k), self.half(w)
        upper_x, lower_y = self.bufs[w][3:5]
        self.copy(w, k, self.UPPER_X).wait_recv()
        self.copy(w, k, self.LOWER_Y).wait_recv()
        self.add(sums.at[p.y, p.x, pl.ds(0, half)], upper_x.at[k])
        self.add(sums.at[p.y, p.x, pl.ds(half, half)], lower_y.at[k])
        if isinstance(k, int):
            if k:
                self.copy(w, k, self.BY_Z).start()
        else:
            pl.when(k != 0)(lambda: self.copy(w, k, self.BY_Z).start())

    def finish(self, w):
        p = self.place
        by_z = self.bufs[w][5]
        for k in range(1, self.depth):
            self.copy(w, k, self.BY_Z).wait_recv()
        total = self.sums(w, 0)[p.y, p.x].astype(F32)
        for k in range(1, self.depth):
            total = total + by_z[k].astype(F32)
        self.out[w][...] = total
        for k in range(self.depth):
            for kind in range(6):
                if kind != self.BY_Z or k:
                    self.copy(w, k, kind).wait_send()


BUFS = 7


def scatter_scratch(grads, depth, resident=()):
    scratch = []
    for w, grad in enumerate(grads):
        rows, columns = grad.shape[-2:]
        half = rows // 2
        shapes = [(depth, 2, 2, rows, columns)]
        shapes += [(depth, 2, half, columns)] * 2 + [(depth, half, columns)] * 2
        shapes += [(depth, rows, columns)]
        shapes += [(8, LANES) if w in resident else (depth, 2, 2, rows, columns)]
        scratch += [pltpu.VMEM(shape, grad.dtype) for shape in shapes]
    count = len(grads)
    scratch += [pltpu.SemaphoreType.DMA((count, depth, 6))] * 2
    return scratch + [pltpu.SemaphoreType.DMA((count, depth))]


def own_lanes(head):
    lane = lax.broadcasted_iota(jnp.int32, (1, LANES), 1)
    return (lane < HEAD_DIM) == (head == 0)


def fill_masks(ids_row, ids_column, masks):
    for b in range(masks.shape[0]):
        masks[b] = jnp.where(ids_column[b] == ids_row[b], 0.0, MASK_FILL).astype(F32)


def at_step(t, work):
    pl.when(pl.program_id(0) * pl.num_programs(1) + pl.program_id(1) == t)(work)


GROUPS = 4
GROUP_PAIRS = PAIRS // GROUPS
GROUP_WIDTH = 3 * LANES * GROUP_PAIRS


def rows_of(block):
    return block.reshape(-1, block.shape[-1])


def qkv_rows_of(rows, weight, h):
    columns = pl.ds(pl.multiple_of((h % GROUP_PAIRS) * 3 * LANES, 3 * LANES), 3 * LANES)
    if len(weight.shape) == 2:
        return dot_over(rows, weight[:, columns], 1, 0)
    return dot_over(rows, rows_of(weight[:, :, :, :, :, columns]), 1, 0)


def attend_kernel(depth, count, seqs, per, *refs):
    ids_row, ids_column, tokens = refs[:3]
    if depth:
        blocks, refs = refs[3 : 3 + count], refs[3 + count :]
        qkv, attended, log_total, whole_qkv, whole_vector = refs[:5]
        riders, refs = refs[5 : 5 + count - GROUPS], refs[5 + count - GROUPS :]
        masks, bias, groups, refs = refs[0], refs[1], refs[2 : 2 + GROUPS], refs[2 + GROUPS :]
        place = Place(depth)
        side = Gather(place, blocks, [*groups, *riders], *refs[:3])
        out_sems = refs[3]
        units = side.units()

        def out_copy(g):
            columns = pl.ds(0, GROUP_WIDTH)
            target = pl.ds(g * GROUP_WIDTH, GROUP_WIDTH)
            return pltpu.make_async_copy(
                groups[g].at[:, :, :, :, :, columns],
                whole_qkv.at[:, :, :, :, :, target],
                out_sems.at[g],
            )

        vector_copy = pltpu.make_async_copy(
            groups[0].at[:, :, :, :, :, pl.ds(GROUP_WIDTH, LANES)], whole_vector, out_sems.at[GROUPS]
        )

        def open_up():
            place.greet()
            side.start_all()
            for t in range(3 * depth):
                side.step(units, t)
            side.receive_all(0)
            out_copy(0).start()
            vector_copy.start()
            for r in range(2 * PAIRS):
                d, j = r // per, r % per
                spot = (d // 8, d // 4 % 2, d // 2 % 2, d % 2)
                row = groups[0][(*spot, slice(j, j + 1), slice(GROUP_WIDTH, GROUP_WIDTH + LANES))]
                bias[r] = row.astype(F32)

        at_step(0, open_up)
        steps = seqs * GROUP_PAIRS

        def each(work, w):
            for k in range(depth):
                work(w, k)

        def ready(g):
            side.receive_all(g)
            out_copy(g).start()

        steps = seqs * PAIRS
        plan = [[] for _ in range(steps)]

        def put(i, work, *what):
            plan[min(i, steps - 1)].append(functools.partial(work, *what))

        proj, up = GROUPS, GROUPS + 1
        put(1, each, side.spread, 3)
        put(2, each, side.hand_over, 1)
        put(2, each, side.relay, 2)
        put(3, each, side.spread, proj)
        put(steps // GROUPS, ready, 1)
        put(5, each, side.relay, 3)
        put(6, each, side.hand_over, 2)
        put(7, each, side.relay, proj)
        put(2 * steps // GROUPS, ready, 2)
        put(8, each, side.hand_over, 3)
        put(9, each, side.hand_over, proj)
        put(3 * steps // GROUPS, ready, 3)
        for k in range(depth):
            put(4 + k, side.spread, up, k)
            put(8 + k, side.relay, up, k)
            put(11 + k, side.hand_over, up, k)
        for i in range(1, steps):

            def more(i=i):
                for work in plan[i]:
                    work()

            if plan[i]:
                at_step(i, more)
    else:
        weight, bias, qkv, attended, log_total, masks = refs[3:]
    at_step(0, lambda: fill_masks(ids_row, ids_column, masks))
    h, b = pl.program_id(0), pl.program_id(1)
    length = masks.shape[1]
    rows = tokens[pl.ds(pl.multiple_of(b * length, length), length), :]
    if depth:
        shifts = [bias[h], jnp.zeros((1, LANES), F32), bias[PAIRS + h]]
        shift = jnp.concatenate(shifts, axis=1)
        for g in range(GROUPS):

            @pl.when(h // GROUP_PAIRS == g)
            def _():
                qkv[...] = (qkv_rows_of(rows, groups[g], h) + shift).astype(BF16)
    else:
        qkv[...] = (dot_over(rows, weight[...], 1, 0) + bias[0]).astype(BF16)
    query = qkv[:, 0:LANES] * BF16(SCALE)
    key = qkv[:, LANES : 2 * LANES]
    value = qkv[:, 2 * LANES : 3 * LANES]
    chunk = length // 2
    outs = []
    for head in range(2):
        own_key = jnp.where(own_lanes(head), key, BF16(0))
        parts = []
        for at in range(0, length, chunk):
            scores = dot_over(own_key, query[at : at + chunk], 1, 1)
            scores = scores + masks[b, :, at : at + chunk]
            top = jnp.max(scores, axis=0, keepdims=True)
            weights = jnp.exp(scores - top)
            total = jnp.sum(weights, axis=0, keepdims=True)
            log_total[0, 0, head : head + 1, at : at + chunk] = top + jnp.log(total)
            probs = (weights * (1.0 / total)).astype(BF16)
            parts.append(dot_over(probs, value, 0, 0))
        outs.append(jnp.concatenate(parts, axis=0))
    attended[...] = jnp.where(own_lanes(0), outs[0], outs[1]).astype(BF16)
    if depth:

        def close():
            for w in range(GROUPS, count):
                side.receive_all(w)
            side.sent_all()
            vector_copy.wait()
            for g in range(GROUPS):
                out_copy(g).wait()

        at_step(seqs * PAIRS - 1, close)


def attend_back_kernel(depth, seqs, per_device, *refs):
    ids_row, ids_column, tokens, qkv, attended_grad, log_total, weight, hidden_grad = refs[:8]
    steps = seqs * PAIRS
    i = pl.program_id(0)
    last = pl.num_programs(0) - 1
    spot = jnp.minimum(i, steps - 1)
    h, b = spot // seqs, spot % seqs
    if depth:
        up_grad, proj_grad, vector_part, input_grad = refs[8:12]
        out, refs = refs[12 : 15 + GROUPS], refs[15 + GROUPS :]
        masks, kept, total, sums, vector, *refs = refs
        groups, refs = refs[:GROUPS], refs[GROUPS:]
        grads = [up_grad, proj_grad, *groups, vector]
        count = len(grads)
        bufs = [refs[BUFS * w : BUFS * w + BUFS] for w in range(count)]
        place = Place(depth)
        side = Scatter(place, grads, out, bufs, *refs[BUFS * count :], resident=range(2, count))
        plan = [[] for _ in range(steps + tokens.shape[0] // ROW_BLOCK)]

        def put(at, work, *what):
            plan[min(at, len(plan) - 1)].append(functools.partial(work, *what))

        def each(work, w):
            def body(k, carry):
                work(w, k)
                return carry

            lax.fori_loop(0, depth, body, 0)

        up, proj, vec = 0, 1, count - 1
        put(0, place.greet)
        put(0, side.start, up)
        put(0, side.start, proj)
        for n, k in enumerate(side.order):
            put(1 + 2 * n, side.first, up, k)
            put(4 + 2 * n + n // 2, side.second, up, k)
            put(7 + 2 * n + n // 2, side.third, up, k)
        put(2, each, side.first, proj)
        put(5, each, side.second, proj)
        put(8, each, side.third, proj)
        per = steps // GROUPS
        for g in range(GROUPS):
            at = per * (g + 1)
            put(at, each, side.begin, 2 + g)
            put(at + 1, each, side.first, 2 + g)
            put(at + min(4, GROUPS + 1 - g), each, side.second, 2 + g)
            put(at + min(7, GROUPS + 2 - g), each, side.third, 2 + g)
        rows_each = per_device

        def make_vector():
            vector[...] = vector_part[...]
            for r in range(2 * PAIRS):
                d, j = r // rows_each, r % rows_each
                source = 0 if r < PAIRS else 2 * LANES
                row = sums[r % PAIRS, :, source : source + LANES]
                vector[d // 8, d // 4 % 2, d // 2 % 2, d % 2, j : j + 1, :] = row

        put(steps, make_vector)
        put(steps + 1, each, side.begin, vec)
        put(steps + 2, each, side.first, vec)
        put(steps + 3, each, side.second, vec)
        for at, works in enumerate(plan):

            def run(works=works):
                for work in works:
                    work()

            if works:
                pl.when(i == at)(run)
    else:
        input_grad, weight_grads, sums, masks, kept, total = refs[8:]
    pl.when(i == 0)(lambda: fill_masks(ids_row, ids_column, masks))
    length = qkv.shape[0]
    chunk = length // 2
    wide = pl.ds(pl.multiple_of(h * 3 * LANES, 3 * LANES), 3 * LANES)
    tall = pl.ds(pl.multiple_of(b * length, length), length)

    @pl.when(i < steps)
    def _():
        query = qkv[:, 0:LANES]
        key = qkv[:, LANES : 2 * LANES]
        value = qkv[:, 2 * LANES : 3 * LANES]
        grad = attended_grad[...]
        scaled = query * BF16(SCALE)
        query_grads, key_grads, value_grads = [], [], []
        for head in range(2):
            own_key = jnp.where(own_lanes(head), key, BF16(0))
            own_value = jnp.where(own_lanes(head), value, BF16(0))
            key_grad = value_grad = None
            parts = []
            for at in range(0, length, chunk):
                piece = slice(at, at + chunk)
                scores = dot_over(own_key, scaled[piece], 1, 1) + masks[b, :, piece]
                probs = jnp.exp(scores - log_total[0, 0, head : head + 1, piece])
                prob_grad = dot_over(own_value, grad[piece], 1, 1)
                row_dot = jnp.sum(probs * prob_grad, axis=0, keepdims=True)
                score_grad = (probs * (prob_grad - row_dot)).astype(BF16)
                value_part = dot_over(probs.astype(BF16), grad[piece], 1, 0)
                key_part = dot_over(score_grad, query[piece], 1, 0)
                value_grad = value_part if value_grad is None else value_grad + value_part
                key_grad = key_part if key_grad is None else key_grad + key_part
                parts.append(dot_over(score_grad, key, 0, 0))
            query_grads.append(jnp.concatenate(parts, axis=0))
            key_grads.append(key_grad)
            value_grads.append(value_grad)
        first = own_lanes(0)
        own = [
            (jnp.where(first, *query_grads) * SCALE).astype(BF16),
            (jnp.where(first, *key_grads) * SCALE).astype(BF16),
            jnp.where(first, *value_grads).astype(BF16),
        ]
        rows_grad = jnp.concatenate(own, axis=1)
        kept[tall, wide] = rows_grad
        part = dot_over(tokens[tall, :], rows_grad, 0, 0)
        part_sums = jnp.sum(rows_grad.astype(F32), axis=0, keepdims=True)

        @pl.when(b == 0)
        def _():
            total[...] = part
            sums[h] = part_sums

        @pl.when(b > 0)
        def _():
            total[...] += part
            sums[h] += part_sums

        @pl.when(b == seqs - 1)
        def _():
            if depth:
                where = (h % GROUP_PAIRS) * 3 * LANES
                columns = pl.ds(pl.multiple_of(where, 3 * LANES), 3 * LANES)
                for g in range(GROUPS):

                    @pl.when(h // GROUP_PAIRS == g)
                    def _():
                        shape = groups[g].shape[:5] + (3 * LANES,)
                        groups[g][:, :, :, :, :, columns] = total[...].astype(BF16).reshape(shape)
            else:
                weight_grads[...] = total[...]

    @pl.when(i >= steps)
    def _():
        at = pl.multiple_of((i - steps) * ROW_BLOCK, ROW_BLOCK)
        back = dot_over(kept[pl.ds(at, ROW_BLOCK), :], weight[...], 1, 1)
        input_grad[...] = (back + hidden_grad[...]).astype(BF16)

    if depth:

        @pl.when(i == last)
        def _():
            each(side.third, vec)
            for w in range(count):
                side.finish(w)


def whole(shape):
    return pl.BlockSpec(shape, lambda h, b: (0,) * len(shape))


def attention_specs(count, length):
    rows = whole((count, 1, length))
    columns = whole((count, length, 1))
    tokens = whole((count * length, D))
    wide = pl.BlockSpec((length, 3 * LANES), lambda h, b: (b, h))
    one = pl.BlockSpec((length, LANES), lambda h, b: (b, h))
    log_total = pl.BlockSpec((1, 1, 2, length), lambda h, b: (b, h, 0, 0))
    weight = pl.BlockSpec((D, 3 * LANES), lambda h, b: (0, h))
    vector = pl.BlockSpec((1, 1, 3 * LANES), lambda h, b: (h, 0, 0))
    return rows, columns, tokens, wide, one, log_total, weight, vector


def kernel_params(collective_id, remote, limit=60 << 20):
    if not remote:
        return pltpu.CompilerParams(vmem_limit_bytes=limit)
    return pltpu.CompilerParams(
        collective_id=collective_id, has_side_effects=True, vmem_limit_bytes=limit
    )


def attend(tokens, doc_ids, weight, bias, blocks, per, depth, collective_id):
    count, length = doc_ids.shape
    rows, columns, all_tokens, wide, one, log_total, part, vector = attention_specs(count, length)
    in_place = pl.BlockSpec(memory_space=pl.ANY)
    out_shape = [
        jax.ShapeDtypeStruct((count * length, 3 * D), BF16),
        jax.ShapeDtypeStruct((count * length, D), BF16),
        jax.ShapeDtypeStruct((count, PAIRS, 2, length), F32),
    ]
    out_specs = [wide, one, log_total]
    in_specs = [rows, columns, all_tokens]
    scratch = [pltpu.VMEM((count, length, length), F32)]
    grid3 = (depth, 2, 2, 2)
    if depth:
        in_specs += [whole(b.shape) for b in blocks]
        tall = blocks[0].shape[0]
        shapes = [(*grid3, tall, 3 * D), (*grid3, tall, LANES)]
        shapes += [grid3 + b.shape for b in blocks[GROUPS:]]
        out_shape += [jax.ShapeDtypeStruct(shape, BF16) for shape in shapes]
        out_specs += [in_place] * len(shapes)
        scratch += [pltpu.VMEM((2 * PAIRS, 1, LANES), F32)]
        scratch += [pltpu.VMEM(grid3 + b.shape, BF16) for b in blocks[:GROUPS]]
        scratch += gather_sems(len(blocks), depth) + [pltpu.SemaphoreType.DMA((GROUPS + 1,))]
        operands = blocks
    else:
        in_specs += [part, vector]
        operands = [weight, bias.reshape(PAIRS, 1, 3 * LANES)]
    return pl.pallas_call(
        functools.partial(attend_kernel, depth, len(blocks), count, per),
        grid=(PAIRS, count),
        in_specs=in_specs,
        out_specs=out_specs,
        out_shape=out_shape,
        scratch_shapes=scratch,
        compiler_params=kernel_params(collective_id, len(blocks)),
        name="attend",
    )(
        doc_ids.reshape(count, 1, length),
        doc_ids.reshape(count, length, 1),
        tokens,
        *operands,
    )


def attend_back(
    tokens, qkv, doc_ids, attended_grad, totals, weight, hidden_grad, grads, per_device, depth, collective_id
):
    seqs, length = doc_ids.shape
    steps = seqs * PAIRS
    blocks = seqs * length // ROW_BLOCK

    def h(i):
        return jnp.minimum(i, steps - 1) // seqs

    def b(i):
        return jnp.minimum(i, steps - 1) % seqs

    def late(i):
        return jnp.maximum(i - steps, 0)

    in_place = pl.BlockSpec(memory_space=pl.ANY)
    in_specs = [
        once((seqs, 1, length)),
        once((seqs, length, 1)),
        once((seqs * length, D)),
        pl.BlockSpec((length, 3 * LANES), lambda i: (b(i), h(i))),
        pl.BlockSpec((length, LANES), lambda i: (b(i), h(i))),
        pl.BlockSpec((1, 1, 2, length), lambda i: (b(i), h(i), 0, 0)),
        once((D, 3 * D)),
        pl.BlockSpec((ROW_BLOCK, D), lambda i: (late(i), 0)),
    ]
    out_specs = [pl.BlockSpec((ROW_BLOCK, D), lambda i: (late(i), 0))]
    out_shape = [jax.ShapeDtypeStruct((seqs * length, D), BF16)]
    scratch = [
        pltpu.VMEM((seqs, length, length), F32),
        pltpu.VMEM((seqs * length, 3 * D), BF16),
        pltpu.VMEM((D, 3 * LANES), F32),
    ]
    if depth:
        up_grad, proj_grad, vector = grads
        tall = up_grad.shape[-2]
        group = jax.ShapeDtypeStruct((depth, 2, 2, 2, tall, GROUP_WIDTH), BF16)
        moved = [up_grad, proj_grad, *([group] * GROUPS), vector]
        in_specs += [in_place, in_place, flat(vector.shape)]
        out_specs += [flat(m.shape[-2:]) for m in moved]
        out_shape += [jax.ShapeDtypeStruct(m.shape[-2:], F32) for m in moved]
        scratch += [pltpu.VMEM((PAIRS, 1, 3 * LANES), F32), pltpu.VMEM(vector.shape, F32)]
        scratch += [pltpu.VMEM(group.shape, BF16)] * GROUPS
        scratch += scatter_scratch(moved, depth, resident=range(2, len(moved)))
    else:
        out_specs += [
            pl.BlockSpec((D, 3 * LANES), lambda i: (0, h(i))),
            flat((PAIRS, 1, 3 * LANES)),
        ]
        out_shape += [
            jax.ShapeDtypeStruct((D, 3 * D), F32),
            jax.ShapeDtypeStruct((PAIRS, 1, 3 * LANES), F32),
        ]
    return pl.pallas_call(
        functools.partial(attend_back_kernel, depth, seqs, per_device),
        grid=(steps + blocks,),
        in_specs=in_specs,
        out_specs=out_specs,
        out_shape=out_shape,
        scratch_shapes=scratch,
        compiler_params=kernel_params(collective_id, depth, 63 << 20),
        name="attend_back",
    )(
        doc_ids.reshape(seqs, 1, length),
        doc_ids.reshape(seqs, length, 1),
        tokens,
        qkv,
        attended_grad,
        totals,
        weight,
        hidden_grad,
        *grads,
    )


TILE = 512
ROW_CHUNK = 256


def widen_kernel(depth, tiles, *refs):
    low, up_weight, up_bias, normed, scales = refs[:5]
    blocks = refs[5:7]
    activated, slope, second_in, whole_up, whole_down = refs[7:12]
    kept, tile_weight, late_up, down, out_sems, *sems = refs[12:]
    place = Place(depth)
    side = Gather(place, blocks, [late_up, down], *sems)
    i = pl.program_id(0)
    per = tiles // depth
    half = tiles // 2

    def out_copy(k):
        zz = place.back(k)
        return pltpu.make_async_copy(down.at[zz], whole_down.at[zz], out_sems.at[k])

    up_copy = pltpu.make_async_copy(late_up, whole_up, out_sems.at[depth])
    plan = [[] for _ in range(tiles + depth)]

    def put(at, work, *what):
        plan[min(at, len(plan) - 1)].append(functools.partial(work, *what))

    put(0, place.greet)
    put(0, side.start_all)
    for k in range(depth):
        put(min(k, half - 1), side.spread, 0, k)
        put(min(k + 2, half), side.relay, 0, k)
    put(half, side.spread, 1, 0)
    put(half, side.spread, 1, 1)
    for k in range(depth):
        put(half, side.hand_over, 0, k)
    put(half, side.receive_all, 0)
    put(half, up_copy.start)
    put(half + 1, side.relay, 1, 0)
    for k in range(2, depth):
        put(half + 2 * k - 2, side.spread, 1, k)
    for k in range(1, depth - 1):
        put(half + 1 + 2 * k, side.relay, 1, k)
    put(tiles + depth - 2, side.relay, 1, depth - 1)
    for k in range(depth):
        put(tiles + k, side.hand_over, 1, k)
    for at, works in enumerate(plan):

        def run(works=works):
            for work in works:
                work()

        if works:
            pl.when(i == at)(run)

    @pl.when(i < half)
    def _():
        tile_weight[...] = up_weight[...]

    @pl.when((i >= half) & (i < tiles))
    def _():
        columns = pl.ds(pl.multiple_of((i - half) * TILE, TILE), TILE)
        tile_weight[...] = rows_of(late_up[:, :, :, :, :, columns])

    @pl.when(i < tiles)
    def _():
        for at in range(0, low.shape[0], ROW_CHUNK):
            rows = slice(at, at + ROW_CHUNK)
            upward = dot_over(low[rows, :], tile_weight[...], 1, 0) + up_bias[...]
            cdf = 0.5 * (1.0 + lax.erf(upward * HALF_ROOT))
            value = (upward * cdf).astype(BF16)
            activated[rows, :] = value
            kept[i, rows, :] = value
            slope[rows, :] = cdf + upward * (PDF_TOP * jnp.exp(-0.5 * upward * upward))

    for k in range(depth):

        def layer(k=k):
            side.receive(1, k)
            out_copy(k).start()
            zz = place.back(k)
            for at in range(0, low.shape[0], ROW_CHUNK):
                rows = slice(at, at + ROW_CHUNK)
                if k == 0:
                    total = normed[rows, :] * scales[0:1, :] + scales[1:2, :] + scales[2:3, :]
                else:
                    total = second_in[rows, :]
                for n in range(per):
                    tile = kept[zz * per + n, rows, :]
                    weight = rows_of(down[zz, n * 2 // per : (n + 1) * 2 // per])
                    total = total + dot_over(tile, weight, 1, 0)
                second_in[rows, :] = total

        pl.when(i == tiles + k)(layer)

    @pl.when(i == tiles + depth - 1)
    def _():
        side.sent_all()
        up_copy.wait()
        for k in range(depth):
            out_copy(k).wait()


def flat(shape):
    return pl.BlockSpec(shape, lambda i: (0,) * len(shape))


def once(shape):
    return pl.BlockSpec(shape, lambda i: (0,) * len(shape), pipeline_mode=pl.Buffered(1))


def widen(low, up_weight, up_bias, normed, scales, blocks, depth, collective_id):
    count = low.shape[0]
    tiles = FF // TILE
    last, half = tiles - 1, tiles // 2
    tile = pl.BlockSpec((count, TILE), lambda i: (0, jnp.minimum(i, last)))
    spread = [(depth, 2, 2, 2) + block.shape for block in blocks]
    in_place = pl.BlockSpec(memory_space=pl.ANY)
    return pl.pallas_call(
        functools.partial(widen_kernel, depth, tiles),
        grid=(tiles + depth,),
        in_specs=[
            once(low.shape),
            pl.BlockSpec((D, TILE), lambda i: (0, jnp.minimum(i, half - 1))),
            pl.BlockSpec((1, TILE), lambda i: (0, jnp.minimum(i, last))),
            once(normed.shape),
            once(scales.shape),
            *[once(block.shape) for block in blocks],
        ],
        out_specs=[tile, tile, flat((count, D)), in_place, in_place],
        out_shape=[
            jax.ShapeDtypeStruct((count, FF), BF16),
            jax.ShapeDtypeStruct((count, FF), F32),
            jax.ShapeDtypeStruct((count, D), F32),
            *[jax.ShapeDtypeStruct(shape, BF16) for shape in spread],
        ],
        scratch_shapes=[
            pltpu.VMEM((tiles, count, TILE), BF16),
            pltpu.VMEM((D, TILE), BF16),
            *[pltpu.VMEM(shape, BF16) for shape in spread],
            pltpu.SemaphoreType.DMA((depth + 1,)),
            *gather_sems(2, depth),
        ],
        compiler_params=kernel_params(collective_id, 1),
        name="widen",
    )(low, up_weight, up_bias[None], normed, scales, *blocks)


def early_tile(i, tiles, depth):
    ahead = (lax.axis_index("dp") // 8 + 1) * (tiles // depth)
    return (jnp.minimum(i, tiles - 1) + ahead) % tiles


def widen_back_kernel(depth, tiles, *refs):
    rows_grad, activated, slope, down_weight, low_turned, up_early, up_late = refs[:7]
    up_grad, branch_grad, sums, down_out = refs[7:11]
    kept, down_grad, total, *rest = refs[11:]
    place = Place(depth)
    side = Scatter(place, [down_grad], [down_out], [rest[:BUFS]], *rest[BUFS:], resident=(0,))
    i = pl.program_id(0)
    per = tiles // depth

    def step_of(t, work):
        pl.when(i == t)(work)

    step_of(0, place.greet)
    now = early_tile(i, tiles, depth)
    for n, k in enumerate(side.order):
        ready = (n + 1) * per
        step_of(ready, functools.partial(side.begin, 0, k))
        step_of(ready + 1, functools.partial(side.first, 0, k))
        step_of(ready + 3, functools.partial(side.second, 0, k))
        step_of(ready + 5, functools.partial(side.third, 0, k))

    @pl.when(i < tiles)
    def _():
        for at in range(0, rows_grad.shape[0], ROW_CHUNK):
            rows = slice(at, at + ROW_CHUNK)
            back = dot_over(rows_grad[rows, :], down_weight[...], 1, 1)
            kept[now, rows, :] = (back * slope[rows, :]).astype(BF16)
        sums[0] = jnp.sum(kept[now].astype(F32), axis=0, keepdims=True)
        grad = dot_over(activated[...], rows_grad[...], 0, 0).astype(BF16)
        blocks = TILE // down_grad.shape[4]
        grad = grad.reshape(1, blocks // 4, 2, 2, down_grad.shape[4], D)[0]
        part = pl.ds((now % per) * (blocks // 4), blocks // 4)
        down_grad[now // per, part] = grad

    @pl.when(i >= tiles)
    def _():
        tile = kept[i - tiles]
        up_grad[...] = dot_over(low_turned[...], tile, 1, 0).astype(BF16)
        up_weight = jnp.where(i - tiles < tiles // 2, up_early[...], up_late[...])
        for at in range(0, rows_grad.shape[0], ROW_CHUNK):
            rows = slice(at, at + ROW_CHUNK)
            part = dot_over(tile[rows, :], up_weight, 1, 1)

            @pl.when(i == tiles)
            def _():
                total[rows, :] = part

            @pl.when(i > tiles)
            def _():
                total[rows, :] += part

    @pl.when(i == 2 * tiles - 1)
    def _():
        branch_grad[...] = total[...]
        side.finish(0)


def widen_back(
    rows_grad, activated, slope, down_weight, low_turned, up_early, up_late, depth, collective_id
):
    count = rows_grad.shape[0]
    tiles = FF // TILE

    half = tiles // 2

    def early(i):
        return early_tile(i, tiles, depth)

    def late(i):
        return jnp.maximum(i - tiles, 0)

    shares = 8 * depth
    spread = jax.ShapeDtypeStruct((depth, 2, 2, 2, FF // shares, D), BF16)
    return pl.pallas_call(
        functools.partial(widen_back_kernel, depth, tiles),
        grid=(2 * tiles,),
        in_specs=[
            once(rows_grad.shape),
            pl.BlockSpec((count, TILE), lambda i: (0, early(i))),
            pl.BlockSpec((count, TILE), lambda i: (0, early(i))),
            pl.BlockSpec((TILE, D), lambda i: (early(i), 0)),
            once(low_turned.shape),
            pl.BlockSpec((D, TILE), lambda i: (0, jnp.minimum(late(i), half - 1))),
            pl.BlockSpec((D, TILE), lambda i: (0, jnp.maximum(late(i) - half, 0))),
        ],
        out_specs=[
            pl.BlockSpec((D, TILE), lambda i: (0, late(i))),
            flat((count, D)),
            pl.BlockSpec((1, 1, TILE), lambda i: (early(i), 0, 0)),
            flat(spread.shape[-2:]),
        ],
        out_shape=[
            jax.ShapeDtypeStruct((D, FF), BF16),
            jax.ShapeDtypeStruct((count, D), F32),
            jax.ShapeDtypeStruct((tiles, 1, TILE), F32),
            jax.ShapeDtypeStruct(spread.shape[-2:], F32),
        ],
        scratch_shapes=[
            pltpu.VMEM((tiles, count, TILE), BF16),
            pltpu.VMEM(spread.shape, BF16),
            pltpu.VMEM((count, D), F32),
            *scatter_scratch([spread], depth, resident=(0,)),
        ],
        compiler_params=kernel_params(collective_id, 1),
        name="widen_back",
    )(rows_grad, activated, slope, down_weight, low_turned, up_early, up_late)


ROW_BLOCK = 256


def mean_of(rows):
    return jnp.sum(rows, axis=-1, keepdims=True) * (1.0 / D)


def normalized(hidden):
    center = hidden - mean_of(hidden)
    root = lax.rsqrt(mean_of(center * center) + NORM_EPS)
    return center * root, root


def norm_back(grad, normed, root, gain):
    scaled = grad * gain
    return root * (scaled - mean_of(scaled) - normed * mean_of(scaled * normed))


def add_sums(sums, *rows):
    new = [jnp.sum(r.astype(F32), axis=0, keepdims=True) for r in rows]

    @pl.when(pl.program_id(0) == 0)
    def _():
        sums[...] = jnp.zeros_like(sums)

    for j, n in enumerate(new):
        sums[j : j + 1, :] += n


def project_kernel(attended, tokens, weight, scales, normed, root, low, turned):
    hidden = dot_over(attended[...], weight[...], 1, 0)
    hidden = tokens[...].astype(F32) + hidden + scales[0:1, :]
    normed[...], root[...] = normalized(hidden)
    branch = normed[...] * scales[1:2, :] + scales[2:3, :]
    low[...] = branch.astype(BF16)
    turned[...] = branch.T.astype(BF16)


def output_kernel(second_in, cotangent, scales, output, rows, grad, sums):
    normed, root = normalized(second_in[...])
    output[...] = (normed * scales[0:1, :] + scales[1:2, :]).astype(BF16)
    upstream = cotangent[...].astype(F32)
    grad[...] = norm_back(upstream, normed, root, scales[0:1, :])
    rows[...] = grad[...].astype(BF16)
    add_sums(sums, upstream * normed, upstream, rows[...])


def project_back_kernel(
    branch_grad, second_grad, normed, root, attended, weight, scales, grad, back, weight_grads, sums, total
):
    upstream = branch_grad[...] + second_grad[...]
    grad[...] = norm_back(upstream, normed[...], root[...], scales[0:1, :])
    rows = grad[...].astype(BF16)
    back[...] = dot_over(rows, weight[...], 1, 1).astype(BF16)
    add_sums(sums, upstream * normed[...], upstream, rows)
    part = dot_over(attended[...], rows, 0, 0)

    @pl.when(pl.program_id(0) == 0)
    def _():
        total[...] = part

    @pl.when(pl.program_id(0) > 0)
    def _():
        total[...] += part

    @pl.when(pl.program_id(0) == pl.num_programs(0) - 1)
    def _():
        weight_grads[...] = total[...].astype(weight_grads.dtype)


def row_block(width=D):
    return pl.BlockSpec((ROW_BLOCK, width), lambda i: (i, 0))


def row_call(kernel, count, in_specs, out_specs, outs, scratch=()):
    return pl.pallas_call(
        kernel,
        grid=(count // ROW_BLOCK,),
        in_specs=in_specs,
        out_specs=out_specs,
        out_shape=[jax.ShapeDtypeStruct(shape, dtype) for shape, dtype in outs],
        scratch_shapes=list(scratch),
        compiler_params=pltpu.CompilerParams(vmem_limit_bytes=60 << 20),
        name=kernel.__name__,
    )


SUMS = (8, D)


def project(attended, tokens, weight, scales):
    count = tokens.shape[0]
    block, matrix = row_block(), flat((D, D))
    turned = pl.BlockSpec((D, ROW_BLOCK), lambda i: (0, i))
    outs = [((count, D), F32), ((count, 1), F32), ((count, D), BF16), ((D, count), BF16)]
    return row_call(
        project_kernel,
        count,
        [block, block, matrix, flat(scales.shape)],
        [block, row_block(1), block, turned],
        outs,
    )(attended, tokens, weight, scales)


def output_and_grad(second_in, cotangent, scales):
    count = second_in.shape[0]
    block = row_block()
    shape = (count, D)
    return row_call(
        output_kernel,
        count,
        [block, block, flat(scales.shape)],
        [block, block, block, flat(SUMS)],
        [(shape, BF16), (shape, BF16), (shape, F32), (SUMS, F32)],
    )(second_in, cotangent, scales)


def project_back(branch_grad, second_grad, normed, root, attended, weight, scales, dtype):
    count = attended.shape[0]
    block, matrix = row_block(), flat((D, D))
    shape = (count, D)
    return row_call(
        project_back_kernel,
        count,
        [block, block, block, row_block(1), block, matrix, flat(scales.shape)],
        [block, block, matrix, flat(SUMS)],
        [(shape, F32), (shape, BF16), ((D, D), dtype), (SUMS, F32)],
        [pltpu.VMEM((D, D), F32)],
    )(branch_grad, second_grad, normed, root, attended, weight, scales)


def split_vector(vector):
    sizes = (D, D, D, D, D, FF, D, D, D)
    parts, at = [], 0
    for size in sizes:
        parts.append(vector[at : at + size])
        at += size
    return parts


def by_pair(columns):
    rows = columns.shape[0]
    return columns.reshape(rows, 3, PAIRS, LANES).swapaxes(1, 2).reshape(rows, 3 * D)


def by_kind(columns):
    rows = columns.shape[0]
    return columns.reshape(rows, PAIRS, 3, LANES).swapaxes(1, 2).reshape(rows, 3 * D)


def stacked(*vectors):
    return jnp.pad(jnp.stack(vectors), ((0, 8 - len(vectors)), (0, 0)))


def column_sums(rows):
    return jnp.sum(rows.astype(F32), axis=0)


def times(rows, matrix):
    return jnp.dot(rows, matrix, preferred_element_type=F32)


def weight_grad(left_rows, right_rows, dtype):
    return dot_over(left_rows, right_rows, 0, 0).astype(dtype)


def back_product(grad_rows, matrix):
    return dot_over(grad_rows, matrix, 1, 1)


def layer_step(tokens, doc_ids, cotangent, masters, devices, depth):
    grad_type = BF16 if depth else F32
    shape = (depth, 2, 2, 2)
    blocks, low_vector = lowered_blocks(masters)
    rows = low_vector.shape[0] // LANES
    if depth:
        tall = blocks[0].shape[0]
        padded = jnp.pad(low_vector.reshape(rows, LANES), ((0, tall - rows), (0, 0)))
        first = [blocks[0][:, g * GROUP_WIDTH : (g + 1) * GROUP_WIDTH] for g in range(GROUPS)]
        first[0] = jnp.concatenate([first[0], padded], axis=1)
        up_blocks = [blocks[2][:, : FF // 2], blocks[2][:, FF // 2 :]]
        qkv, attended, totals, qkv_weight, vectors, proj_weight, up_weight = attend(
            tokens, doc_ids, None, None, [*first, blocks[1], up_blocks[0]], rows, depth, 1
        )
        vector = vectors.reshape(devices, tall, LANES)[:, :rows].reshape(-1)
        qkv_weight, proj_weight, up_weight = map(rows_of, (qkv_weight, proj_weight, up_weight))
    else:
        weights = [lax.all_gather(b, "dp", axis=0, tiled=True) for b in blocks]
        qkv_weight, proj_weight, up_weight, down_weight = weights
        vector = lax.all_gather(low_vector, "dp", axis=0, tiled=True)
    (
        bias_query,
        bias_value,
        bias_proj,
        gain_first,
        shift_first,
        bias_up,
        bias_down,
        gain_second,
        shift_second,
    ) = split_vector(vector.astype(F32))
    if not depth:
        bias_all = jnp.concatenate([bias_query, jnp.zeros_like(bias_query), bias_value])
        bias_all = by_pair(bias_all[None])[0]
        qkv, attended, totals = attend(tokens, doc_ids, qkv_weight, bias_all, [], 0, 0, 0)
    normed, root, branch_low, low_turned = project(
        attended, tokens, proj_weight, stacked(bias_proj, gain_first, shift_first)
    )
    if depth:
        activated, slope, second_in, up_late, down_weight = widen(
            branch_low,
            up_weight,
            bias_up,
            normed,
            stacked(gain_first, shift_first, bias_down),
            [up_blocks[1], blocks[3]],
            depth,
            2,
        )
        up_late, down_weight = rows_of(up_late), rows_of(down_weight)
    else:
        upward = times(branch_low, up_weight) + bias_up
        cdf = 0.5 * (1.0 + lax.erf(upward * HALF_ROOT))
        activated = (upward * cdf).astype(BF16)
        slope = cdf + upward * (PDF_TOP * jnp.exp(-0.5 * upward * upward))
        branch = normed * gain_first + shift_first
        second_in = branch + times(activated, down_weight) + bias_down
    output, down_rows, second_grad, second_sums = output_and_grad(
        second_in, cotangent, stacked(gain_second, shift_second)
    )
    if depth:
        up_grad, branch_grad, bias_up_grad, down_owned = widen_back(
            down_rows,
            activated,
            slope,
            down_weight,
            low_turned,
            up_weight,
            up_late,
            depth,
            3,
        )
        bias_up_grad = bias_up_grad.reshape(-1)
    else:
        down_grad = weight_grad(activated, down_rows, F32)
        up_rows = (back_product(down_rows, down_weight) * slope).astype(BF16)
        bias_up_grad = column_sums(up_rows)
        up_grad = weight_grad(branch_low, up_rows, F32)
        branch_grad = back_product(up_rows, up_weight)
    hidden_grad, attended_grad, proj_grad, first_sums = project_back(
        branch_grad,
        second_grad,
        normed,
        root,
        attended,
        proj_weight,
        stacked(gain_first),
        grad_type,
    )
    known = [
        first_sums[2],
        first_sums[0],
        first_sums[1],
        bias_up_grad,
        second_sums[2],
        second_sums[0],
        second_sums[1],
    ]
    riders = []
    if depth:
        vector_part = jnp.concatenate([jnp.zeros((2 * D,), F32), *known])
        vector_part = vector_part.reshape(devices, rows, LANES)
        vector_part = jnp.pad(vector_part, ((0, 0), (0, 16 - rows), (0, 0)))
        riders = [g.reshape(*shape, -1, g.shape[1]) for g in (up_grad, proj_grad)]
        riders += [vector_part.reshape(*shape, 16, LANES)]
    input_grad, *summed = attend_back(
        tokens,
        qkv,
        doc_ids,
        attended_grad,
        totals,
        qkv_weight,
        hidden_grad,
        riders,
        rows,
        depth,
        4,
    )
    if depth:
        up_owned, proj_owned, *qkv_owned, vector_owned = summed
        owned = [jnp.concatenate(qkv_owned, axis=1), proj_owned, up_owned, down_owned]
        owned += [vector_owned[:rows]]
    else:
        qkv_grad, qkv_sums = summed
        qkv_sums = by_kind(qkv_sums.reshape(1, -1))[0]
        vector_grad = jnp.concatenate([qkv_sums[0:D], qkv_sums[2 * D : 3 * D], *known])
        grads = (qkv_grad, proj_grad, up_grad, down_grad, vector_grad[:, None])
        owned = [
            lax.psum_scatter(
                grad.reshape(devices, -1, grad.shape[-1]), "dp", scatter_dimension=0, tiled=True
            )[0]
            for grad in grads
        ]
    owned[0] = by_kind(owned[0])
    return output, input_grad, [own.reshape(-1) for own in owned]


def adam_update(master, moment_one, moment_two, grad, rate):
    one_new = BETA_FIRST * moment_one + (1.0 - BETA_FIRST) * grad
    two_new = BETA_SECOND * moment_two + (1.0 - BETA_SECOND) * grad * grad
    one_hat = one_new / (1.0 - BETA_FIRST**STEP)
    two_hat = two_new / (1.0 - BETA_SECOND**STEP)
    master_new = master - rate * (one_hat / (jnp.sqrt(two_hat) + ADAM_EPS) + WEIGHT_DECAY * master)
    return (grad, one_new, two_new, master_new, master_new.astype(BF16))


WIDTHS = (3 * D, D, FF, D)


def lowered_blocks(masters):
    lowered = [master.astype(BF16) for master in masters]
    blocks = [low.reshape(-1, width) for low, width in zip(lowered, WIDTHS)]
    blocks[0] = by_pair(blocks[0])
    return blocks, lowered[4]


def body(depth, tokens, segment_ids, out_grad, *states):
    devices = lax.axis_size("dp")
    masters = states[0::3]
    output, input_grad, owned = layer_step(
        tokens, segment_ids, out_grad, masters, devices, depth
    )
    outs = [output, input_grad]
    for i in range(5):
        outs += adam_update(*states[3 * i : 3 * i + 3], owned[i], RATES[i])
    return tuple(outs)


def solution(mesh):
    rows = P("dp", None)
    flat = P("dp")
    return jax.shard_map(
        functools.partial(body, depth_of(mesh)),
        mesh=mesh,
        in_specs=(rows,) * 3 + (flat,) * 15,
        out_specs=(rows,) * 2 + (flat,) * 25,
        check_vma=False,
    )
```

```python
import functools

import jax
import jax.numpy as jnp
from jax import lax
from jax.experimental import pallas as pl
from jax.experimental.pallas import tpu as pltpu
from jax.sharding import PartitionSpec as P

D = 1024
HEADS = 16
HEAD_DIM = 64
FF = 4096
STEP = 3
LANES = 128
PAIRS = HEADS * HEAD_DIM // LANES

NORM_EPS = 1e-05
BETA_FIRST = 0.5
BETA_SECOND = 0.5
ADAM_EPS = 1e-08
WEIGHT_DECAY = 0.01
MASK_FILL = -1000000000.0
RATES = (0.01, 0.03, 0.01, 0.005, 0.05)
SCALE = HEAD_DIM ** (-0.5)
HALF_ROOT = 0.7071067811865476
PDF_TOP = 0.3989422804014327

F32 = jnp.float32
BF16 = jnp.bfloat16
MESH = pl.DeviceIdType.MESH


def dot_over(left, right, left_dim, right_dim):
    return lax.dot_general(
        left, right, (((left_dim,), (right_dim,)), ((), ())), preferred_element_type=F32
    )


PLANNED_DEPTH = 4


def depth_of(mesh):
    devices = list(mesh.devices.flat)
    if len(devices) % 8:
        return 0
    try:
        spots = [(*d.coords, d.core_on_chip) for d in devices]
    except AttributeError:
        return 0
    low = [min(s[i] for s in spots) for i in range(4)]
    depth = len(devices) // 8
    if depth != PLANNED_DEPTH:
        return 0
    for index, (x, y, z, core) in enumerate(spots):
        spot = (((z - low[2]) * 2 + y - low[1]) * 2 + x - low[0]) * 2 + core - low[3]
        if spot != index:
            return 0
    return depth


class Place:
    def __init__(self, depth):
        me = lax.axis_index("dp")
        self.depth = depth
        self.core = me % 2
        self.x = (me // 2) % 2
        self.y = (me // 4) % 2
        self.z = me // 8

    def index(self, z, y, x, core):
        return ((z * 2 + y) * 2 + x) * 2 + core

    def ahead(self, k):
        return (self.z + k) % self.depth

    def back(self, k):
        return (self.z + self.depth - k) % self.depth

    def twin(self):
        return self.index(self.z, self.y, self.x, 1 - self.core)

    def x_mate(self):
        return self.index(self.z, self.y, 1 - self.x, self.core)

    def y_mate(self):
        return self.index(self.z, 1 - self.y, self.x, self.core)

    def z_mate(self, k):
        return self.index(self.ahead(k), self.y, self.x, self.core)

    def greet(self):
        barrier = pltpu.get_barrier_semaphore()
        mates = [self.twin(), self.x_mate(), self.y_mate()]
        mates += [self.z_mate(k) for k in range(1, self.depth)]
        for mate in mates:
            pl.semaphore_signal(barrier, inc=1, device_id=(mate,), device_id_type=MESH)
        pl.semaphore_wait(barrier, len(mates))


def send(source, target, send_sem, recv_sem, device):
    return pltpu.make_async_remote_copy(
        src_ref=source,
        dst_ref=target,
        send_sem=send_sem,
        recv_sem=recv_sem,
        device_id=(device,),
        device_id_type=MESH,
    )


class Gather:
    BY_Z, BY_X, BY_Y, UPPER, LOWER, OWN, FROM_X, FROM_Y, CROSS = range(9)

    def __init__(self, place, blocks, full, send_sems, recv_sems, local_sems):
        self.place = place
        self.blocks = blocks
        self.full = full
        self.sems = (send_sems, recv_sems)
        self.local_sems = local_sems
        self.depth = place.depth

    def home(self, w):
        p = self.place
        return self.full[w].at[p.z, p.y, p.x, p.core]

    def copy(self, w, k, kind):
        p, full = self.place, self.full[w]
        half = self.blocks[w].shape[0] // 2
        sems = [sem.at[w, k, kind] for sem in self.sems]
        zz = p.back(k)
        if kind == self.BY_Z:
            return send(self.blocks[w], self.home(w), *sems, p.z_mate(k))
        if kind in (self.BY_X, self.BY_Y, self.OWN):
            block = full.at[zz, p.y, p.x, p.core]
            source = self.blocks[w] if k == 0 else block
            mate = {self.BY_X: p.x_mate, self.BY_Y: p.y_mate, self.OWN: p.twin}[kind]()
            return send(source, block, *sems, mate)
        if kind == self.UPPER:
            block = full.at[zz, p.y, 1 - p.x, p.core, pl.ds(0, half)]
            return send(block, block, *sems, p.y_mate())
        if kind == self.LOWER:
            block = full.at[zz, 1 - p.y, p.x, p.core, pl.ds(half, half)]
            return send(block, block, *sems, p.x_mate())
        if kind == self.FROM_X:
            block = full.at[zz, p.y, 1 - p.x, p.core]
        elif kind == self.FROM_Y:
            block = full.at[zz, 1 - p.y, p.x, p.core]
        else:
            block = full.at[zz, 1 - p.y, 1 - p.x, p.core]
        return send(block, block, *sems, p.twin())

    def local(self, w):
        return pltpu.make_async_copy(self.blocks[w], self.home(w), self.local_sems.at[w])

    def start(self, w):
        for k in range(1, self.depth):
            self.copy(w, k, self.BY_Z).start()
        self.local(w).start()

    def spread(self, w, k):
        if k:
            self.copy(w, k, self.BY_Z).wait_recv()
        for kind in (self.BY_X, self.BY_Y, self.OWN):
            self.copy(w, k, kind).start()

    def relay(self, w, k):
        self.copy(w, k, self.BY_X).wait_recv()
        self.copy(w, k, self.UPPER).start()
        self.copy(w, k, self.FROM_X).start()
        self.copy(w, k, self.BY_Y).wait_recv()
        self.copy(w, k, self.LOWER).start()
        self.copy(w, k, self.FROM_Y).start()

    def hand_over(self, w, k):
        self.copy(w, k, self.UPPER).wait_recv()
        self.copy(w, k, self.LOWER).wait_recv()
        self.copy(w, k, self.CROSS).start()

    def receive(self, w, k):
        if k == 0:
            self.local(w).wait()
        for kind in (self.OWN, self.FROM_X, self.FROM_Y, self.CROSS):
            self.copy(w, k, kind).wait_recv()

    def receive_all(self, w):
        for k in range(self.depth):
            self.receive(w, k)

    def sent(self, w):
        for k in range(self.depth):
            for kind in range(9):
                if kind != self.BY_Z or k:
                    self.copy(w, k, kind).wait_send()

    def sent_all(self):
        for w in range(len(self.blocks)):
            self.sent(w)

    def step(self, units, t):
        lag = self.depth
        if t < len(units):
            self.spread(*units[t])
        if 0 <= t - lag < len(units):
            self.relay(*units[t - lag])
        if 0 <= t - 2 * lag < len(units):
            self.hand_over(*units[t - 2 * lag])

    def units(self):
        return [(w, k) for w in range(len(self.blocks)) for k in range(self.depth)]

    def start_all(self):
        for w in range(len(self.blocks)):
            self.start(w)

def gather_sems(count, depth):
    return [
        pltpu.SemaphoreType.DMA((count, depth, 9)),
        pltpu.SemaphoreType.DMA((count, depth, 9)),
        pltpu.SemaphoreType.DMA((count,)),
    ]


class Scatter:
    TWIN, UPPER_Y, LOWER_X, UPPER_X, LOWER_Y, BY_Z = range(6)

    def __init__(self, place, grads, out, bufs, send_sems, recv_sems, local_sems, resident=()):
        self.place = place
        self.resident = resident
        self.grads = grads
        self.out = out
        self.bufs = bufs
        self.sems = (send_sems, recv_sems)
        self.local_sems = local_sems
        self.depth = place.depth
        self.order = list(range(1, self.depth)) + [0]

    def load(self, w, k):
        p = self.place
        return pltpu.make_async_copy(
            self.grads[w].at[p.ahead(k), :, :, p.core],
            self.bufs[w][6].at[k],
            self.local_sems.at[w, k],
        )

    def sums(self, w, k):
        if w in self.resident:
            return self.grads[w].at[self.place.ahead(k), :, :, self.place.core]
        return self.bufs[w][6].at[k]

    def half(self, w):
        return self.grads[w].shape[-2] // 2

    def copy(self, w, k, kind):
        p = self.place
        twin, upper_y, lower_x, upper_x, lower_y, by_z = self.bufs[w][:6]
        sums, half = self.sums(w, k), self.half(w)
        sems = [sem.at[w, k, kind] for sem in self.sems]
        top, bottom = pl.ds(0, half), pl.ds(half, half)
        if kind == self.TWIN:
            source = self.grads[w].at[p.ahead(k), :, :, 1 - p.core]
            return send(source, twin.at[k], *sems, p.twin())
        if kind == self.UPPER_Y:
            return send(sums.at[1 - p.y, :, top], upper_y.at[k], *sems, p.y_mate())
        if kind == self.LOWER_X:
            return send(sums.at[:, 1 - p.x, bottom], lower_x.at[k], *sems, p.x_mate())
        if kind == self.UPPER_X:
            return send(sums.at[p.y, 1 - p.x, top], upper_x.at[k], *sems, p.x_mate())
        if kind == self.LOWER_Y:
            return send(sums.at[1 - p.y, p.x, bottom], lower_y.at[k], *sems, p.y_mate())
        return send(sums.at[p.y, p.x], by_z.at[k], *sems, p.z_mate(k))

    @staticmethod
    def add(target, extra):
        target[...] = target[...] + extra[...]

    def start(self, w):
        for k in self.order:
            self.begin(w, k)

    def begin(self, w, k):
        self.copy(w, k, self.TWIN).start()
        if w not in self.resident:
            self.load(w, k).start()

    def first(self, w, k):
        sums, twin = self.sums(w, k), self.bufs[w][0]
        if w not in self.resident:
            self.load(w, k).wait()
        self.copy(w, k, self.TWIN).wait_recv()

        def body(i, carry):
            self.add(sums.at[i // 2, i % 2], twin.at[k, i // 2, i % 2])
            return carry

        lax.fori_loop(0, 4, body, 0)
        self.copy(w, k, self.UPPER_Y).start()
        self.copy(w, k, self.LOWER_X).start()

    def second(self, w, k):
        p = self.place
        sums, half = self.sums(w, k), self.half(w)
        upper_y, lower_x = self.bufs[w][1:3]
        self.copy(w, k, self.UPPER_Y).wait_recv()
        self.copy(w, k, self.LOWER_X).wait_recv()

        def body(i, carry):
            self.add(sums.at[p.y, i, pl.ds(0, half)], upper_y.at[k, i])
            self.add(sums.at[i, p.x, pl.ds(half, half)], lower_x.at[k, i])
            return carry

        lax.fori_loop(0, 2, body, 0)
        self.copy(w, k, self.UPPER_X).start()
        self.copy(w, k, self.LOWER_Y).start()

    def third(self, w, k):
        p = self.place
        sums, half = self.sums(w, k), self.half(w)
        upper_x, lower_y = self.bufs[w][3:5]
        self.copy(w, k, self.UPPER_X).wait_recv()
        self.copy(w, k, self.LOWER_Y).wait_recv()
        self.add(sums.at[p.y, p.x, pl.ds(0, half)], upper_x.at[k])
        self.add(sums.at[p.y, p.x, pl.ds(half, half)], lower_y.at[k])
        if isinstance(k, int):
            if k:
                self.copy(w, k, self.BY_Z).start()
        else:
            pl.when(k != 0)(lambda: self.copy(w, k, self.BY_Z).start())

    def finish(self, w):
        p = self.place
        by_z = self.bufs[w][5]
        for k in range(1, self.depth):
            self.copy(w, k, self.BY_Z).wait_recv()
        total = self.sums(w, 0)[p.y, p.x].astype(F32)
        for k in range(1, self.depth):
            total = total + by_z[k].astype(F32)
        self.out[w][...] = total
        for k in range(self.depth):
            for kind in range(6):
                if kind != self.BY_Z or k:
                    self.copy(w, k, kind).wait_send()


BUFS = 7


def scatter_scratch(grads, depth, resident=()):
    scratch = []
    for w, grad in enumerate(grads):
        rows, columns = grad.shape[-2:]
        half = rows // 2
        shapes = [(depth, 2, 2, rows, columns)]
        shapes += [(depth, 2, half, columns)] * 2 + [(depth, half, columns)] * 2
        shapes += [(depth, rows, columns)]
        shapes += [(8, LANES) if w in resident else (depth, 2, 2, rows, columns)]
        scratch += [pltpu.VMEM(shape, grad.dtype) for shape in shapes]
    count = len(grads)
    scratch += [pltpu.SemaphoreType.DMA((count, depth, 6))] * 2
    return scratch + [pltpu.SemaphoreType.DMA((count, depth))]


def own_lanes(head):
    lane = lax.broadcasted_iota(jnp.int32, (1, LANES), 1)
    return (lane < HEAD_DIM) == (head == 0)


def fill_masks(ids_row, ids_column, masks):
    for b in range(masks.shape[0]):
        masks[b] = jnp.where(ids_column[b] == ids_row[b], 0.0, MASK_FILL).astype(F32)


def at_step(t, work):
    pl.when(pl.program_id(0) * pl.num_programs(1) + pl.program_id(1) == t)(work)


GROUPS = 4
GROUP_PAIRS = PAIRS // GROUPS
GROUP_WIDTH = 3 * LANES * GROUP_PAIRS


def rows_of(block):
    return block.reshape(-1, block.shape[-1])


def attend_kernel(depth, count, seqs, per, *refs):
    ids_row, ids_column, tokens = refs[:3]
    if depth:
        blocks, refs = refs[3 : 3 + count], refs[3 + count :]
        qkv, attended, log_total, whole_qkv, whole_vector = refs[:5]
        riders, refs = refs[5 : 5 + count - GROUPS], refs[5 + count - GROUPS :]
        masks, bias, store, refs = refs[0], refs[1], refs[2], refs[3:]
        groups = [
            store.at[g, :, :, :, :, :, pl.ds(0, blocks[g].shape[1])] for g in range(GROUPS)
        ]
        place = Place(depth)
        side = Gather(place, blocks, [*groups, *riders], *refs[:3])
        out_sems = refs[3]
        units = side.units()

        def out_copy(g):
            columns = pl.ds(0, GROUP_WIDTH)
            target = pl.ds(g * GROUP_WIDTH, GROUP_WIDTH)
            return pltpu.make_async_copy(
                groups[g].at[:, :, :, :, :, columns],
                whole_qkv.at[:, :, :, :, :, target],
                out_sems.at[g],
            )

        vector_copy = pltpu.make_async_copy(
            groups[0].at[:, :, :, :, :, pl.ds(GROUP_WIDTH, LANES)], whole_vector, out_sems.at[GROUPS]
        )

        def open_up():
            place.greet()
            side.start_all()
            for t in range(3 * depth):
                side.step(units, t)
            side.receive_all(0)
            out_copy(0).start()
            vector_copy.start()
            for r in range(2 * PAIRS):
                d, j = r // per, r % per
                spot = (d // 8, d // 4 % 2, d // 2 % 2, d % 2)
                row = store[(0, *spot, slice(j, j + 1), slice(GROUP_WIDTH, GROUP_WIDTH + LANES))]
                bias[r] = row.astype(F32)

        at_step(0, open_up)
        steps = seqs * GROUP_PAIRS

        def each(work, w):
            for k in range(depth):
                work(w, k)

        def ready(g):
            side.receive_all(g)
            out_copy(g).start()

        steps = seqs * PAIRS
        plan = [[] for _ in range(steps)]

        def put(i, work, *what):
            plan[min(i, steps - 1)].append(functools.partial(work, *what))

        proj, up = GROUPS, GROUPS + 1
        put(1, each, side.spread, 3)
        put(2, each, side.hand_over, 1)
        put(2, each, side.relay, 2)
        put(3, each, side.spread, proj)
        put(steps // GROUPS, ready, 1)
        put(5, each, side.relay, 3)
        put(6, each, side.hand_over, 2)
        put(7, each, side.relay, proj)
        put(2 * steps // GROUPS, ready, 2)
        put(8, each, side.hand_over, 3)
        put(9, each, side.hand_over, proj)
        put(3 * steps // GROUPS, ready, 3)
        for k in range(depth):
            put(4 + k, side.spread, up, k)
            put(8 + k, side.relay, up, k)
            put(11 + k, side.hand_over, up, k)
        for i in range(1, steps):

            def more(i=i):
                for work in plan[i]:
                    work()

            if plan[i]:
                at_step(i, more)
    else:
        weight, bias, qkv, attended, log_total, masks = refs[3:]
    at_step(0, lambda: fill_masks(ids_row, ids_column, masks))
    h, b = pl.program_id(0), pl.program_id(1)
    length = masks.shape[1]
    rows = tokens[pl.ds(pl.multiple_of(b * length, length), length), :]
    if depth:
        shifts = [bias[h], jnp.zeros((1, LANES), F32), bias[PAIRS + h]]
        shift = jnp.concatenate(shifts, axis=1)
        columns = pl.ds(pl.multiple_of((h % GROUP_PAIRS) * 3 * LANES, 3 * LANES), 3 * LANES)
        weight = rows_of(store[h // GROUP_PAIRS, :, :, :, :, :, columns])
        qkv[...] = (dot_over(rows, weight, 1, 0) + shift).astype(BF16)
    else:
        qkv[...] = (dot_over(rows, weight[...], 1, 0) + bias[0]).astype(BF16)
    query = qkv[:, 0:LANES] * BF16(SCALE)
    key = qkv[:, LANES : 2 * LANES]
    value = qkv[:, 2 * LANES : 3 * LANES]
    chunk = length // 2
    outs = []
    for head in range(2):
        own_key = jnp.where(own_lanes(head), key, BF16(0))
        parts = []
        for at in range(0, length, chunk):
            scores = dot_over(own_key, query[at : at + chunk], 1, 1)
            scores = scores + masks[b, :, at : at + chunk]
            top = jnp.max(scores, axis=0, keepdims=True)
            weights = jnp.exp(scores - top)
            total = jnp.sum(weights, axis=0, keepdims=True)
            log_total[0, 0, head : head + 1, at : at + chunk] = top + jnp.log(total)
            probs = (weights * (1.0 / total)).astype(BF16)
            parts.append(dot_over(probs, value, 0, 0))
        outs.append(jnp.concatenate(parts, axis=0))
    attended[...] = jnp.where(own_lanes(0), outs[0], outs[1]).astype(BF16)
    if depth:

        def close():
            for w in range(GROUPS, count):
                side.receive_all(w)
            side.sent_all()
            vector_copy.wait()
            for g in range(GROUPS):
                out_copy(g).wait()

        at_step(seqs * PAIRS - 1, close)


def attend_back_kernel(depth, seqs, per_device, *refs):
    ids_row, ids_column, tokens, qkv, attended_grad, log_total, weight, hidden_grad = refs[:8]
    steps = seqs * PAIRS
    i = pl.program_id(0)
    last = pl.num_programs(0) - 1
    spot = jnp.minimum(i, steps - 1)
    h, b = spot // seqs, spot % seqs
    if depth:
        up_grad, proj_grad, vector_part, input_grad = refs[8:12]
        out, refs = refs[12 : 15 + GROUPS], refs[15 + GROUPS :]
        masks, kept, total, sums, vector, *refs = refs
        groups, refs = refs[:GROUPS], refs[GROUPS:]
        grads = [up_grad, proj_grad, *groups, vector]
        count = len(grads)
        bufs = [refs[BUFS * w : BUFS * w + BUFS] for w in range(count)]
        place = Place(depth)
        side = Scatter(place, grads, out, bufs, *refs[BUFS * count :], resident=range(2, count))
        plan = [[] for _ in range(steps + tokens.shape[0] // ROW_BLOCK)]

        def put(at, work, *what):
            plan[min(at, len(plan) - 1)].append(functools.partial(work, *what))

        def each(work, w):
            def body(k, carry):
                work(w, k)
                return carry

            lax.fori_loop(0, depth, body, 0)

        up, proj, vec = 0, 1, count - 1
        put(0, place.greet)
        put(0, side.start, up)
        put(0, side.start, proj)
        for n, k in enumerate(side.order):
            put(1 + 2 * n, side.first, up, k)
            put(4 + 2 * n + n // 2, side.second, up, k)
            put(7 + 2 * n + n // 2, side.third, up, k)
        put(2, each, side.first, proj)
        put(5, each, side.second, proj)
        put(8, each, side.third, proj)
        per = steps // GROUPS
        for g in range(GROUPS):
            at = per * (g + 1)
            put(at, each, side.begin, 2 + g)
            put(at + 1, each, side.first, 2 + g)
            put(at + min(4, GROUPS + 1 - g), each, side.second, 2 + g)
            put(at + min(7, GROUPS + 2 - g), each, side.third, 2 + g)
        rows_each = per_device

        def make_vector():
            vector[...] = vector_part[...]
            for r in range(2 * PAIRS):
                d, j = r // rows_each, r % rows_each
                source = 0 if r < PAIRS else 2 * LANES
                row = sums[r % PAIRS, :, source : source + LANES]
                vector[d // 8, d // 4 % 2, d // 2 % 2, d % 2, j : j + 1, :] = row

        put(steps, make_vector)
        put(steps + 1, each, side.begin, vec)
        put(steps + 2, each, side.first, vec)
        put(steps + 3, each, side.second, vec)
        for at, works in enumerate(plan):

            def run(works=works):
                for work in works:
                    work()

            if works:
                pl.when(i == at)(run)
    else:
        input_grad, weight_grads, sums, masks, kept, total = refs[8:]
    pl.when(i == 0)(lambda: fill_masks(ids_row, ids_column, masks))
    length = qkv.shape[0]
    chunk = length
    wide = pl.ds(pl.multiple_of(h * 3 * LANES, 3 * LANES), 3 * LANES)
    tall = pl.ds(pl.multiple_of(b * length, length), length)

    @pl.when(i < steps)
    def _():
        query = qkv[:, 0:LANES]
        key = qkv[:, LANES : 2 * LANES]
        value = qkv[:, 2 * LANES : 3 * LANES]
        grad = attended_grad[...]
        scaled = query * BF16(SCALE)
        query_grads, key_grads, value_grads = [], [], []
        for head in range(2):
            own_key = jnp.where(own_lanes(head), key, BF16(0))
            own_value = jnp.where(own_lanes(head), value, BF16(0))
            key_grad = value_grad = None
            parts = []
            for at in range(0, length, chunk):
                piece = slice(at, at + chunk)
                scores = dot_over(own_key, scaled[piece], 1, 1) + masks[b, :, piece]
                probs = jnp.exp(scores - log_total[0, 0, head : head + 1, piece])
                prob_grad = dot_over(own_value, grad[piece], 1, 1)
                row_dot = jnp.sum(probs * prob_grad, axis=0, keepdims=True)
                score_grad = (probs * (prob_grad - row_dot)).astype(BF16)
                value_part = dot_over(probs.astype(BF16), grad[piece], 1, 0)
                key_part = dot_over(score_grad, query[piece], 1, 0)
                value_grad = value_part if value_grad is None else value_grad + value_part
                key_grad = key_part if key_grad is None else key_grad + key_part
                parts.append(dot_over(score_grad, key, 0, 0))
            query_grads.append(jnp.concatenate(parts, axis=0))
            key_grads.append(key_grad)
            value_grads.append(value_grad)
        first = own_lanes(0)
        own = [
            (jnp.where(first, *query_grads) * SCALE).astype(BF16),
            (jnp.where(first, *key_grads) * SCALE).astype(BF16),
            jnp.where(first, *value_grads).astype(BF16),
        ]
        rows_grad = jnp.concatenate(own, axis=1)
        kept[tall, wide] = rows_grad
        part = dot_over(tokens[tall, :], rows_grad, 0, 0)
        part_sums = jnp.sum(rows_grad.astype(F32), axis=0, keepdims=True)

        @pl.when(b == 0)
        def _():
            total[...] = part
            sums[h] = part_sums

        @pl.when(b > 0)
        def _():
            total[...] += part
            sums[h] += part_sums

        @pl.when(b == seqs - 1)
        def _():
            if depth:
                where = (h % GROUP_PAIRS) * 3 * LANES
                columns = pl.ds(pl.multiple_of(where, 3 * LANES), 3 * LANES)
                for g in range(GROUPS):

                    @pl.when(h // GROUP_PAIRS == g)
                    def _():
                        shape = groups[g].shape[:5] + (3 * LANES,)
                        groups[g][:, :, :, :, :, columns] = total[...].astype(BF16).reshape(shape)
            else:
                weight_grads[...] = total[...]

    @pl.when(i >= steps)
    def _():
        at = pl.multiple_of((i - steps) * ROW_BLOCK, ROW_BLOCK)
        back = dot_over(kept[pl.ds(at, ROW_BLOCK), :], weight[...], 1, 1)
        input_grad[...] = (back + hidden_grad[...]).astype(BF16)

    if depth:

        @pl.when(i == last)
        def _():
            each(side.third, vec)
            for w in range(count):
                side.finish(w)


def whole(shape):
    return pl.BlockSpec(shape, lambda h, b: (0,) * len(shape))


def attention_specs(count, length):
    rows = whole((count, 1, length))
    columns = whole((count, length, 1))
    tokens = whole((count * length, D))
    wide = pl.BlockSpec((length, 3 * LANES), lambda h, b: (b, h))
    one = pl.BlockSpec((length, LANES), lambda h, b: (b, h))
    log_total = pl.BlockSpec((1, 1, 2, length), lambda h, b: (b, h, 0, 0))
    weight = pl.BlockSpec((D, 3 * LANES), lambda h, b: (0, h))
    vector = pl.BlockSpec((1, 1, 3 * LANES), lambda h, b: (h, 0, 0))
    return rows, columns, tokens, wide, one, log_total, weight, vector


def kernel_params(collective_id, remote, limit=60 << 20):
    if not remote:
        return pltpu.CompilerParams(vmem_limit_bytes=limit)
    return pltpu.CompilerParams(
        collective_id=collective_id, has_side_effects=True, vmem_limit_bytes=limit
    )


def attend(tokens, doc_ids, weight, bias, blocks, per, depth, collective_id):
    count, length = doc_ids.shape
    rows, columns, all_tokens, wide, one, log_total, part, vector = attention_specs(count, length)
    in_place = pl.BlockSpec(memory_space=pl.ANY)
    out_shape = [
        jax.ShapeDtypeStruct((count * length, 3 * D), BF16),
        jax.ShapeDtypeStruct((count * length, D), BF16),
        jax.ShapeDtypeStruct((count, PAIRS, 2, length), F32),
    ]
    out_specs = [wide, one, log_total]
    in_specs = [rows, columns, all_tokens]
    scratch = [pltpu.VMEM((count, length, length), F32)]
    grid3 = (depth, 2, 2, 2)
    if depth:
        in_specs += [whole(b.shape) for b in blocks]
        tall = blocks[0].shape[0]
        shapes = [(*grid3, tall, 3 * D), (*grid3, tall, LANES)]
        shapes += [grid3 + b.shape for b in blocks[GROUPS:]]
        out_shape += [jax.ShapeDtypeStruct(shape, BF16) for shape in shapes]
        out_specs += [in_place] * len(shapes)
        scratch += [pltpu.VMEM((2 * PAIRS, 1, LANES), F32)]
        scratch += [pltpu.VMEM((GROUPS, *grid3, *blocks[0].shape), BF16)]
        scratch += gather_sems(len(blocks), depth) + [pltpu.SemaphoreType.DMA((GROUPS + 1,))]
        operands = blocks
    else:
        in_specs += [part, vector]
        operands = [weight, bias.reshape(PAIRS, 1, 3 * LANES)]
    return pl.pallas_call(
        functools.partial(attend_kernel, depth, len(blocks), count, per),
        grid=(PAIRS, count),
        in_specs=in_specs,
        out_specs=out_specs,
        out_shape=out_shape,
        scratch_shapes=scratch,
        compiler_params=kernel_params(collective_id, len(blocks)),
        name="attend",
    )(
        doc_ids.reshape(count, 1, length),
        doc_ids.reshape(count, length, 1),
        tokens,
        *operands,
    )


def attend_back(
    tokens, qkv, doc_ids, attended_grad, totals, weight, hidden_grad, grads, per_device, depth, collective_id
):
    seqs, length = doc_ids.shape
    steps = seqs * PAIRS
    blocks = seqs * length // ROW_BLOCK

    def h(i):
        return jnp.minimum(i, steps - 1) // seqs

    def b(i):
        return jnp.minimum(i, steps - 1) % seqs

    def late(i):
        return jnp.maximum(i - steps, 0)

    in_place = pl.BlockSpec(memory_space=pl.ANY)
    in_specs = [
        once((seqs, 1, length)),
        once((seqs, length, 1)),
        once((seqs * length, D)),
        pl.BlockSpec((length, 3 * LANES), lambda i: (b(i), h(i))),
        pl.BlockSpec((length, LANES), lambda i: (b(i), h(i))),
        pl.BlockSpec((1, 1, 2, length), lambda i: (b(i), h(i), 0, 0)),
        once((D, 3 * D)),
        pl.BlockSpec((ROW_BLOCK, D), lambda i: (late(i), 0)),
    ]
    out_specs = [pl.BlockSpec((ROW_BLOCK, D), lambda i: (late(i), 0))]
    out_shape = [jax.ShapeDtypeStruct((seqs * length, D), BF16)]
    scratch = [
        pltpu.VMEM((seqs, length, length), F32),
        pltpu.VMEM((seqs * length, 3 * D), BF16),
        pltpu.VMEM((D, 3 * LANES), F32),
    ]
    if depth:
        up_grad, proj_grad, vector = grads
        tall = up_grad.shape[-2]
        group = jax.ShapeDtypeStruct((depth, 2, 2, 2, tall, GROUP_WIDTH), BF16)
        moved = [up_grad, proj_grad, *([group] * GROUPS), vector]
        in_specs += [in_place, in_place, flat(vector.shape)]
        out_specs += [flat(m.shape[-2:]) for m in moved]
        out_shape += [jax.ShapeDtypeStruct(m.shape[-2:], F32) for m in moved]
        scratch += [pltpu.VMEM((PAIRS, 1, 3 * LANES), F32), pltpu.VMEM(vector.shape, F32)]
        scratch += [pltpu.VMEM(group.shape, BF16)] * GROUPS
        scratch += scatter_scratch(moved, depth, resident=range(2, len(moved)))
    else:
        out_specs += [
            pl.BlockSpec((D, 3 * LANES), lambda i: (0, h(i))),
            flat((PAIRS, 1, 3 * LANES)),
        ]
        out_shape += [
            jax.ShapeDtypeStruct((D, 3 * D), F32),
            jax.ShapeDtypeStruct((PAIRS, 1, 3 * LANES), F32),
        ]
    return pl.pallas_call(
        functools.partial(attend_back_kernel, depth, seqs, per_device),
        grid=(steps + blocks,),
        in_specs=in_specs,
        out_specs=out_specs,
        out_shape=out_shape,
        scratch_shapes=scratch,
        compiler_params=kernel_params(collective_id, depth, 63 << 20),
        name="attend_back",
    )(
        doc_ids.reshape(seqs, 1, length),
        doc_ids.reshape(seqs, length, 1),
        tokens,
        qkv,
        attended_grad,
        totals,
        weight,
        hidden_grad,
        *grads,
    )


TILE = 512
ROW_CHUNK = 256


def widen_kernel(depth, tiles, *refs):
    low, up_weight, up_bias, normed, scales = refs[:5]
    blocks = refs[5:7]
    activated, slope, second_in, whole_up, whole_down = refs[7:12]
    kept, tile_weight, late_up, down, out_sems, *sems = refs[12:]
    place = Place(depth)
    side = Gather(place, blocks, [late_up, down], *sems)
    i = pl.program_id(0)
    per = tiles // depth
    half = tiles // 2

    def out_copy(k):
        zz = place.back(k)
        return pltpu.make_async_copy(down.at[zz], whole_down.at[zz], out_sems.at[k])

    up_copy = pltpu.make_async_copy(late_up, whole_up, out_sems.at[depth])
    plan = [[] for _ in range(tiles + depth)]

    def put(at, work, *what):
        plan[min(at, len(plan) - 1)].append(functools.partial(work, *what))

    put(0, place.greet)
    put(0, side.start_all)
    for k in range(depth):
        put(min(k, half - 1), side.spread, 0, k)
        put(min(k + 2, half), side.relay, 0, k)
    put(half, side.spread, 1, 0)
    put(half, side.spread, 1, 1)
    for k in range(depth):
        put(half, side.hand_over, 0, k)
    put(half, side.receive_all, 0)
    put(half, up_copy.start)
    put(half + 1, side.relay, 1, 0)
    for k in range(2, depth):
        put(half + 2 * k - 2, side.spread, 1, k)
    for k in range(1, depth - 1):
        put(half + 1 + 2 * k, side.relay, 1, k)
    put(tiles + depth - 2, side.relay, 1, depth - 1)
    for k in range(depth):
        put(tiles + k, side.hand_over, 1, k)
    for at, works in enumerate(plan):

        def run(works=works):
            for work in works:
                work()

        if works:
            pl.when(i == at)(run)

    @pl.when(i < half)
    def _():
        tile_weight[...] = up_weight[...]

    @pl.when((i >= half) & (i < tiles))
    def _():
        columns = pl.ds(pl.multiple_of((i - half) * TILE, TILE), TILE)
        tile_weight[...] = rows_of(late_up[:, :, :, :, :, columns])

    @pl.when(i < tiles)
    def _():
        for at in range(0, low.shape[0], ROW_CHUNK):
            rows = slice(at, at + ROW_CHUNK)
            upward = dot_over(low[rows, :], tile_weight[...], 1, 0) + up_bias[...]
            cdf = 0.5 * (1.0 + lax.erf(upward * HALF_ROOT))
            value = (upward * cdf).astype(BF16)
            activated[rows, :] = value
            kept[i, rows, :] = value
            slope[rows, :] = cdf + upward * (PDF_TOP * jnp.exp(-0.5 * upward * upward))

    for k in range(depth):

        def layer(k=k):
            side.receive(1, k)
            out_copy(k).start()
            zz = place.back(k)
            for at in range(0, low.shape[0], ROW_CHUNK):
                rows = slice(at, at + ROW_CHUNK)
                if k == 0:
                    total = normed[rows, :] * scales[0:1, :] + scales[1:2, :] + scales[2:3, :]
                else:
                    total = second_in[rows, :]
                for n in range(per):
                    tile = kept[zz * per + n, rows, :]
                    weight = rows_of(down[zz, n * 2 // per : (n + 1) * 2 // per])
                    total = total + dot_over(tile, weight, 1, 0)
                second_in[rows, :] = total

        pl.when(i == tiles + k)(layer)

    @pl.when(i == tiles + depth - 1)
    def _():
        side.sent_all()
        up_copy.wait()
        for k in range(depth):
            out_copy(k).wait()


def flat(shape):
    return pl.BlockSpec(shape, lambda i: (0,) * len(shape))


def once(shape):
    return pl.BlockSpec(shape, lambda i: (0,) * len(shape), pipeline_mode=pl.Buffered(1))


def widen(low, up_weight, up_bias, normed, scales, blocks, depth, collective_id):
    count = low.shape[0]
    tiles = FF // TILE
    last, half = tiles - 1, tiles // 2
    tile = pl.BlockSpec((count, TILE), lambda i: (0, jnp.minimum(i, last)))
    spread = [(depth, 2, 2, 2) + block.shape for block in blocks]
    in_place = pl.BlockSpec(memory_space=pl.ANY)
    return pl.pallas_call(
        functools.partial(widen_kernel, depth, tiles),
        grid=(tiles + depth,),
        in_specs=[
            once(low.shape),
            pl.BlockSpec((D, TILE), lambda i: (0, jnp.minimum(i, half - 1))),
            pl.BlockSpec((1, TILE), lambda i: (0, jnp.minimum(i, last))),
            once(normed.shape),
            once(scales.shape),
            *[once(block.shape) for block in blocks],
        ],
        out_specs=[tile, tile, flat((count, D)), in_place, in_place],
        out_shape=[
            jax.ShapeDtypeStruct((count, FF), BF16),
            jax.ShapeDtypeStruct((count, FF), F32),
            jax.ShapeDtypeStruct((count, D), F32),
            *[jax.ShapeDtypeStruct(shape, BF16) for shape in spread],
        ],
        scratch_shapes=[
            pltpu.VMEM((tiles, count, TILE), BF16),
            pltpu.VMEM((D, TILE), BF16),
            *[pltpu.VMEM(shape, BF16) for shape in spread],
            pltpu.SemaphoreType.DMA((depth + 1,)),
            *gather_sems(2, depth),
        ],
        compiler_params=kernel_params(collective_id, 1),
        name="widen",
    )(low, up_weight, up_bias[None], normed, scales, *blocks)


def early_tile(i, tiles, depth):
    ahead = (lax.axis_index("dp") // 8 + 1) * (tiles // depth)
    return (jnp.minimum(i, tiles - 1) + ahead) % tiles


def widen_back_kernel(depth, tiles, *refs):
    rows_grad, activated, slope, down_weight, low_turned, up_early, up_late = refs[:7]
    up_grad, branch_grad, sums, down_out = refs[7:11]
    kept, down_grad, total, *rest = refs[11:]
    place = Place(depth)
    side = Scatter(place, [down_grad], [down_out], [rest[:BUFS]], *rest[BUFS:], resident=(0,))
    i = pl.program_id(0)
    per = tiles // depth

    def step_of(t, work):
        pl.when(i == t)(work)

    step_of(0, place.greet)
    now = early_tile(i, tiles, depth)
    for n, k in enumerate(side.order):
        ready = (n + 1) * per
        step_of(ready, functools.partial(side.begin, 0, k))
        step_of(ready + 1, functools.partial(side.first, 0, k))
        step_of(ready + 3, functools.partial(side.second, 0, k))
        step_of(ready + 5, functools.partial(side.third, 0, k))

    @pl.when(i < tiles)
    def _():
        for at in range(0, rows_grad.shape[0], ROW_CHUNK):
            rows = slice(at, at + ROW_CHUNK)
            back = dot_over(rows_grad[rows, :], down_weight[...], 1, 1)
            kept[now, rows, :] = (back * slope[rows, :]).astype(BF16)
        sums[0] = jnp.sum(kept[now].astype(F32), axis=0, keepdims=True)
        grad = dot_over(activated[...], rows_grad[...], 0, 0).astype(BF16)
        blocks = TILE // down_grad.shape[4]
        grad = grad.reshape(1, blocks // 4, 2, 2, down_grad.shape[4], D)[0]
        part = pl.ds((now % per) * (blocks // 4), blocks // 4)
        down_grad[now // per, part] = grad

    @pl.when(i >= tiles)
    def _():
        tile = kept[i - tiles]
        up_grad[...] = dot_over(low_turned[...], tile, 1, 0).astype(BF16)
        up_weight = jnp.where(i - tiles < tiles // 2, up_early[...], up_late[...])
        for at in range(0, rows_grad.shape[0], ROW_CHUNK):
            rows = slice(at, at + ROW_CHUNK)
            part = dot_over(tile[rows, :], up_weight, 1, 1)

            @pl.when(i == tiles)
            def _():
                total[rows, :] = part

            @pl.when(i > tiles)
            def _():
                total[rows, :] += part

    @pl.when(i == 2 * tiles - 1)
    def _():
        branch_grad[...] = total[...]
        side.finish(0)


def widen_back(
    rows_grad, activated, slope, down_weight, low_turned, up_early, up_late, depth, collective_id
):
    count = rows_grad.shape[0]
    tiles = FF // TILE

    half = tiles // 2

    def early(i):
        return early_tile(i, tiles, depth)

    def late(i):
        return jnp.maximum(i - tiles, 0)

    shares = 8 * depth
    spread = jax.ShapeDtypeStruct((depth, 2, 2, 2, FF // shares, D), BF16)
    return pl.pallas_call(
        functools.partial(widen_back_kernel, depth, tiles),
        grid=(2 * tiles,),
        in_specs=[
            once(rows_grad.shape),
            pl.BlockSpec((count, TILE), lambda i: (0, early(i))),
            pl.BlockSpec((count, TILE), lambda i: (0, early(i))),
            pl.BlockSpec((TILE, D), lambda i: (early(i), 0)),
            once(low_turned.shape),
            pl.BlockSpec((D, TILE), lambda i: (0, jnp.minimum(late(i), half - 1))),
            pl.BlockSpec((D, TILE), lambda i: (0, jnp.maximum(late(i) - half, 0))),
        ],
        out_specs=[
            pl.BlockSpec((D, TILE), lambda i: (0, late(i))),
            flat((count, D)),
            pl.BlockSpec((1, 1, TILE), lambda i: (early(i), 0, 0)),
            flat(spread.shape[-2:]),
        ],
        out_shape=[
            jax.ShapeDtypeStruct((D, FF), BF16),
            jax.ShapeDtypeStruct((count, D), F32),
            jax.ShapeDtypeStruct((tiles, 1, TILE), F32),
            jax.ShapeDtypeStruct(spread.shape[-2:], F32),
        ],
        scratch_shapes=[
            pltpu.VMEM((tiles, count, TILE), BF16),
            pltpu.VMEM(spread.shape, BF16),
            pltpu.VMEM((count, D), F32),
            *scatter_scratch([spread], depth, resident=(0,)),
        ],
        compiler_params=kernel_params(collective_id, 1),
        name="widen_back",
    )(rows_grad, activated, slope, down_weight, low_turned, up_early, up_late)


ROW_BLOCK = 256


def mean_of(rows):
    return jnp.sum(rows, axis=-1, keepdims=True) * (1.0 / D)


def normalized(hidden):
    center = hidden - mean_of(hidden)
    root = lax.rsqrt(mean_of(center * center) + NORM_EPS)
    return center * root, root


def norm_back(grad, normed, root, gain):
    scaled = grad * gain
    return root * (scaled - mean_of(scaled) - normed * mean_of(scaled * normed))


def add_sums(sums, *rows):
    new = [jnp.sum(r.astype(F32), axis=0, keepdims=True) for r in rows]

    @pl.when(pl.program_id(0) == 0)
    def _():
        sums[...] = jnp.zeros_like(sums)

    for j, n in enumerate(new):
        sums[j : j + 1, :] += n


def project_kernel(attended, tokens, weight, scales, normed, root, low, turned):
    hidden = dot_over(attended[...], weight[...], 1, 0)
    hidden = tokens[...].astype(F32) + hidden + scales[0:1, :]
    normed[...], root[...] = normalized(hidden)
    branch = normed[...] * scales[1:2, :] + scales[2:3, :]
    low[...] = branch.astype(BF16)
    turned[...] = branch.T.astype(BF16)


def output_kernel(second_in, cotangent, scales, output, rows, grad, sums):
    normed, root = normalized(second_in[...])
    output[...] = (normed * scales[0:1, :] + scales[1:2, :]).astype(BF16)
    upstream = cotangent[...].astype(F32)
    grad[...] = norm_back(upstream, normed, root, scales[0:1, :])
    rows[...] = grad[...].astype(BF16)
    add_sums(sums, upstream * normed, upstream, rows[...])


def project_back_kernel(
    branch_grad, second_grad, normed, root, attended, weight, scales, grad, back, weight_grads, sums, total
):
    upstream = branch_grad[...] + second_grad[...]
    grad[...] = norm_back(upstream, normed[...], root[...], scales[0:1, :])
    rows = grad[...].astype(BF16)
    back[...] = dot_over(rows, weight[...], 1, 1).astype(BF16)
    add_sums(sums, upstream * normed[...], upstream, rows)
    part = dot_over(attended[...], rows, 0, 0)

    @pl.when(pl.program_id(0) == 0)
    def _():
        total[...] = part

    @pl.when(pl.program_id(0) > 0)
    def _():
        total[...] += part

    @pl.when(pl.program_id(0) == pl.num_programs(0) - 1)
    def _():
        weight_grads[...] = total[...].astype(weight_grads.dtype)


def row_block(width=D):
    return pl.BlockSpec((ROW_BLOCK, width), lambda i: (i, 0))


def row_call(kernel, count, in_specs, out_specs, outs, scratch=()):
    return pl.pallas_call(
        kernel,
        grid=(count // ROW_BLOCK,),
        in_specs=in_specs,
        out_specs=out_specs,
        out_shape=[jax.ShapeDtypeStruct(shape, dtype) for shape, dtype in outs],
        scratch_shapes=list(scratch),
        compiler_params=pltpu.CompilerParams(vmem_limit_bytes=60 << 20),
        name=kernel.__name__,
    )


SUMS = (8, D)


def project(attended, tokens, weight, scales):
    count = tokens.shape[0]
    block, matrix = row_block(), flat((D, D))
    turned = pl.BlockSpec((D, ROW_BLOCK), lambda i: (0, i))
    outs = [((count, D), F32), ((count, 1), F32), ((count, D), BF16), ((D, count), BF16)]
    return row_call(
        project_kernel,
        count,
        [block, block, matrix, flat(scales.shape)],
        [block, row_block(1), block, turned],
        outs,
    )(attended, tokens, weight, scales)


def output_and_grad(second_in, cotangent, scales):
    count = second_in.shape[0]
    block = row_block()
    shape = (count, D)
    return row_call(
        output_kernel,
        count,
        [block, block, flat(scales.shape)],
        [block, block, block, flat(SUMS)],
        [(shape, BF16), (shape, BF16), (shape, F32), (SUMS, F32)],
    )(second_in, cotangent, scales)


def project_back(branch_grad, second_grad, normed, root, attended, weight, scales, dtype):
    count = attended.shape[0]
    block, matrix = row_block(), flat((D, D))
    shape = (count, D)
    return row_call(
        project_back_kernel,
        count,
        [block, block, block, row_block(1), block, matrix, flat(scales.shape)],
        [block, block, matrix, flat(SUMS)],
        [(shape, F32), (shape, BF16), ((D, D), dtype), (SUMS, F32)],
        [pltpu.VMEM((D, D), F32)],
    )(branch_grad, second_grad, normed, root, attended, weight, scales)


def split_vector(vector):
    sizes = (D, D, D, D, D, FF, D, D, D)
    parts, at = [], 0
    for size in sizes:
        parts.append(vector[at : at + size])
        at += size
    return parts


def by_pair(columns):
    rows = columns.shape[0]
    return columns.reshape(rows, 3, PAIRS, LANES).swapaxes(1, 2).reshape(rows, 3 * D)


def by_kind(columns):
    rows = columns.shape[0]
    return columns.reshape(rows, PAIRS, 3, LANES).swapaxes(1, 2).reshape(rows, 3 * D)


def stacked(*vectors):
    return jnp.pad(jnp.stack(vectors), ((0, 8 - len(vectors)), (0, 0)))


def column_sums(rows):
    return jnp.sum(rows.astype(F32), axis=0)


def times(rows, matrix):
    return jnp.dot(rows, matrix, preferred_element_type=F32)


def weight_grad(left_rows, right_rows, dtype):
    return dot_over(left_rows, right_rows, 0, 0).astype(dtype)


def back_product(grad_rows, matrix):
    return dot_over(grad_rows, matrix, 1, 1)


def layer_step(tokens, doc_ids, cotangent, masters, devices, depth):
    grad_type = BF16 if depth else F32
    shape = (depth, 2, 2, 2)
    blocks, low_vector = lowered_blocks(masters)
    rows = low_vector.shape[0] // LANES
    if depth:
        tall = blocks[0].shape[0]
        padded = jnp.pad(low_vector.reshape(rows, LANES), ((0, tall - rows), (0, 0)))
        first = [blocks[0][:, g * GROUP_WIDTH : (g + 1) * GROUP_WIDTH] for g in range(GROUPS)]
        first[0] = jnp.concatenate([first[0], padded], axis=1)
        up_blocks = [blocks[2][:, : FF // 2], blocks[2][:, FF // 2 :]]
        qkv, attended, totals, qkv_weight, vectors, proj_weight, up_weight = attend(
            tokens, doc_ids, None, None, [*first, blocks[1], up_blocks[0]], rows, depth, 1
        )
        vector = vectors.reshape(devices, tall, LANES)[:, :rows].reshape(-1)
        qkv_weight, proj_weight, up_weight = map(rows_of, (qkv_weight, proj_weight, up_weight))
    else:
        weights = [lax.all_gather(b, "dp", axis=0, tiled=True) for b in blocks]
        qkv_weight, proj_weight, up_weight, down_weight = weights
        vector = lax.all_gather(low_vector, "dp", axis=0, tiled=True)
    (
        bias_query,
        bias_value,
        bias_proj,
        gain_first,
        shift_first,
        bias_up,
        bias_down,
        gain_second,
        shift_second,
    ) = split_vector(vector.astype(F32))
    if not depth:
        bias_all = jnp.concatenate([bias_query, jnp.zeros_like(bias_query), bias_value])
        bias_all = by_pair(bias_all[None])[0]
        qkv, attended, totals = attend(tokens, doc_ids, qkv_weight, bias_all, [], 0, 0, 0)
    normed, root, branch_low, low_turned = project(
        attended, tokens, proj_weight, stacked(bias_proj, gain_first, shift_first)
    )
    if depth:
        activated, slope, second_in, up_late, down_weight = widen(
            branch_low,
            up_weight,
            bias_up,
            normed,
            stacked(gain_first, shift_first, bias_down),
            [up_blocks[1], blocks[3]],
            depth,
            2,
        )
        up_late, down_weight = rows_of(up_late), rows_of(down_weight)
    else:
        upward = times(branch_low, up_weight) + bias_up
        cdf = 0.5 * (1.0 + lax.erf(upward * HALF_ROOT))
        activated = (upward * cdf).astype(BF16)
        slope = cdf + upward * (PDF_TOP * jnp.exp(-0.5 * upward * upward))
        branch = normed * gain_first + shift_first
        second_in = branch + times(activated, down_weight) + bias_down
    output, down_rows, second_grad, second_sums = output_and_grad(
        second_in, cotangent, stacked(gain_second, shift_second)
    )
    if depth:
        up_grad, branch_grad, bias_up_grad, down_owned = widen_back(
            down_rows,
            activated,
            slope,
            down_weight,
            low_turned,
            up_weight,
            up_late,
            depth,
            3,
        )
        bias_up_grad = bias_up_grad.reshape(-1)
    else:
        down_grad = weight_grad(activated, down_rows, F32)
        up_rows = (back_product(down_rows, down_weight) * slope).astype(BF16)
        bias_up_grad = column_sums(up_rows)
        up_grad = weight_grad(branch_low, up_rows, F32)
        branch_grad = back_product(up_rows, up_weight)
    hidden_grad, attended_grad, proj_grad, first_sums = project_back(
        branch_grad,
        second_grad,
        normed,
        root,
        attended,
        proj_weight,
        stacked(gain_first),
        grad_type,
    )
    known = [
        first_sums[2],
        first_sums[0],
        first_sums[1],
        bias_up_grad,
        second_sums[2],
        second_sums[0],
        second_sums[1],
    ]
    riders = []
    if depth:
        vector_part = jnp.concatenate([jnp.zeros((2 * D,), F32), *known])
        vector_part = vector_part.reshape(devices, rows, LANES)
        vector_part = jnp.pad(vector_part, ((0, 0), (0, 16 - rows), (0, 0)))
        riders = [g.reshape(*shape, -1, g.shape[1]) for g in (up_grad, proj_grad)]
        riders += [vector_part.reshape(*shape, 16, LANES)]
    input_grad, *summed = attend_back(
        tokens,
        qkv,
        doc_ids,
        attended_grad,
        totals,
        qkv_weight,
        hidden_grad,
        riders,
        rows,
        depth,
        4,
    )
    if depth:
        up_owned, proj_owned, *qkv_owned, vector_owned = summed
        owned = [jnp.concatenate(qkv_owned, axis=1), proj_owned, up_owned, down_owned]
        owned += [vector_owned[:rows]]
    else:
        qkv_grad, qkv_sums = summed
        qkv_sums = by_kind(qkv_sums.reshape(1, -1))[0]
        vector_grad = jnp.concatenate([qkv_sums[0:D], qkv_sums[2 * D : 3 * D], *known])
        grads = (qkv_grad, proj_grad, up_grad, down_grad, vector_grad[:, None])
        owned = [
            lax.psum_scatter(
                grad.reshape(devices, -1, grad.shape[-1]), "dp", scatter_dimension=0, tiled=True
            )[0]
            for grad in grads
        ]
    owned[0] = by_kind(owned[0])
    return output, input_grad, [own.reshape(-1) for own in owned]


def adam_update(master, moment_one, moment_two, grad, rate):
    one_new = BETA_FIRST * moment_one + (1.0 - BETA_FIRST) * grad
    two_new = BETA_SECOND * moment_two + (1.0 - BETA_SECOND) * grad * grad
    one_hat = one_new / (1.0 - BETA_FIRST**STEP)
    two_hat = two_new / (1.0 - BETA_SECOND**STEP)
    master_new = master - rate * (one_hat / (jnp.sqrt(two_hat) + ADAM_EPS) + WEIGHT_DECAY * master)
    return (grad, one_new, two_new, master_new, master_new.astype(BF16))


WIDTHS = (3 * D, D, FF, D)


def lowered_blocks(masters):
    lowered = [master.astype(BF16) for master in masters]
    blocks = [low.reshape(-1, width) for low, width in zip(lowered, WIDTHS)]
    blocks[0] = by_pair(blocks[0])
    return blocks, lowered[4]


def body(depth, tokens, segment_ids, out_grad, *states):
    devices = lax.axis_size("dp")
    masters = states[0::3]
    output, input_grad, owned = layer_step(
        tokens, segment_ids, out_grad, masters, devices, depth
    )
    outs = [output, input_grad]
    for i in range(5):
        outs += adam_update(*states[3 * i : 3 * i + 3], owned[i], RATES[i])
    return tuple(outs)


def solution(mesh):
    rows = P("dp", None)
    flat = P("dp")
    return jax.shard_map(
        functools.partial(body, depth_of(mesh)),
        mesh=mesh,
        in_specs=(rows,) * 3 + (flat,) * 15,
        out_specs=(rows,) * 2 + (flat,) * 25,
        check_vma=False,
    )
```

```python
import functools

import jax
import jax.numpy as jnp
from jax import lax
from jax.experimental import pallas as pl
from jax.experimental.pallas import tpu as pltpu
from jax.sharding import PartitionSpec as P

D = 1024
HEADS = 16
HEAD_DIM = 64
FF = 4096
STEP = 3
LANES = 128
PAIRS = HEADS * HEAD_DIM // LANES

NORM_EPS = 1e-05
BETA_FIRST = 0.5
BETA_SECOND = 0.5
ADAM_EPS = 1e-08
WEIGHT_DECAY = 0.01
MASK_FILL = -1000000000.0
RATES = (0.01, 0.03, 0.01, 0.005, 0.05)
SCALE = HEAD_DIM ** (-0.5)
HALF_ROOT = 0.7071067811865476
PDF_TOP = 0.3989422804014327

F32 = jnp.float32
BF16 = jnp.bfloat16
MESH = pl.DeviceIdType.MESH


def dot_over(left, right, left_dim, right_dim):
    return lax.dot_general(
        left, right, (((left_dim,), (right_dim,)), ((), ())), preferred_element_type=F32
    )


PLANNED_DEPTH = 4


def depth_of(mesh):
    devices = list(mesh.devices.flat)
    if len(devices) % 8:
        return 0
    try:
        spots = [(*d.coords, d.core_on_chip) for d in devices]
    except AttributeError:
        return 0
    low = [min(s[i] for s in spots) for i in range(4)]
    depth = len(devices) // 8
    if depth != PLANNED_DEPTH:
        return 0
    for index, (x, y, z, core) in enumerate(spots):
        spot = (((z - low[2]) * 2 + y - low[1]) * 2 + x - low[0]) * 2 + core - low[3]
        if spot != index:
            return 0
    return depth


class Place:
    def __init__(self, depth):
        me = lax.axis_index("dp")
        self.depth = depth
        self.core = me % 2
        self.x = (me // 2) % 2
        self.y = (me // 4) % 2
        self.z = me // 8

    def index(self, z, y, x, core):
        return ((z * 2 + y) * 2 + x) * 2 + core

    def ahead(self, k):
        return (self.z + k) % self.depth

    def back(self, k):
        return (self.z + self.depth - k) % self.depth

    def twin(self):
        return self.index(self.z, self.y, self.x, 1 - self.core)

    def x_mate(self):
        return self.index(self.z, self.y, 1 - self.x, self.core)

    def y_mate(self):
        return self.index(self.z, 1 - self.y, self.x, self.core)

    def z_mate(self, k):
        return self.index(self.ahead(k), self.y, self.x, self.core)

    def greet(self):
        barrier = pltpu.get_barrier_semaphore()
        mates = [self.twin(), self.x_mate(), self.y_mate()]
        mates += [self.z_mate(k) for k in range(1, self.depth)]
        for mate in mates:
            pl.semaphore_signal(barrier, inc=1, device_id=(mate,), device_id_type=MESH)
        pl.semaphore_wait(barrier, len(mates))


def send(source, target, send_sem, recv_sem, device):
    return pltpu.make_async_remote_copy(
        src_ref=source,
        dst_ref=target,
        send_sem=send_sem,
        recv_sem=recv_sem,
        device_id=(device,),
        device_id_type=MESH,
    )


class Gather:
    BY_Z, BY_X, BY_Y, UPPER, LOWER, OWN, FROM_X, FROM_Y, CROSS = range(9)

    def __init__(self, place, blocks, full, send_sems, recv_sems, local_sems):
        self.place = place
        self.blocks = blocks
        self.full = full
        self.sems = (send_sems, recv_sems)
        self.local_sems = local_sems
        self.depth = place.depth

    def home(self, w):
        p = self.place
        return self.full[w].at[p.z, p.y, p.x, p.core]

    def copy(self, w, k, kind):
        p, full = self.place, self.full[w]
        half = self.blocks[w].shape[0] // 2
        sems = [sem.at[w, k, kind] for sem in self.sems]
        zz = p.back(k)
        if kind == self.BY_Z:
            return send(self.blocks[w], self.home(w), *sems, p.z_mate(k))
        if kind in (self.BY_X, self.BY_Y, self.OWN):
            block = full.at[zz, p.y, p.x, p.core]
            source = self.blocks[w] if k == 0 else block
            mate = {self.BY_X: p.x_mate, self.BY_Y: p.y_mate, self.OWN: p.twin}[kind]()
            return send(source, block, *sems, mate)
        if kind == self.UPPER:
            block = full.at[zz, p.y, 1 - p.x, p.core, pl.ds(0, half)]
            return send(block, block, *sems, p.y_mate())
        if kind == self.LOWER:
            block = full.at[zz, 1 - p.y, p.x, p.core, pl.ds(half, half)]
            return send(block, block, *sems, p.x_mate())
        if kind == self.FROM_X:
            block = full.at[zz, p.y, 1 - p.x, p.core]
        elif kind == self.FROM_Y:
            block = full.at[zz, 1 - p.y, p.x, p.core]
        else:
            block = full.at[zz, 1 - p.y, 1 - p.x, p.core]
        return send(block, block, *sems, p.twin())

    def local(self, w):
        return pltpu.make_async_copy(self.blocks[w], self.home(w), self.local_sems.at[w])

    def start(self, w):
        for k in range(1, self.depth):
            self.copy(w, k, self.BY_Z).start()
        self.local(w).start()

    def spread(self, w, k):
        if k:
            self.copy(w, k, self.BY_Z).wait_recv()
        for kind in (self.BY_X, self.BY_Y, self.OWN):
            self.copy(w, k, kind).start()

    def relay(self, w, k):
        self.copy(w, k, self.BY_X).wait_recv()
        self.copy(w, k, self.UPPER).start()
        self.copy(w, k, self.FROM_X).start()
        self.copy(w, k, self.BY_Y).wait_recv()
        self.copy(w, k, self.LOWER).start()
        self.copy(w, k, self.FROM_Y).start()

    def hand_over(self, w, k):
        self.copy(w, k, self.UPPER).wait_recv()
        self.copy(w, k, self.LOWER).wait_recv()
        self.copy(w, k, self.CROSS).start()

    def receive(self, w, k):
        if k == 0:
            self.local(w).wait()
        for kind in (self.OWN, self.FROM_X, self.FROM_Y, self.CROSS):
            self.copy(w, k, kind).wait_recv()

    def receive_all(self, w):
        for k in range(self.depth):
            self.receive(w, k)

    def sent(self, w):
        for k in range(self.depth):
            for kind in range(9):
                if kind != self.BY_Z or k:
                    self.copy(w, k, kind).wait_send()

    def sent_all(self):
        for w in range(len(self.blocks)):
            self.sent(w)

    def step(self, units, t):
        lag = self.depth
        if t < len(units):
            self.spread(*units[t])
        if 0 <= t - lag < len(units):
            self.relay(*units[t - lag])
        if 0 <= t - 2 * lag < len(units):
            self.hand_over(*units[t - 2 * lag])

    def units(self):
        return [(w, k) for w in range(len(self.blocks)) for k in range(self.depth)]

    def start_all(self):
        for w in range(len(self.blocks)):
            self.start(w)

def gather_sems(count, depth):
    return [
        pltpu.SemaphoreType.DMA((count, depth, 9)),
        pltpu.SemaphoreType.DMA((count, depth, 9)),
        pltpu.SemaphoreType.DMA((count,)),
    ]


class Scatter:
    TWIN, UPPER_Y, LOWER_X, UPPER_X, LOWER_Y, BY_Z = range(6)

    def __init__(self, place, grads, out, bufs, send_sems, recv_sems, local_sems, resident=()):
        self.place = place
        self.resident = resident
        self.grads = grads
        self.out = out
        self.bufs = bufs
        self.sems = (send_sems, recv_sems)
        self.local_sems = local_sems
        self.depth = place.depth
        self.order = list(range(1, self.depth)) + [0]

    def load(self, w, k):
        p = self.place
        return pltpu.make_async_copy(
            self.grads[w].at[p.ahead(k), :, :, p.core],
            self.bufs[w][6].at[k],
            self.local_sems.at[w, k],
        )

    def sums(self, w, k):
        if w in self.resident:
            return self.grads[w].at[self.place.ahead(k), :, :, self.place.core]
        return self.bufs[w][6].at[k]

    def half(self, w):
        return self.grads[w].shape[-2] // 2

    def copy(self, w, k, kind):
        p = self.place
        twin, upper_y, lower_x, upper_x, lower_y, by_z = self.bufs[w][:6]
        sums, half = self.sums(w, k), self.half(w)
        sems = [sem.at[w, k, kind] for sem in self.sems]
        top, bottom = pl.ds(0, half), pl.ds(half, half)
        if kind == self.TWIN:
            source = self.grads[w].at[p.ahead(k), :, :, 1 - p.core]
            return send(source, twin.at[k], *sems, p.twin())
        if kind == self.UPPER_Y:
            return send(sums.at[1 - p.y, :, top], upper_y.at[k], *sems, p.y_mate())
        if kind == self.LOWER_X:
            return send(sums.at[:, 1 - p.x, bottom], lower_x.at[k], *sems, p.x_mate())
        if kind == self.UPPER_X:
            return send(sums.at[p.y, 1 - p.x, top], upper_x.at[k], *sems, p.x_mate())
        if kind == self.LOWER_Y:
            return send(sums.at[1 - p.y, p.x, bottom], lower_y.at[k], *sems, p.y_mate())
        return send(sums.at[p.y, p.x], by_z.at[k], *sems, p.z_mate(k))

    @staticmethod
    def add(target, extra):
        target[...] = target[...] + extra[...]

    def start(self, w):
        for k in self.order:
            self.begin(w, k)

    def begin(self, w, k):
        self.copy(w, k, self.TWIN).start()
        if w not in self.resident:
            self.load(w, k).start()

    def first(self, w, k):
        sums, twin = self.sums(w, k), self.bufs[w][0]
        if w not in self.resident:
            self.load(w, k).wait()
        self.copy(w, k, self.TWIN).wait_recv()

        def body(i, carry):
            self.add(sums.at[i // 2, i % 2], twin.at[k, i // 2, i % 2])
            return carry

        lax.fori_loop(0, 4, body, 0)
        self.copy(w, k, self.UPPER_Y).start()
        self.copy(w, k, self.LOWER_X).start()

    def second(self, w, k):
        p = self.place
        sums, half = self.sums(w, k), self.half(w)
        upper_y, lower_x = self.bufs[w][1:3]
        self.copy(w, k, self.UPPER_Y).wait_recv()
        self.copy(w, k, self.LOWER_X).wait_recv()

        def body(i, carry):
            self.add(sums.at[p.y, i, pl.ds(0, half)], upper_y.at[k, i])
            self.add(sums.at[i, p.x, pl.ds(half, half)], lower_x.at[k, i])
            return carry

        lax.fori_loop(0, 2, body, 0)
        self.copy(w, k, self.UPPER_X).start()
        self.copy(w, k, self.LOWER_Y).start()

    def third(self, w, k):
        p = self.place
        sums, half = self.sums(w, k), self.half(w)
        upper_x, lower_y = self.bufs[w][3:5]
        self.copy(w, k, self.UPPER_X).wait_recv()
        self.copy(w, k, self.LOWER_Y).wait_recv()
        self.add(sums.at[p.y, p.x, pl.ds(0, half)], upper_x.at[k])
        self.add(sums.at[p.y, p.x, pl.ds(half, half)], lower_y.at[k])
        if isinstance(k, int):
            if k:
                self.copy(w, k, self.BY_Z).start()
        else:
            pl.when(k != 0)(lambda: self.copy(w, k, self.BY_Z).start())

    def finish(self, w):
        p = self.place
        by_z = self.bufs[w][5]
        for k in range(1, self.depth):
            self.copy(w, k, self.BY_Z).wait_recv()
        total = self.sums(w, 0)[p.y, p.x].astype(F32)
        for k in range(1, self.depth):
            total = total + by_z[k].astype(F32)
        self.out[w][...] = total
        for k in range(self.depth):
            for kind in range(6):
                if kind != self.BY_Z or k:
                    self.copy(w, k, kind).wait_send()


BUFS = 7


def scatter_scratch(grads, depth, resident=()):
    scratch = []
    for w, grad in enumerate(grads):
        rows, columns = grad.shape[-2:]
        half = rows // 2
        shapes = [(depth, 2, 2, rows, columns)]
        shapes += [(depth, 2, half, columns)] * 2 + [(depth, half, columns)] * 2
        shapes += [(depth, rows, columns)]
        shapes += [(8, LANES) if w in resident else (depth, 2, 2, rows, columns)]
        scratch += [pltpu.VMEM(shape, grad.dtype) for shape in shapes]
    count = len(grads)
    scratch += [pltpu.SemaphoreType.DMA((count, depth, 6))] * 2
    return scratch + [pltpu.SemaphoreType.DMA((count, depth))]


def own_lanes(head):
    lane = lax.broadcasted_iota(jnp.int32, (1, LANES), 1)
    return (lane < HEAD_DIM) == (head == 0)


def fill_masks(ids_row, ids_column, masks):
    for b in range(masks.shape[0]):
        masks[b] = jnp.where(ids_column[b] == ids_row[b], 0.0, MASK_FILL).astype(F32)


def at_step(t, work):
    pl.when(pl.program_id(0) * pl.num_programs(1) + pl.program_id(1) == t)(work)


GROUPS = 4
GROUP_PAIRS = PAIRS // GROUPS
GROUP_WIDTH = 3 * LANES * GROUP_PAIRS


def rows_of(block):
    return block.reshape(-1, block.shape[-1])


def attend_kernel(depth, count, seqs, per, *refs):
    ids_row, ids_column, tokens = refs[:3]
    if depth:
        blocks, refs = refs[3 : 3 + count], refs[3 + count :]
        qkv, attended, log_total, whole_qkv, whole_vector = refs[:5]
        riders, refs = refs[5 : 5 + count - GROUPS], refs[5 + count - GROUPS :]
        masks, bias, store, refs = refs[0], refs[1], refs[2], refs[3:]
        groups = [
            store.at[g, :, :, :, :, :, pl.ds(0, blocks[g].shape[1])] for g in range(GROUPS)
        ]
        place = Place(depth)
        side = Gather(place, blocks, [*groups, *riders], *refs[:3])
        out_sems = refs[3]
        units = side.units()

        def out_copy(g):
            columns = pl.ds(0, GROUP_WIDTH)
            target = pl.ds(g * GROUP_WIDTH, GROUP_WIDTH)
            return pltpu.make_async_copy(
                groups[g].at[:, :, :, :, :, columns],
                whole_qkv.at[:, :, :, :, :, target],
                out_sems.at[g],
            )

        vector_copy = pltpu.make_async_copy(
            groups[0].at[:, :, :, :, :, pl.ds(GROUP_WIDTH, LANES)], whole_vector, out_sems.at[GROUPS]
        )

        def open_up():
            place.greet()
            side.start_all()
            for t in range(3 * depth):
                side.step(units, t)
            side.receive_all(0)
            out_copy(0).start()
            vector_copy.start()
            for r in range(2 * PAIRS):
                d, j = r // per, r % per
                spot = (d // 8, d // 4 % 2, d // 2 % 2, d % 2)
                row = store[(0, *spot, slice(j, j + 1), slice(GROUP_WIDTH, GROUP_WIDTH + LANES))]
                bias[r] = row.astype(F32)

        at_step(0, open_up)
        steps = seqs * GROUP_PAIRS

        def each(work, w):
            for k in range(depth):
                work(w, k)

        def ready(g):
            side.receive_all(g)
            out_copy(g).start()

        steps = seqs * PAIRS
        plan = [[] for _ in range(steps)]

        def put(i, work, *what):
            plan[min(i, steps - 1)].append(functools.partial(work, *what))

        proj, up = GROUPS, GROUPS + 1
        put(1, each, side.spread, 3)
        put(2, each, side.hand_over, 1)
        put(2, each, side.relay, 2)
        put(3, each, side.spread, proj)
        put(steps // GROUPS, ready, 1)
        put(5, each, side.relay, 3)
        put(6, each, side.hand_over, 2)
        put(7, each, side.relay, proj)
        put(2 * steps // GROUPS, ready, 2)
        put(8, each, side.hand_over, 3)
        put(9, each, side.hand_over, proj)
        put(3 * steps // GROUPS, ready, 3)
        for k in range(depth):
            put(4 + k, side.spread, up, k)
            put(8 + k, side.relay, up, k)
            put(11 + k, side.hand_over, up, k)
        for i in range(1, steps):

            def more(i=i):
                for work in plan[i]:
                    work()

            if plan[i]:
                at_step(i, more)
    else:
        weight, bias, qkv, attended, log_total, masks = refs[3:]
    at_step(0, lambda: fill_masks(ids_row, ids_column, masks))
    h, b = pl.program_id(0), pl.program_id(1)
    length = masks.shape[1]
    rows = tokens[pl.ds(pl.multiple_of(b * length, length), length), :]
    if depth:
        shifts = [bias[h], jnp.zeros((1, LANES), F32), bias[PAIRS + h]]
        shift = jnp.concatenate(shifts, axis=1)
        columns = pl.ds(pl.multiple_of((h % GROUP_PAIRS) * 3 * LANES, 3 * LANES), 3 * LANES)
        weight = rows_of(store[h // GROUP_PAIRS, :, :, :, :, :, columns])
        qkv[...] = (dot_over(rows, weight, 1, 0) + shift).astype(BF16)
    else:
        qkv[...] = (dot_over(rows, weight[...], 1, 0) + bias[0]).astype(BF16)
    query = qkv[:, 0:LANES] * BF16(SCALE)
    key = qkv[:, LANES : 2 * LANES]
    value = qkv[:, 2 * LANES : 3 * LANES]
    chunk = length // 2
    outs = []
    for head in range(2):
        own_key = jnp.where(own_lanes(head), key, BF16(0))
        parts = []
        for at in range(0, length, chunk):
            scores = dot_over(own_key, query[at : at + chunk], 1, 1)
            scores = scores + masks[b, :, at : at + chunk]
            top = jnp.max(scores, axis=0, keepdims=True)
            weights = jnp.exp(scores - top)
            total = jnp.sum(weights, axis=0, keepdims=True)
            log_total[0, 0, head : head + 1, at : at + chunk] = top + jnp.log(total)
            probs = (weights * (1.0 / total)).astype(BF16)
            parts.append(dot_over(probs, value, 0, 0))
        outs.append(jnp.concatenate(parts, axis=0))
    attended[...] = jnp.where(own_lanes(0), outs[0], outs[1]).astype(BF16)
    if depth:

        def close():
            for w in range(GROUPS, count):
                side.receive_all(w)
            side.sent_all()
            vector_copy.wait()
            for g in range(GROUPS):
                out_copy(g).wait()

        at_step(seqs * PAIRS - 1, close)


def attend_back_kernel(depth, seqs, per_device, *refs):
    ids_row, ids_column, tokens, qkv, attended_grad, log_total, weight, hidden_grad = refs[:8]
    steps = seqs * PAIRS
    i = pl.program_id(0)
    last = pl.num_programs(0) - 1
    spot = jnp.minimum(i, steps - 1)
    h, b = spot // seqs, spot % seqs
    if depth:
        up_grad, proj_grad, vector_part, input_grad = refs[8:12]
        out, refs = refs[12 : 15 + GROUPS], refs[15 + GROUPS :]
        masks, kept, total, sums, vector, *refs = refs
        groups, refs = refs[:GROUPS], refs[GROUPS:]
        grads = [up_grad, proj_grad, *groups, vector]
        count = len(grads)
        bufs = [refs[BUFS * w : BUFS * w + BUFS] for w in range(count)]
        place = Place(depth)
        side = Scatter(place, grads, out, bufs, *refs[BUFS * count :], resident=range(2, count))
        plan = [[] for _ in range(steps + tokens.shape[0] // ROW_BLOCK)]

        def put(at, work, *what):
            plan[min(at, len(plan) - 1)].append(functools.partial(work, *what))

        def each(work, w):
            def body(k, carry):
                work(w, k)
                return carry

            lax.fori_loop(0, depth, body, 0)

        up, proj, vec = 0, 1, count - 1
        put(0, place.greet)
        put(0, side.start, up)
        put(0, side.start, proj)
        for n, k in enumerate(side.order):
            put(1 + 2 * n, side.first, up, k)
            put(4 + 2 * n + (n + 1) // 2, side.second, up, k)
            put(8 + 2 * n + (n + 1) // 2, side.third, up, k)
        put(2, each, side.first, proj)
        put(7, each, side.second, proj)
        put(12, each, side.third, proj)
        per = steps // GROUPS
        for g in range(GROUPS):
            at = per * (g + 1)
            put(at, each, side.begin, 2 + g)
            put(at + 1, each, side.first, 2 + g)
            put(at + (7, 6, 4, 2)[g], each, side.second, 2 + g)
            put(at + (10, 8, 5, 3)[g], each, side.third, 2 + g)
        rows_each = per_device

        def make_vector():
            vector[...] = vector_part[...]
            for r in range(2 * PAIRS):
                d, j = r // rows_each, r % rows_each
                source = 0 if r < PAIRS else 2 * LANES
                row = sums[r % PAIRS, :, source : source + LANES]
                vector[d // 8, d // 4 % 2, d // 2 % 2, d % 2, j : j + 1, :] = row

        put(steps, make_vector)
        put(steps + 1, each, side.begin, vec)
        put(steps + 2, each, side.first, vec)
        put(steps + 3, each, side.second, vec)
        for at, works in enumerate(plan):

            def run(works=works):
                for work in works:
                    work()

            if works:
                pl.when(i == at)(run)
    else:
        input_grad, weight_grads, sums, masks, kept, total = refs[8:]
    pl.when(i == 0)(lambda: fill_masks(ids_row, ids_column, masks))
    length = qkv.shape[0]
    chunk = length
    wide = pl.ds(pl.multiple_of(h * 3 * LANES, 3 * LANES), 3 * LANES)
    tall = pl.ds(pl.multiple_of(b * length, length), length)

    @pl.when(i < steps)
    def _():
        query = qkv[:, 0:LANES]
        key = qkv[:, LANES : 2 * LANES]
        value = qkv[:, 2 * LANES : 3 * LANES]
        grad = attended_grad[...]
        scaled = query * BF16(SCALE)
        query_grads, key_grads, value_grads = [], [], []
        for head in range(2):
            own_key = jnp.where(own_lanes(head), key, BF16(0))
            own_value = jnp.where(own_lanes(head), value, BF16(0))
            key_grad = value_grad = None
            parts = []
            for at in range(0, length, chunk):
                piece = slice(at, at + chunk)
                scores = dot_over(own_key, scaled[piece], 1, 1) + masks[b, :, piece]
                probs = jnp.exp(scores - log_total[0, 0, head : head + 1, piece])
                prob_grad = dot_over(own_value, grad[piece], 1, 1)
                row_dot = jnp.sum(probs * prob_grad, axis=0, keepdims=True)
                score_grad = (probs * (prob_grad - row_dot)).astype(BF16)
                value_part = dot_over(probs.astype(BF16), grad[piece], 1, 0)
                key_part = dot_over(score_grad, query[piece], 1, 0)
                value_grad = value_part if value_grad is None else value_grad + value_part
                key_grad = key_part if key_grad is None else key_grad + key_part
                parts.append(dot_over(score_grad, key, 0, 0))
            query_grads.append(jnp.concatenate(parts, axis=0))
            key_grads.append(key_grad)
            value_grads.append(value_grad)
        first = own_lanes(0)
        own = [
            (jnp.where(first, *query_grads) * SCALE).astype(BF16),
            (jnp.where(first, *key_grads) * SCALE).astype(BF16),
            jnp.where(first, *value_grads).astype(BF16),
        ]
        rows_grad = jnp.concatenate(own, axis=1)
        kept[tall, wide] = rows_grad
        part = dot_over(tokens[tall, :], rows_grad, 0, 0)
        part_sums = jnp.sum(rows_grad.astype(F32), axis=0, keepdims=True)

        @pl.when(b == 0)
        def _():
            total[...] = part
            sums[h] = part_sums

        @pl.when(b > 0)
        def _():
            total[...] += part
            sums[h] += part_sums

        @pl.when(b == seqs - 1)
        def _():
            if depth:
                where = (h % GROUP_PAIRS) * 3 * LANES
                columns = pl.ds(pl.multiple_of(where, 3 * LANES), 3 * LANES)
                for g in range(GROUPS):

                    @pl.when(h // GROUP_PAIRS == g)
                    def _():
                        shape = groups[g].shape[:5] + (3 * LANES,)
                        groups[g][:, :, :, :, :, columns] = total[...].astype(BF16).reshape(shape)
            else:
                weight_grads[...] = total[...]

    @pl.when(i >= steps)
    def _():
        at = pl.multiple_of((i - steps) * ROW_BLOCK, ROW_BLOCK)
        back = dot_over(kept[pl.ds(at, ROW_BLOCK), :], weight[...], 1, 1)
        input_grad[...] = (back + hidden_grad[...]).astype(BF16)

    if depth:

        @pl.when(i == last)
        def _():
            each(side.third, vec)
            for w in range(count):
                side.finish(w)


def whole(shape):
    return pl.BlockSpec(shape, lambda h, b: (0,) * len(shape))


def attention_specs(count, length):
    rows = whole((count, 1, length))
    columns = whole((count, length, 1))
    tokens = whole((count * length, D))
    wide = pl.BlockSpec((length, 3 * LANES), lambda h, b: (b, h))
    one = pl.BlockSpec((length, LANES), lambda h, b: (b, h))
    log_total = pl.BlockSpec((1, 1, 2, length), lambda h, b: (b, h, 0, 0))
    weight = pl.BlockSpec((D, 3 * LANES), lambda h, b: (0, h))
    vector = pl.BlockSpec((1, 1, 3 * LANES), lambda h, b: (h, 0, 0))
    return rows, columns, tokens, wide, one, log_total, weight, vector


def kernel_params(collective_id, remote, limit=60 << 20):
    if not remote:
        return pltpu.CompilerParams(vmem_limit_bytes=limit)
    return pltpu.CompilerParams(
        collective_id=collective_id, has_side_effects=True, vmem_limit_bytes=limit
    )


def attend(tokens, doc_ids, weight, bias, blocks, per, depth, collective_id):
    count, length = doc_ids.shape
    rows, columns, all_tokens, wide, one, log_total, part, vector = attention_specs(count, length)
    in_place = pl.BlockSpec(memory_space=pl.ANY)
    out_shape = [
        jax.ShapeDtypeStruct((count * length, 3 * D), BF16),
        jax.ShapeDtypeStruct((count * length, D), BF16),
        jax.ShapeDtypeStruct((count, PAIRS, 2, length), F32),
    ]
    out_specs = [wide, one, log_total]
    in_specs = [rows, columns, all_tokens]
    scratch = [pltpu.VMEM((count, length, length), F32)]
    grid3 = (depth, 2, 2, 2)
    if depth:
        in_specs += [whole(b.shape) for b in blocks]
        tall = blocks[0].shape[0]
        shapes = [(*grid3, tall, 3 * D), (*grid3, tall, LANES)]
        shapes += [grid3 + b.shape for b in blocks[GROUPS:]]
        out_shape += [jax.ShapeDtypeStruct(shape, BF16) for shape in shapes]
        out_specs += [in_place] * len(shapes)
        scratch += [pltpu.VMEM((2 * PAIRS, 1, LANES), F32)]
        scratch += [pltpu.VMEM((GROUPS, *grid3, *blocks[0].shape), BF16)]
        scratch += gather_sems(len(blocks), depth) + [pltpu.SemaphoreType.DMA((GROUPS + 1,))]
        operands = blocks
    else:
        in_specs += [part, vector]
        operands = [weight, bias.reshape(PAIRS, 1, 3 * LANES)]
    return pl.pallas_call(
        functools.partial(attend_kernel, depth, len(blocks), count, per),
        grid=(PAIRS, count),
        in_specs=in_specs,
        out_specs=out_specs,
        out_shape=out_shape,
        scratch_shapes=scratch,
        compiler_params=kernel_params(collective_id, len(blocks)),
        name="attend",
    )(
        doc_ids.reshape(count, 1, length),
        doc_ids.reshape(count, length, 1),
        tokens,
        *operands,
    )


def attend_back(
    tokens, qkv, doc_ids, attended_grad, totals, weight, hidden_grad, grads, per_device, depth, collective_id
):
    seqs, length = doc_ids.shape
    steps = seqs * PAIRS
    blocks = seqs * length // ROW_BLOCK

    def h(i):
        return jnp.minimum(i, steps - 1) // seqs

    def b(i):
        return jnp.minimum(i, steps - 1) % seqs

    def late(i):
        return jnp.maximum(i - steps, 0)

    in_place = pl.BlockSpec(memory_space=pl.ANY)
    in_specs = [
        once((seqs, 1, length)),
        once((seqs, length, 1)),
        once((seqs * length, D)),
        pl.BlockSpec((length, 3 * LANES), lambda i: (b(i), h(i))),
        pl.BlockSpec((length, LANES), lambda i: (b(i), h(i))),
        pl.BlockSpec((1, 1, 2, length), lambda i: (b(i), h(i), 0, 0)),
        once((D, 3 * D)),
        pl.BlockSpec((ROW_BLOCK, D), lambda i: (late(i), 0)),
    ]
    out_specs = [pl.BlockSpec((ROW_BLOCK, D), lambda i: (late(i), 0))]
    out_shape = [jax.ShapeDtypeStruct((seqs * length, D), BF16)]
    scratch = [
        pltpu.VMEM((seqs, length, length), F32),
        pltpu.VMEM((seqs * length, 3 * D), BF16),
        pltpu.VMEM((D, 3 * LANES), F32),
    ]
    if depth:
        up_grad, proj_grad, vector = grads
        tall = up_grad.shape[-2]
        group = jax.ShapeDtypeStruct((depth, 2, 2, 2, tall, GROUP_WIDTH), BF16)
        moved = [up_grad, proj_grad, *([group] * GROUPS), vector]
        in_specs += [in_place, in_place, flat(vector.shape)]
        out_specs += [flat(m.shape[-2:]) for m in moved]
        out_shape += [jax.ShapeDtypeStruct(m.shape[-2:], F32) for m in moved]
        scratch += [pltpu.VMEM((PAIRS, 1, 3 * LANES), F32), pltpu.VMEM(vector.shape, F32)]
        scratch += [pltpu.VMEM(group.shape, BF16)] * GROUPS
        scratch += scatter_scratch(moved, depth, resident=range(2, len(moved)))
    else:
        out_specs += [
            pl.BlockSpec((D, 3 * LANES), lambda i: (0, h(i))),
            flat((PAIRS, 1, 3 * LANES)),
        ]
        out_shape += [
            jax.ShapeDtypeStruct((D, 3 * D), F32),
            jax.ShapeDtypeStruct((PAIRS, 1, 3 * LANES), F32),
        ]
    return pl.pallas_call(
        functools.partial(attend_back_kernel, depth, seqs, per_device),
        grid=(steps + blocks,),
        in_specs=in_specs,
        out_specs=out_specs,
        out_shape=out_shape,
        scratch_shapes=scratch,
        compiler_params=kernel_params(collective_id, depth, 63 << 20),
        name="attend_back",
    )(
        doc_ids.reshape(seqs, 1, length),
        doc_ids.reshape(seqs, length, 1),
        tokens,
        qkv,
        attended_grad,
        totals,
        weight,
        hidden_grad,
        *grads,
    )


TILE = 512
ROW_CHUNK = 256


def widen_kernel(depth, tiles, *refs):
    low, up_weight, up_bias, normed, scales = refs[:5]
    blocks = refs[5:7]
    activated, slope, second_in, whole_up, whole_down = refs[7:12]
    kept, tile_weight, late_up, down, out_sems, *sems = refs[12:]
    place = Place(depth)
    side = Gather(place, blocks, [late_up, down], *sems)
    i = pl.program_id(0)
    per = tiles // depth
    half = tiles // 2

    def out_copy(k):
        zz = place.back(k)
        return pltpu.make_async_copy(down.at[zz], whole_down.at[zz], out_sems.at[k])

    up_copy = pltpu.make_async_copy(late_up, whole_up, out_sems.at[depth])
    plan = [[] for _ in range(tiles + depth)]

    def put(at, work, *what):
        plan[min(at, len(plan) - 1)].append(functools.partial(work, *what))

    put(0, place.greet)
    put(0, side.start_all)
    for k in range(depth):
        put(min(k, half - 1), side.spread, 0, k)
        put(min(k + 2, half), side.relay, 0, k)
    put(half, side.spread, 1, 0)
    put(half, side.spread, 1, 1)
    for k in range(depth):
        put(half, side.hand_over, 0, k)
    put(half, side.receive_all, 0)
    put(half, up_copy.start)
    put(half + 1, side.relay, 1, 0)
    for k in range(2, depth):
        put(half + 2 * k - 2, side.spread, 1, k)
    for k in range(1, depth - 1):
        put(half + 1 + 2 * k, side.relay, 1, k)
    put(tiles + depth - 2, side.relay, 1, depth - 1)
    for k in range(depth):
        put(tiles + k, side.hand_over, 1, k)
    for at, works in enumerate(plan):

        def run(works=works):
            for work in works:
                work()

        if works:
            pl.when(i == at)(run)

    @pl.when(i < half)
    def _():
        tile_weight[...] = up_weight[...]

    @pl.when((i >= half) & (i < tiles))
    def _():
        columns = pl.ds(pl.multiple_of((i - half) * TILE, TILE), TILE)
        tile_weight[...] = rows_of(late_up[:, :, :, :, :, columns])

    @pl.when(i < tiles)
    def _():
        for at in range(0, low.shape[0], ROW_CHUNK):
            rows = slice(at, at + ROW_CHUNK)
            upward = dot_over(low[rows, :], tile_weight[...], 1, 0) + up_bias[...]
            cdf = 0.5 * (1.0 + lax.erf(upward * HALF_ROOT))
            value = (upward * cdf).astype(BF16)
            activated[rows, :] = value
            kept[i, rows, :] = value
            slope[rows, :] = cdf + upward * (PDF_TOP * jnp.exp(-0.5 * upward * upward))

    for k in range(depth):

        def layer(k=k):
            side.receive(1, k)
            out_copy(k).start()
            zz = place.back(k)
            for at in range(0, low.shape[0], ROW_CHUNK):
                rows = slice(at, at + ROW_CHUNK)
                if k == 0:
                    total = normed[rows, :] * scales[0:1, :] + scales[1:2, :] + scales[2:3, :]
                else:
                    total = second_in[rows, :]
                for n in range(per):
                    tile = kept[zz * per + n, rows, :]
                    weight = rows_of(down[zz, n * 2 // per : (n + 1) * 2 // per])
                    total = total + dot_over(tile, weight, 1, 0)
                second_in[rows, :] = total

        pl.when(i == tiles + k)(layer)

    @pl.when(i == tiles + depth - 1)
    def _():
        side.sent_all()
        up_copy.wait()
        for k in range(depth):
            out_copy(k).wait()


def flat(shape):
    return pl.BlockSpec(shape, lambda i: (0,) * len(shape))


def once(shape):
    return pl.BlockSpec(shape, lambda i: (0,) * len(shape), pipeline_mode=pl.Buffered(1))


def widen(low, up_weight, up_bias, normed, scales, blocks, depth, collective_id):
    count = low.shape[0]
    tiles = FF // TILE
    last, half = tiles - 1, tiles // 2
    tile = pl.BlockSpec((count, TILE), lambda i: (0, jnp.minimum(i, last)))
    spread = [(depth, 2, 2, 2) + block.shape for block in blocks]
    in_place = pl.BlockSpec(memory_space=pl.ANY)
    return pl.pallas_call(
        functools.partial(widen_kernel, depth, tiles),
        grid=(tiles + depth,),
        in_specs=[
            once(low.shape),
            pl.BlockSpec((D, TILE), lambda i: (0, jnp.minimum(i, half - 1))),
            pl.BlockSpec((1, TILE), lambda i: (0, jnp.minimum(i, last))),
            once(normed.shape),
            once(scales.shape),
            *[once(block.shape) for block in blocks],
        ],
        out_specs=[tile, tile, flat((count, D)), in_place, in_place],
        out_shape=[
            jax.ShapeDtypeStruct((count, FF), BF16),
            jax.ShapeDtypeStruct((count, FF), F32),
            jax.ShapeDtypeStruct((count, D), F32),
            *[jax.ShapeDtypeStruct(shape, BF16) for shape in spread],
        ],
        scratch_shapes=[
            pltpu.VMEM((tiles, count, TILE), BF16),
            pltpu.VMEM((D, TILE), BF16),
            *[pltpu.VMEM(shape, BF16) for shape in spread],
            pltpu.SemaphoreType.DMA((depth + 1,)),
            *gather_sems(2, depth),
        ],
        compiler_params=kernel_params(collective_id, 1),
        name="widen",
    )(low, up_weight, up_bias[None], normed, scales, *blocks)


def early_tile(i, tiles, depth):
    ahead = (lax.axis_index("dp") // 8 + 1) * (tiles // depth)
    return (jnp.minimum(i, tiles - 1) + ahead) % tiles


def widen_back_kernel(depth, tiles, *refs):
    rows_grad, activated, slope, down_weight, low_turned, up_early, up_late = refs[:7]
    up_grad, branch_grad, sums, down_out = refs[7:11]
    kept, down_grad, total, *rest = refs[11:]
    place = Place(depth)
    side = Scatter(place, [down_grad], [down_out], [rest[:BUFS]], *rest[BUFS:], resident=(0,))
    i = pl.program_id(0)
    per = tiles // depth

    def step_of(t, work):
        pl.when(i == t)(work)

    step_of(0, place.greet)
    now = early_tile(i, tiles, depth)
    for n, k in enumerate(side.order):
        ready = (n + 1) * per
        step_of(ready, functools.partial(side.begin, 0, k))
        step_of(ready + 1, functools.partial(side.first, 0, k))
        step_of(ready + 3, functools.partial(side.second, 0, k))
        step_of(ready + 5, functools.partial(side.third, 0, k))

    @pl.when(i < tiles)
    def _():
        for at in range(0, rows_grad.shape[0], ROW_CHUNK):
            rows = slice(at, at + ROW_CHUNK)
            back = dot_over(rows_grad[rows, :], down_weight[...], 1, 1)
            kept[now, rows, :] = (back * slope[rows, :]).astype(BF16)
        sums[0] = jnp.sum(kept[now].astype(F32), axis=0, keepdims=True)
        grad = dot_over(activated[...], rows_grad[...], 0, 0).astype(BF16)
        blocks = TILE // down_grad.shape[4]
        grad = grad.reshape(1, blocks // 4, 2, 2, down_grad.shape[4], D)[0]
        part = pl.ds((now % per) * (blocks // 4), blocks // 4)
        down_grad[now // per, part] = grad

    @pl.when(i >= tiles)
    def _():
        tile = kept[i - tiles]
        up_grad[...] = dot_over(low_turned[...], tile, 1, 0).astype(BF16)
        up_weight = jnp.where(i - tiles < tiles // 2, up_early[...], up_late[...])
        for at in range(0, rows_grad.shape[0], ROW_CHUNK):
            rows = slice(at, at + ROW_CHUNK)
            part = dot_over(tile[rows, :], up_weight, 1, 1)

            @pl.when(i == tiles)
            def _():
                total[rows, :] = part

            @pl.when(i > tiles)
            def _():
                total[rows, :] += part

    @pl.when(i == 2 * tiles - 1)
    def _():
        branch_grad[...] = total[...]
        side.finish(0)


def widen_back(
    rows_grad, activated, slope, down_weight, low_turned, up_early, up_late, depth, collective_id
):
    count = rows_grad.shape[0]
    tiles = FF // TILE

    half = tiles // 2

    def early(i):
        return early_tile(i, tiles, depth)

    def late(i):
        return jnp.maximum(i - tiles, 0)

    shares = 8 * depth
    spread = jax.ShapeDtypeStruct((depth, 2, 2, 2, FF // shares, D), BF16)
    return pl.pallas_call(
        functools.partial(widen_back_kernel, depth, tiles),
        grid=(2 * tiles,),
        in_specs=[
            once(rows_grad.shape),
            pl.BlockSpec((count, TILE), lambda i: (0, early(i))),
            pl.BlockSpec((count, TILE), lambda i: (0, early(i))),
            pl.BlockSpec((TILE, D), lambda i: (early(i), 0)),
            once(low_turned.shape),
            pl.BlockSpec((D, TILE), lambda i: (0, jnp.minimum(late(i), half - 1))),
            pl.BlockSpec((D, TILE), lambda i: (0, jnp.maximum(late(i) - half, 0))),
        ],
        out_specs=[
            pl.BlockSpec((D, TILE), lambda i: (0, late(i))),
            flat((count, D)),
            pl.BlockSpec((1, 1, TILE), lambda i: (early(i), 0, 0)),
            flat(spread.shape[-2:]),
        ],
        out_shape=[
            jax.ShapeDtypeStruct((D, FF), BF16),
            jax.ShapeDtypeStruct((count, D), F32),
            jax.ShapeDtypeStruct((tiles, 1, TILE), F32),
            jax.ShapeDtypeStruct(spread.shape[-2:], F32),
        ],
        scratch_shapes=[
            pltpu.VMEM((tiles, count, TILE), BF16),
            pltpu.VMEM(spread.shape, BF16),
            pltpu.VMEM((count, D), F32),
            *scatter_scratch([spread], depth, resident=(0,)),
        ],
        compiler_params=kernel_params(collective_id, 1),
        name="widen_back",
    )(rows_grad, activated, slope, down_weight, low_turned, up_early, up_late)


ROW_BLOCK = 256


def mean_of(rows):
    return jnp.sum(rows, axis=-1, keepdims=True) * (1.0 / D)


def normalized(hidden):
    center = hidden - mean_of(hidden)
    root = lax.rsqrt(mean_of(center * center) + NORM_EPS)
    return center * root, root


def norm_back(grad, normed, root, gain):
    scaled = grad * gain
    return root * (scaled - mean_of(scaled) - normed * mean_of(scaled * normed))


def add_sums(sums, *rows):
    new = [jnp.sum(r.astype(F32), axis=0, keepdims=True) for r in rows]

    @pl.when(pl.program_id(0) == 0)
    def _():
        sums[...] = jnp.zeros_like(sums)

    for j, n in enumerate(new):
        sums[j : j + 1, :] += n


def project_kernel(attended, tokens, weight, scales, normed, root, low, turned):
    hidden = dot_over(attended[...], weight[...], 1, 0)
    hidden = tokens[...].astype(F32) + hidden + scales[0:1, :]
    normed[...], root[...] = normalized(hidden)
    branch = normed[...] * scales[1:2, :] + scales[2:3, :]
    low[...] = branch.astype(BF16)
    turned[...] = branch.T.astype(BF16)


def output_kernel(second_in, cotangent, scales, output, rows, grad, sums):
    normed, root = normalized(second_in[...])
    output[...] = (normed * scales[0:1, :] + scales[1:2, :]).astype(BF16)
    upstream = cotangent[...].astype(F32)
    grad[...] = norm_back(upstream, normed, root, scales[0:1, :])
    rows[...] = grad[...].astype(BF16)
    add_sums(sums, upstream * normed, upstream, rows[...])


def project_back_kernel(
    branch_grad, second_grad, normed, root, attended, weight, scales, grad, back, weight_grads, sums, total
):
    upstream = branch_grad[...] + second_grad[...]
    grad[...] = norm_back(upstream, normed[...], root[...], scales[0:1, :])
    rows = grad[...].astype(BF16)
    back[...] = dot_over(rows, weight[...], 1, 1).astype(BF16)
    add_sums(sums, upstream * normed[...], upstream, rows)
    part = dot_over(attended[...], rows, 0, 0)

    @pl.when(pl.program_id(0) == 0)
    def _():
        total[...] = part

    @pl.when(pl.program_id(0) > 0)
    def _():
        total[...] += part

    @pl.when(pl.program_id(0) == pl.num_programs(0) - 1)
    def _():
        weight_grads[...] = total[...].astype(weight_grads.dtype)


def row_block(width=D):
    return pl.BlockSpec((ROW_BLOCK, width), lambda i: (i, 0))


def row_call(kernel, count, in_specs, out_specs, outs, scratch=()):
    return pl.pallas_call(
        kernel,
        grid=(count // ROW_BLOCK,),
        in_specs=in_specs,
        out_specs=out_specs,
        out_shape=[jax.ShapeDtypeStruct(shape, dtype) for shape, dtype in outs],
        scratch_shapes=list(scratch),
        compiler_params=pltpu.CompilerParams(vmem_limit_bytes=60 << 20),
        name=kernel.__name__,
    )


SUMS = (8, D)


def project(attended, tokens, weight, scales):
    count = tokens.shape[0]
    block, matrix = row_block(), flat((D, D))
    turned = pl.BlockSpec((D, ROW_BLOCK), lambda i: (0, i))
    outs = [((count, D), F32), ((count, 1), F32), ((count, D), BF16), ((D, count), BF16)]
    return row_call(
        project_kernel,
        count,
        [block, block, matrix, flat(scales.shape)],
        [block, row_block(1), block, turned],
        outs,
    )(attended, tokens, weight, scales)


def output_and_grad(second_in, cotangent, scales):
    count = second_in.shape[0]
    block = row_block()
    shape = (count, D)
    return row_call(
        output_kernel,
        count,
        [block, block, flat(scales.shape)],
        [block, block, block, flat(SUMS)],
        [(shape, BF16), (shape, BF16), (shape, F32), (SUMS, F32)],
    )(second_in, cotangent, scales)


def project_back(branch_grad, second_grad, normed, root, attended, weight, scales, dtype):
    count = attended.shape[0]
    block, matrix = row_block(), flat((D, D))
    shape = (count, D)
    return row_call(
        project_back_kernel,
        count,
        [block, block, block, row_block(1), block, matrix, flat(scales.shape)],
        [block, block, matrix, flat(SUMS)],
        [(shape, F32), (shape, BF16), ((D, D), dtype), (SUMS, F32)],
        [pltpu.VMEM((D, D), F32)],
    )(branch_grad, second_grad, normed, root, attended, weight, scales)


def split_vector(vector):
    sizes = (D, D, D, D, D, FF, D, D, D)
    parts, at = [], 0
    for size in sizes:
        parts.append(vector[at : at + size])
        at += size
    return parts


def by_pair(columns):
    rows = columns.shape[0]
    return columns.reshape(rows, 3, PAIRS, LANES).swapaxes(1, 2).reshape(rows, 3 * D)


def by_kind(columns):
    rows = columns.shape[0]
    return columns.reshape(rows, PAIRS, 3, LANES).swapaxes(1, 2).reshape(rows, 3 * D)


def stacked(*vectors):
    return jnp.pad(jnp.stack(vectors), ((0, 8 - len(vectors)), (0, 0)))


def column_sums(rows):
    return jnp.sum(rows.astype(F32), axis=0)


def times(rows, matrix):
    return jnp.dot(rows, matrix, preferred_element_type=F32)


def weight_grad(left_rows, right_rows, dtype):
    return dot_over(left_rows, right_rows, 0, 0).astype(dtype)


def back_product(grad_rows, matrix):
    return dot_over(grad_rows, matrix, 1, 1)


def layer_step(tokens, doc_ids, cotangent, masters, devices, depth):
    grad_type = BF16 if depth else F32
    shape = (depth, 2, 2, 2)
    blocks, low_vector = lowered_blocks(masters)
    rows = low_vector.shape[0] // LANES
    if depth:
        tall = blocks[0].shape[0]
        padded = jnp.pad(low_vector.reshape(rows, LANES), ((0, tall - rows), (0, 0)))
        first = [blocks[0][:, g * GROUP_WIDTH : (g + 1) * GROUP_WIDTH] for g in range(GROUPS)]
        first[0] = jnp.concatenate([first[0], padded], axis=1)
        up_blocks = [blocks[2][:, : FF // 2], blocks[2][:, FF // 2 :]]
        qkv, attended, totals, qkv_weight, vectors, proj_weight, up_weight = attend(
            tokens, doc_ids, None, None, [*first, blocks[1], up_blocks[0]], rows, depth, 1
        )
        vector = vectors.reshape(devices, tall, LANES)[:, :rows].reshape(-1)
        qkv_weight, proj_weight, up_weight = map(rows_of, (qkv_weight, proj_weight, up_weight))
    else:
        weights = [lax.all_gather(b, "dp", axis=0, tiled=True) for b in blocks]
        qkv_weight, proj_weight, up_weight, down_weight = weights
        vector = lax.all_gather(low_vector, "dp", axis=0, tiled=True)
    (
        bias_query,
        bias_value,
        bias_proj,
        gain_first,
        shift_first,
        bias_up,
        bias_down,
        gain_second,
        shift_second,
    ) = split_vector(vector.astype(F32))
    if not depth:
        bias_all = jnp.concatenate([bias_query, jnp.zeros_like(bias_query), bias_value])
        bias_all = by_pair(bias_all[None])[0]
        qkv, attended, totals = attend(tokens, doc_ids, qkv_weight, bias_all, [], 0, 0, 0)
    normed, root, branch_low, low_turned = project(
        attended, tokens, proj_weight, stacked(bias_proj, gain_first, shift_first)
    )
    if depth:
        activated, slope, second_in, up_late, down_weight = widen(
            branch_low,
            up_weight,
            bias_up,
            normed,
            stacked(gain_first, shift_first, bias_down),
            [up_blocks[1], blocks[3]],
            depth,
            2,
        )
        up_late, down_weight = rows_of(up_late), rows_of(down_weight)
    else:
        upward = times(branch_low, up_weight) + bias_up
        cdf = 0.5 * (1.0 + lax.erf(upward * HALF_ROOT))
        activated = (upward * cdf).astype(BF16)
        slope = cdf + upward * (PDF_TOP * jnp.exp(-0.5 * upward * upward))
        branch = normed * gain_first + shift_first
        second_in = branch + times(activated, down_weight) + bias_down
    output, down_rows, second_grad, second_sums = output_and_grad(
        second_in, cotangent, stacked(gain_second, shift_second)
    )
    if depth:
        up_grad, branch_grad, bias_up_grad, down_owned = widen_back(
            down_rows,
            activated,
            slope,
            down_weight,
            low_turned,
            up_weight,
            up_late,
            depth,
            3,
        )
        bias_up_grad = bias_up_grad.reshape(-1)
    else:
        down_grad = weight_grad(activated, down_rows, F32)
        up_rows = (back_product(down_rows, down_weight) * slope).astype(BF16)
        bias_up_grad = column_sums(up_rows)
        up_grad = weight_grad(branch_low, up_rows, F32)
        branch_grad = back_product(up_rows, up_weight)
    hidden_grad, attended_grad, proj_grad, first_sums = project_back(
        branch_grad,
        second_grad,
        normed,
        root,
        attended,
        proj_weight,
        stacked(gain_first),
        grad_type,
    )
    known = [
        first_sums[2],
        first_sums[0],
        first_sums[1],
        bias_up_grad,
        second_sums[2],
        second_sums[0],
        second_sums[1],
    ]
    riders = []
    if depth:
        vector_part = jnp.concatenate([jnp.zeros((2 * D,), F32), *known])
        vector_part = vector_part.reshape(devices, rows, LANES)
        vector_part = jnp.pad(vector_part, ((0, 0), (0, 16 - rows), (0, 0)))
        riders = [g.reshape(*shape, -1, g.shape[1]) for g in (up_grad, proj_grad)]
        riders += [vector_part.reshape(*shape, 16, LANES)]
    input_grad, *summed = attend_back(
        tokens,
        qkv,
        doc_ids,
        attended_grad,
        totals,
        qkv_weight,
        hidden_grad,
        riders,
        rows,
        depth,
        4,
    )
    if depth:
        up_owned, proj_owned, *qkv_owned, vector_owned = summed
        owned = [jnp.concatenate(qkv_owned, axis=1), proj_owned, up_owned, down_owned]
        owned += [vector_owned[:rows]]
    else:
        qkv_grad, qkv_sums = summed
        qkv_sums = by_kind(qkv_sums.reshape(1, -1))[0]
        vector_grad = jnp.concatenate([qkv_sums[0:D], qkv_sums[2 * D : 3 * D], *known])
        grads = (qkv_grad, proj_grad, up_grad, down_grad, vector_grad[:, None])
        owned = [
            lax.psum_scatter(
                grad.reshape(devices, -1, grad.shape[-1]), "dp", scatter_dimension=0, tiled=True
            )[0]
            for grad in grads
        ]
    owned[0] = by_kind(owned[0])
    return output, input_grad, [own.reshape(-1) for own in owned]


def adam_update(master, moment_one, moment_two, grad, rate):
    one_new = BETA_FIRST * moment_one + (1.0 - BETA_FIRST) * grad
    two_new = BETA_SECOND * moment_two + (1.0 - BETA_SECOND) * grad * grad
    one_hat = one_new / (1.0 - BETA_FIRST**STEP)
    two_hat = two_new / (1.0 - BETA_SECOND**STEP)
    master_new = master - rate * (one_hat / (jnp.sqrt(two_hat) + ADAM_EPS) + WEIGHT_DECAY * master)
    return (grad, one_new, two_new, master_new, master_new.astype(BF16))


WIDTHS = (3 * D, D, FF, D)


def lowered_blocks(masters):
    lowered = [master.astype(BF16) for master in masters]
    blocks = [low.reshape(-1, width) for low, width in zip(lowered, WIDTHS)]
    blocks[0] = by_pair(blocks[0])
    return blocks, lowered[4]


def body(depth, tokens, segment_ids, out_grad, *states):
    devices = lax.axis_size("dp")
    masters = states[0::3]
    output, input_grad, owned = layer_step(
        tokens, segment_ids, out_grad, masters, devices, depth
    )
    outs = [output, input_grad]
    for i in range(5):
        outs += adam_update(*states[3 * i : 3 * i + 3], owned[i], RATES[i])
    return tuple(outs)


def solution(mesh):
    rows = P("dp", None)
    flat = P("dp")
    return jax.shard_map(
        functools.partial(body, depth_of(mesh)),
        mesh=mesh,
        in_specs=(rows,) * 3 + (flat,) * 15,
        out_specs=(rows,) * 2 + (flat,) * 25,
        check_vma=False,
    )
```
